32 devices in a mesh: seq: 4 (over y, core), fsdp: 8 (over z, x).
Axes of the slice: x: 2, y: 2, z: 4, core: 2. Of those that a mesh axis runs over, the one named last changes fastest.
Arguments:
- tokens: bfloat16 [8, 1536, 1024], P('fsdp', 'seq'), may hold values from -6 to 6
- lengths: int32 [8, 3], P('fsdp'), may hold values from 1 to 1024, 1536 in all within a row
- time_steps: int32 [8, 3], P('fsdp'), may hold values from 0 to 999
- order: int32 [8, 1536], P('fsdp', 'seq'), may hold values from 0 to 1535, each once within a row
- w_time: bfloat16 [256, 2048], P('fsdp'), may hold values from -0.375 to 0.375
- w_qkv: bfloat16 [1024, 3072], P('fsdp'), may hold values from -0.1875 to 0.1875
- w_out: bfloat16 [1024, 1024], P('fsdp'), may hold values from -1.5 to 1.5
- w_up: bfloat16 [1024, 4096], P('fsdp'), may hold values from -0.1875 to 0.1875
- w_down: bfloat16 [4096, 1024], P('fsdp'), may hold values from -0.09375 to 0.09375
- cotangent: bfloat16 [8, 1536, 1024], P('fsdp', 'seq'), may hold values from -6 to 6
Outputs:
- output: bfloat16 [8, 1536, 1024], P('fsdp', 'seq')
- input_grad: float32 [8, 1536, 1024], P('fsdp', 'seq')
- grad_time: float32 [256, 2048], P('fsdp')
- grad_qkv: float32 [1024, 3072], P('fsdp')
- grad_out: float32 [1024, 1024], P('fsdp')
- grad_up: float32 [1024, 4096], P('fsdp')
- grad_down: float32 [4096, 1024], P('fsdp')
The draws below stay inside these ranges and needn't reach their ends.
Inputs may be any that keep to these rules, and one draw needn't show every extreme that they name: Each group's 3 lengths sum to 1536; the longest is exactly 1024. `order`: each group's row is a permutation of the indices 0 to 1535.
All inputs are finite; a program needn't handle non-finite values.
Results may differ from the reference program's by a relative error of at most 0.02.
Values may be sent and summed in bfloat16 or wider, within the bound.
A program may use at most 192 MiB of HBM per device.

```python
import math
import jax
import jax.numpy as jnp
import numpy as np
from jax import lax

D = 1024
H = 16
HD = 64
FF = 4096
TEMB = 256
NSEQ = 3
GROUPS = 8
GROUP = 1536
MOST = 1024


def plant(entries, stream_key, smallest, top_value):
    spot = [jax.random.randint(jax.random.fold_in(stream_key, axis), (), 0, length) for axis, length in enumerate(entries.shape)]
    widest = entries.shape.index(max(entries.shape))
    next_to = spot[:widest] + [(spot[widest] + 1) % entries.shape[widest]] + spot[widest + 1:]
    return entries.at[tuple(spot)].set(smallest).at[tuple(next_to)].set(top_value)


def steps_of(stream_key, dims, split, least, largest):
    loudness = 1.0
    for axis_at, shards_of in split:
        steps = jax.random.uniform(jax.random.fold_in(jax.random.fold_in(stream_key, 6), axis_at), (shards_of,), jnp.float32, least / len(split), largest / len(split))
        loudness = loudness * jnp.repeat(jnp.exp(steps), dims[axis_at] // shards_of).reshape((-1,) + (1,) * (len(dims) - 1 - axis_at))
    return loudness


def length_profile(amount, total, limit, slope):
    weights = [(1 << 20) // math.isqrt(standing ** slope) + 1 for standing in range(2, amount + 1)]
    surplus, holding = total - limit - (amount - 1), [1] * (amount - 1)
    while surplus > 0:
        free = [i for i in range(amount - 1) if holding[i] < limit]
        whole, remaining = sum([weights[i] for i in free]), surplus
        for i in free:
            more = min(limit - holding[i], max(1, remaining * weights[i] // whole), surplus)
            holding[i] = holding[i] + more
            surplus = surplus - more
    return np.array([limit] + holding)


def uneven_parts(stream_key, amount, total, limit, lean):
    if amount == 2:
        one = jax.random.randint(stream_key, (), max(1, total - limit), min(limit, total - 1) + 1)
        return jnp.stack([one, total - one])
    tallies = jnp.asarray(length_profile(amount, total, limit, lean), jnp.int32)
    twos = (amount - 1) // 2
    giver, receiver = tallies[1:1 + 2 * twos:2], tallies[2:2 + 2 * twos:2]
    margin = jnp.minimum(giver - 1, limit - receiver)
    shifted = jax.random.randint(jax.random.fold_in(stream_key, 1), (twos,), 0, 1 << 20) % (margin + 1)
    tallies = tallies.at[1:1 + 2 * twos:2].set(giver - shifted).at[2:2 + 2 * twos:2].set(receiver + shifted)
    return tallies[jax.random.permutation(jax.random.fold_in(stream_key, 2), amount)]


def scatter_about(rng, extent, scale, reach, shards=(), kind=jnp.bfloat16):
    factor_of = steps_of(rng, extent, shards, -0.22, 0.18) if shards else 1.0
    values = jax.random.normal(rng, extent, jnp.float32) * scale * factor_of
    return jnp.minimum(jnp.maximum(values, -reach), reach).astype(kind)


def setup_inputs(seed: int = 0) -> dict:
    seeds = jax.random.split(jax.random.key(seed), 11)
    tokens = scatter_about(seeds[0], (GROUPS, GROUP, D), 1.0, 6.0, ((0, 8), (1, 4)))
    lengths = jax.vmap(lambda own: uneven_parts(own, NSEQ, GROUP, MOST, 2))(jax.random.split(seeds[1], GROUPS)).reshape((GROUPS, NSEQ)).astype(jnp.int32)
    time_steps = plant(jax.random.randint(seeds[2], (GROUPS, NSEQ), 0, 1000), jax.random.fold_in(seeds[2], 1), 0, 999).astype(jnp.int32)
    order = jax.vmap(lambda own: jax.random.permutation(own, GROUP))(jax.random.split(seeds[3], GROUPS)).reshape((GROUPS, GROUP)).astype(jnp.int32)
    w_time = scatter_about(seeds[4], (TEMB, 2 * D), TEMB ** -0.5, 0.375, ((0, 8),))
    w_qkv = scatter_about(seeds[5], (D, 3 * D), D ** -0.5, 0.1875, ((0, 8),))
    w_out = scatter_about(seeds[6], (D, D), 16 ** -0.5, 1.5, ((0, 8),))
    w_up = scatter_about(seeds[7], (D, FF), D ** -0.5, 0.1875, ((0, 8),))
    w_down = scatter_about(seeds[8], (FF, D), FF ** -0.5, 0.09375, ((0, 8),))
    cotangent = scatter_about(seeds[9], (GROUPS, GROUP, D), 1.0, 6.0, ((0, 8), (1, 4)))
    return {"tokens": tokens, "lengths": lengths, "time_steps": time_steps, "order": order, "w_time": w_time, "w_qkv": w_qkv, "w_out": w_out, "w_up": w_up, "w_down": w_down, "cotangent": cotangent}


@jax.custom_vjp
def low(v):
    return lax.optimization_barrier(v.astype(jnp.bfloat16)).astype(jnp.float32)

@jax.custom_vjp
def low_back(v):
    return v

def low_keep(v):
    return (low(v), None)

def low_pass(kept, grad):
    return (grad,)

def back_keep(v):
    return (v, None)

def back_low(kept, grad):
    return (low(grad),)
low.defvjp(low_keep, low_pass)
low_back.defvjp(back_keep, back_low)
EPS = 1e-05
NEG = -1e+30
BASE = 10000.0

def hdot(left, right):
    return jnp.matmul(left, right, precision=lax.Precision.HIGHEST)

def time_embedding(steps):
    half = TEMB // 2
    freqs = jnp.exp(-math.log(BASE) * jnp.arange(half, dtype=jnp.float32) / half)
    angles = steps.astype(jnp.float32)[:, None] * freqs[None, :]
    return jnp.concatenate([jnp.sin(angles), jnp.cos(angles)], axis=-1)

def layout(lens, places):
    ends = jnp.cumsum(lens).astype(jnp.int32)
    starts = (ends - lens).astype(jnp.int32)
    member = (places[:, None] >= starts[None, :]) & (places[:, None] < ends[None, :])
    labels = jnp.arange(NSEQ, dtype=jnp.int32)
    segment = lax.optimization_barrier(jnp.sum(jnp.where(member, labels[None, :], 0), axis=1)).astype(jnp.int32)
    offset = (places - lax.optimization_barrier(jnp.sum(jnp.where(member, starts[None, :], 0), axis=1))).astype(jnp.int32)
    return (member.astype(jnp.float32), segment, offset)

def rotate(values, offset, sign):
    half = HD // 2
    freqs = jnp.exp(-math.log(BASE) * jnp.arange(half, dtype=jnp.float32) * 2.0 / HD)
    angles = offset.astype(jnp.float32)[:, None] * freqs[None, :]
    cosine = jnp.cos(angles)[:, None, :]
    sine = sign * jnp.sin(angles)[:, None, :]
    first = values[..., :half]
    second = values[..., half:]
    return jnp.concatenate([first * cosine - second * sine, second * cosine + first * sine], axis=-1)

def norm_mod(values, scale):
    centre = lax.optimization_barrier(jnp.mean(values, axis=-1, keepdims=True))
    centred = values - centre
    spread = lax.optimization_barrier(jnp.mean(centred * centred, axis=-1, keepdims=True))
    return centred * lax.rsqrt(spread + EPS) * (1.0 + scale)

def attend_head(packed):
    query, key, value, segment = packed
    scores = low_back(hdot(query, key.T) * HD ** (-0.5))
    scores = jnp.where(segment[:, None] == segment[None, :], scores, NEG)
    peak = lax.optimization_barrier(jnp.max(scores, axis=-1, keepdims=True))
    expo = jnp.exp(scores - peak)
    probs = low(expo / lax.optimization_barrier(jnp.sum(expo, axis=-1, keepdims=True)))
    return hdot(probs, value)

def layer(inputs, w_time, w_qkv, w_out, w_up, w_down, emb, member, segment, offset):
    count = inputs.shape[0]
    scales = hdot(member, hdot(emb, w_time))
    scale_one = scales[:, :D]
    scale_two = scales[:, D:]
    h_one = low(norm_mod(inputs, scale_one))
    projected = low_back(hdot(h_one, w_qkv))
    query = low(rotate(projected[:, :D].reshape(count, H, HD), offset, 1.0))
    key = low(rotate(projected[:, D:2 * D].reshape(count, H, HD), offset, 1.0))
    value = low(projected[:, 2 * D:].reshape(count, H, HD))
    segs = jnp.broadcast_to(segment[None, :], (H, count))
    heads_out = lax.map(jax.checkpoint(attend_head), (query.transpose(1, 0, 2), key.transpose(1, 0, 2), value.transpose(1, 0, 2), segs))
    mixed = low(low_back(heads_out.transpose(1, 0, 2).reshape(count, D)))
    x_two = inputs + low_back(hdot(mixed, w_out))
    h_two = low(norm_mod(x_two, scale_two))
    hidden = low(jax.nn.gelu(low_back(hdot(h_two, w_up))))
    return x_two + hdot(hidden, w_down)

def reference(tokens, lengths, time_steps, order, w_time, w_qkv, w_out, w_up, w_down, cotangent):
    weights = tuple((w.astype(jnp.float32) for w in (w_time, w_qkv, w_out, w_up, w_down)))

    def one_group(totals, packed):
        rows_in, lens, steps, places, cot = packed
        member, segment, offset = layout(lens, places)
        emb = low(time_embedding(steps))

        def forward(inputs, wa, wb, wc, wd, we):
            return layer(inputs, wa, wb, wc, wd, we, emb, member, segment, offset)
        result, pull = jax.vjp(forward, rows_in.astype(jnp.float32), *weights)
        cot_dealt = jnp.take(cot, places, axis=0).astype(jnp.float32)
        grads = pull(cot_dealt)
        out_orig = jnp.zeros_like(result).at[places].set(result).astype(jnp.bfloat16)
        totals = tuple((t + g for t, g in zip(totals, grads[1:])))
        return (totals, (out_orig, grads[0]))
    zeros = tuple((jnp.zeros(w.shape, jnp.float32) for w in weights))
    totals, outs = lax.scan(one_group, zeros, (tokens, lengths, time_steps, order, cotangent))
    return (outs[0], outs[1], totals[0], totals[1], totals[2], totals[3], totals[4])
```

```python
import functools
import math

import jax
import jax.numpy as jnp
from jax import lax
from jax.experimental import pallas as pl
from jax.experimental.pallas import tpu as pltpu
from jax.sharding import PartitionSpec as P

H = 16
HD = 64
TEMB = 256
NSEQ = 3

EPS = 1e-05
NEG = -1e30
BASE = 10000.0
LOG2E = math.log2(math.e)
CORES = 2
XS = 2
BF = jnp.bfloat16

ANY = pl.BlockSpec(memory_space=pl.ANY)
VM = pl.BlockSpec(memory_space=pltpu.VMEM)
DMA = pltpu.SemaphoreType.DMA
MESH = pl.DeviceIdType.MESH
VMEM_ALL = 67043328

GATHER_CLASS = {"t": "D", "q": "DCD", "o": "D", "u": "CDDC", "d": "DCDD"}
SUM_CLASS = {"t": "DD", "q": "CDC", "o": "D", "u": "CDCD", "d": "CDCC"}


class Place:
    def __init__(self, slices, shards):
        self.Y, self.Z = slices // CORES, shards // XS
        seq, fsdp = lax.axis_index("seq"), lax.axis_index("fsdp")
        self.y, self.c = lax.div(seq, CORES), lax.rem(seq, CORES)
        self.z, self.x = lax.div(fsdp, XS), lax.rem(fsdp, XS)

    def at(self, z=None, x=None, y=None, c=None):
        z = self.z if z is None else z
        x = self.x if x is None else x
        y = self.y if y is None else y
        c = self.c if c is None else c
        return {"seq": y * CORES + c, "fsdp": z * XS + x}

    def next_y(self, d):
        return lax.rem(self.y + d, self.Y)

    def next_z(self, d):
        return lax.rem(self.z + d, self.Z)


def greet(place, fsdp=True):
    barrier = pltpu.get_barrier_semaphore()
    others = [place.at(c=1 - place.c)]
    others += [place.at(y=place.next_y(d)) for d in range(1, place.Y)]
    if fsdp:
        others += [place.at(x=1 - place.x)]
        others += [place.at(z=place.next_z(d)) for d in range(1, place.Z)]
    for other in others:
        pl.semaphore_signal(barrier, inc=1, device_id=other, device_id_type=MESH)
    pl.semaphore_wait(barrier, len(others))


def push(src, dst, send_sem, recv_sem, device):
    copy = pltpu.make_async_remote_copy(
        src_ref=src,
        dst_ref=dst,
        send_sem=send_sem,
        recv_sem=recv_sem,
        device_id=device,
        device_id_type=MESH,
    )
    copy.start()
    return copy


def keep(src, dst, sem):
    copy = pltpu.make_async_copy(src, dst, sem)
    copy.start()
    return copy


def pipeline(plan, stages):
    for t in range(len(plan) + len(stages) - 1):
        for k, stage in enumerate(stages):
            if stage is not None and 0 <= t - k < len(plan):
                stage(plan[t - k])


class RowGather:
    def __init__(self, place, src, out, bounce, sems, rsems, lsem):
        self.place, self.src, self.out = place, src, out
        self.bounce, self.sems, self.rsems, self.lsem = bounce, sems, rsems, lsem

    def load(self):
        self.own = keep(self.src, self.bounce, self.lsem)

    def start(self):
        p = self.place
        slot = self.out.at[p.y, p.c]
        self.over_y = [
            push(self.src, slot, self.sems.at[d], self.rsems.at[d], p.at(y=p.next_y(d)))
            for d in range(1, p.Y)
        ]
        self.own.wait()
        self.own = keep(self.bounce, slot, self.lsem)

    def middle(self):
        p = self.place
        for copy in self.over_y:
            copy.wait_recv()
        self.own.wait()
        half = self.out.at[:, p.c]
        self.over_c = push(half, half, self.sems.at[0], self.rsems.at[0], p.at(c=1 - p.c))

    def end(self):
        for copy in self.over_y:
            copy.wait_send()
        self.over_c.wait()


def pieces(rows, width, which, classes):
    out = []
    for j, name in enumerate(which):
        if name == "t":
            for k, kind in enumerate(classes["t"]):
                span = 2 * width // len(classes["t"])
                out.append((j, 0, rows // 4, k * span, span, kind))
        elif name == "d":
            for k, kind in enumerate(classes["d"]):
                out.append((j, k * rows, rows, 0, width, kind))
        else:
            for k, kind in enumerate(classes[name]):
                out.append((j, 0, rows, k * width, width, kind))
    return out


class WeightGather:
    def __init__(self, place, items, shards, outs, bounce, ssem, rsem, lsem):
        self.place = place
        self.shards, self.outs, self.bounce = shards, outs, bounce
        self.ssem, self.rsem, self.lsem = ssem, rsem, lsem
        self.plan = []
        for i, (w, r0, rn, c0, cn, kind) in enumerate(items):
            half = cn // CORES
            width = half // place.Y if kind == "D" else half
            first = c0 + place.c * half
            if kind == "D":
                first = first + place.y * width
            self.plan.append(
                dict(
                    i=i,
                    w=w,
                    kind=kind,
                    rows=pl.ds(r0, rn),
                    cols=pl.ds(pl.multiple_of(first, 128), width),
                    half=pl.ds(pl.multiple_of(c0 + place.c * half, 128), half),
                    held=bounce.at[i, pl.ds(0, rn), pl.ds(0, width)],
                )
            )

    def region(self, p, z, x, cols):
        return self.outs[p["w"]].at[z, x, p["rows"], cols]

    def load(self):
        for p in self.plan:
            p["own"] = keep(
                self.shards[p["w"]].at[p["rows"], p["cols"]], p["held"], self.lsem.at[p["i"]]
            )

    def store(self):
        place = self.place
        for p in self.plan:
            p["own"].wait()
            p["own"] = keep(
                p["held"], self.region(p, place.z, place.x, p["cols"]), self.lsem.at[p["i"]]
            )

    def post(self, p, slot, src, dst, device):
        return push(src, dst, self.ssem.at[p["i"], slot], self.rsem.at[p["i"], slot], device)

    def over_z(self, p):
        place = self.place
        src = self.shards[p["w"]].at[p["rows"], p["cols"]]
        dst = self.region(p, place.z, place.x, p["cols"])
        p["z"] = [
            self.post(p, d - 1, src, dst, place.at(z=place.next_z(d))) for d in range(1, place.Z)
        ]

    def over_x(self, p):
        place = self.place
        for copy in p["z"]:
            copy.wait_recv()
        p["own"].wait()
        part = self.region(p, pl.ds(0, place.Z), place.x, p["cols"])
        p["x"] = self.post(p, place.Z - 1, part, part, place.at(x=1 - place.x))

    def over_y(self, p):
        place = self.place
        p["x"].wait_recv()
        p["y"] = []
        if p["kind"] == "D":
            part = self.region(p, pl.ds(0, place.Z), pl.ds(0, XS), p["cols"])
            p["y"] = [
                self.post(p, place.Z - 1 + d, part, part, place.at(y=place.next_y(d)))
                for d in range(1, place.Y)
            ]

    def over_c(self, p):
        place = self.place
        for copy in p["y"]:
            copy.wait_recv()
        part = self.region(p, pl.ds(0, place.Z), pl.ds(0, XS), p["half"])
        p["c"] = self.post(p, place.Z - 1 + place.Y, part, part, place.at(c=1 - place.c))

    def finish(self, p):
        p["c"].wait()
        for copy in p["z"] + p["y"] + [p["x"]]:
            copy.wait_send()

    def stages(self):
        return [self.over_z, self.over_x, self.over_y, self.over_c, self.finish]


def gather_body(slices, shards, items, nw, *refs):
    ws, rows_in = refs[:nw], refs[nw : nw + 2]
    outs, rows_out = refs[nw + 2 : 2 * nw + 2], refs[2 * nw + 2 : 2 * nw + 4]
    bounce, ssem, rsem, lsem, b0, b1, sseq, rseq, lseq = refs[2 * nw + 4 :]
    place = Place(slices, shards)
    gather = WeightGather(place, items, ws, outs, bounce, ssem, rsem, lsem)
    rows = [
        RowGather(place, src, out, b, sseq.at[k], rseq.at[k], lseq.at[k])
        for k, (src, out, b) in enumerate(zip(rows_in, rows_out, (b0, b1)))
    ]
    gather.load()
    for r in rows:
        r.load()
    greet(place)
    gather.over_z(gather.plan[0])
    rows[0].start()
    rows[1].start()
    gather.store()
    stages = gather.stages()
    first = gather.plan[0]
    stages[0] = lambda p: None if p is first else gather.over_z(p)
    pipeline(gather.plan, stages)
    for r in rows:
        r.middle()
    for r in rows:
        r.end()


def gather_all(slices, shards, width, ws, rows_in):
    Y, Z = slices // CORES, shards // XS
    rows = ws[1].shape[0]
    items = pieces(rows, width, "tqoud", GATHER_CLASS)
    n, nw = len(items), len(ws)
    widest = max(cn // CORES // (Y if kind == "D" else 1) for _, _, _, _, cn, kind in items)
    out = pl.pallas_call(
        functools.partial(gather_body, slices, shards, items, nw),
        out_shape=[jax.ShapeDtypeStruct((Z, XS) + w.shape, w.dtype) for w in ws]
        + [jax.ShapeDtypeStruct((Y, CORES) + r.shape, r.dtype) for r in rows_in],
        in_specs=[ANY] * (nw + 2),
        out_specs=[ANY] * (nw + 2),
        scratch_shapes=[
            pltpu.VMEM((n, rows, widest), BF),
            DMA((n, Z + Y)),
            DMA((n, Z + Y)),
            DMA((n,)),
        ]
        + [pltpu.VMEM(r.shape, r.dtype) for r in rows_in]
        + [DMA((2, Y)), DMA((2, Y)), DMA((2,))],
        compiler_params=pltpu.CompilerParams(
            collective_id=0, has_side_effects=True, vmem_limit_bytes=VMEM_ALL
        ),
    )(*ws, *rows_in)
    full = [g.reshape(-1, g.shape[-1]) for g in out[:nw]]
    return full, [g.reshape((slices,) + r.shape) for g, r in zip(out[nw:], rows_in)]


def add_into(dst, src, rn):
    lead = dst.shape[:-2]

    def step(k, _):
        idx, rest = [], k
        for size in reversed(lead[1:]):
            idx.append(lax.rem(rest, size))
            rest = lax.div(rest, size)
        idx = tuple(reversed(idx + [rest]))
        a, b = dst.at[idx], src.at[idx]
        rows = pl.ds(0, rn)
        a[rows, :] = (a[rows, :].astype(jnp.float32) + b[rows, :].astype(jnp.float32)).astype(BF)
        return 0

    lax.fori_loop(0, math.prod(lead), step, 0)


class GradSum:
    def __init__(self, place, items, grads, outs, acc, rc, ry, rx, rz, fin, rf, lsem, ssem, rsem):
        self.place, self.grads, self.outs = place, grads, outs
        self.acc, self.rc, self.ry, self.rx, self.rz = acc, rc, ry, rx, rz
        self.fin, self.rf = fin, rf
        self.lsem, self.ssem, self.rsem = lsem, ssem, rsem
        self.wide = acc.shape[-1]
        self.plan = []
        for i, (w, r0, rn, c0, cn, kind) in enumerate(items):
            p = dict(i=i, w=w, kind=kind, rn=rn, c0=c0, half=cn // CORES)
            p.update(rows=pl.ds(r0, rn), vr=pl.ds(0, rn), sends=[])
            self.plan.append(p)

    def post(self, p, slot, src, dst, device):
        copy = push(src, dst, self.ssem.at[p["i"], slot], self.rsem.at[p["i"], slot], device)
        p["sends"].append(copy)
        return copy

    def cols(self, p, core, part=None):
        first = p["c0"] + core * p["half"]
        if part is None:
            return pl.ds(pl.multiple_of(first, 128), p["half"])
        return pl.ds(pl.multiple_of(first + part * self.wide, 128), self.wide)

    def parts(self, p):
        return [self.place.y] if p["kind"] == "D" else list(range(self.place.Y))

    def over_c(self, p):
        place, i, vr = self.place, p["i"], p["vr"]
        g = self.grads[p["w"]]
        first = place.Z + place.Y + place.Y
        p["own"], p["c"] = [], []
        for part in range(place.Y):
            p["own"].append(
                keep(
                    g.at[:, :, p["rows"], self.cols(p, place.c, part)],
                    self.acc.at[i, part, :, :, vr, :],
                    self.lsem.at[i, part],
                )
            )
            p["c"].append(
                self.post(
                    p,
                    first + part,
                    g.at[:, :, p["rows"], self.cols(p, 1 - place.c, part)],
                    self.rc.at[i, part, :, :, vr, :],
                    place.at(c=1 - place.c),
                )
            )

    def over_y(self, p):
        place, i, vr = self.place, p["i"], p["vr"]
        for copy in p["own"]:
            copy.wait()
        for copy in p["c"]:
            copy.wait_recv()
        for part in range(place.Y):
            add_into(self.acc.at[i, part], self.rc.at[i, part], p["rn"])
        p["y"] = []
        if p["kind"] == "D":
            for d in range(1, place.Y):
                y = place.next_y(d)
                p["y"].append(
                    self.post(
                        p,
                        d,
                        self.acc.at[i, y, :, :, vr, :],
                        self.ry.at[i, d - 1, :, :, vr, :],
                        place.at(y=y),
                    )
                )

    def over_x(self, p):
        place, i, vr = self.place, p["i"], p["vr"]
        for d, copy in enumerate(p["y"]):
            copy.wait_recv()
            add_into(self.acc.at[i, place.y], self.ry.at[i, d], p["rn"])
        other = 1 - place.x
        if p["kind"] == "D":
            src, dst = self.acc.at[i, place.y, :, other, vr, :], self.rx.at[i, 0, :, vr, :]
        else:
            src, dst = self.acc.at[i, :, :, other, vr, :], self.rx.at[i, :, :, vr, :]
        p["x"] = self.post(p, place.Y, src, dst, place.at(x=other))

    def over_z(self, p):
        place, i, vr = self.place, p["i"], p["vr"]
        p["x"].wait_recv()
        for k, part in enumerate(self.parts(p)):
            add_into(self.acc.at[i, part, :, place.x], self.rx.at[i, k], p["rn"])
        p["z"] = []
        for d in range(1, place.Z):
            z = place.next_z(d)
            if p["kind"] == "D":
                src = self.acc.at[i, place.y, z, place.x, vr, :]
                dst = self.rz.at[i, d - 1, 0, vr, :]
            else:
                src = self.acc.at[i, :, z, place.x, vr, :]
                dst = self.rz.at[i, d - 1, :, vr, :]
            p["z"].append(self.post(p, place.Y + d, src, dst, place.at(z=z)))

    def region(self, p, core, part=None):
        return self.outs[p["w"]].at[p["rows"], self.cols(p, core, part)]

    def back_y(self, p):
        place, i, vr = self.place, p["i"], p["vr"]
        for copy in p["z"]:
            copy.wait_recv()
        for k, part in enumerate(self.parts(p)):
            total = self.acc[i, part, place.z, place.x, vr, :].astype(jnp.float32)
            for d in range(1, place.Z):
                total = total + self.rz[i, d - 1, k, vr, :].astype(jnp.float32)
            if p["kind"] == "D":
                self.fin[i, 0, vr, :] = total.astype(BF)
            else:
                self.rf[i, place.y, part, vr, :] = total.astype(BF)
        first = place.Z + place.Y - 1
        p["f"], p["st"] = [], []
        if p["kind"] == "D":
            src, dst = self.fin.at[i, 0, vr, :], self.region(p, place.c, place.y)
            p["st"].append(keep(src, dst, self.lsem.at[i, 0]))
        else:
            src = dst = self.rf.at[i, place.y, :, vr, :]
        for d in range(1, place.Y):
            p["f"].append(self.post(p, first + d, src, dst, place.at(y=place.next_y(d))))

    def back_c(self, p):
        place, i, vr = self.place, p["i"], p["vr"]
        for copy in p["f"]:
            copy.wait_recv()
        if p["kind"] == "C":
            for part in range(place.Y):
                total = self.rf[i, 0, part, vr, :].astype(jnp.float32)
                for y in range(1, place.Y):
                    total = total + self.rf[i, y, part, vr, :].astype(jnp.float32)
                self.fin[i, part, vr, :] = total.astype(BF)
                src, dst = self.fin.at[i, part, vr, :], self.region(p, place.c, part)
                p["st"].append(keep(src, dst, self.lsem.at[i, part]))
        for copy in p["st"]:
            copy.wait()
        part = self.region(p, place.c)
        p["e"] = self.post(p, 0, part, part, place.at(c=1 - place.c))

    def finish(self, p):
        p["e"].wait_recv()
        for copy in p["sends"]:
            copy.wait_send()

    def stages(self):
        return [
            self.over_c,
            self.over_y,
            self.over_x,
            self.over_z,
            self.back_y,
            self.back_c,
            self.finish,
        ]


def sum_scratch(slices, shards, items, rows):
    Y, Z = slices // CORES, shards // XS
    n, wide = len(items), items[0][4] // CORES // Y
    return [
        pltpu.VMEM((n, Y, Z, XS, rows, wide), BF),
        pltpu.VMEM((n, Y, Z, XS, rows, wide), BF),
        pltpu.VMEM((n, Y - 1, Z, XS, rows, wide), BF),
        pltpu.VMEM((n, Y, Z, rows, wide), BF),
        pltpu.VMEM((n, Z - 1, Y, rows, wide), BF),
        pltpu.VMEM((n, Y, rows, wide), BF),
        pltpu.VMEM((n, Y, Y, rows, wide), BF),
        DMA((n, Y)),
        DMA((n, Z + 3 * Y)),
        DMA((n, Z + 3 * Y)),
    ]


def sum_body(slices, shards, items, nw, nr, *refs):
    grads, rows_in = refs[:nw], refs[nw : nw + nr]
    outs, rows_out = refs[nw + nr : 2 * nw + nr], refs[2 * nw + nr : 2 * (nw + nr)]
    scratch = refs[2 * (nw + nr) :]
    place = Place(slices, shards)
    sums = GradSum(place, items, grads, outs, *scratch[:10])
    rows = []
    for k in range(nr):
        b, s, r, m = scratch[10 + 4 * k : 14 + 4 * k]
        rows.append(RowGather(place, rows_in[k], rows_out[k], b, s, r, m.at[0]))
    for r in rows:
        r.load()
    greet(place)
    for r in rows:
        r.start()
    pipeline(sums.plan, sums.stages())
    for r in rows:
        r.middle()
    for r in rows:
        r.end()


def sum_grads(slices, shards, width, which, grads, rows_in, cid):
    Y, Z = slices // CORES, shards // XS
    rows = width // shards
    items = pieces(rows, width, which, SUM_CLASS)
    nw, nr = len(grads), len(rows_in)
    grads = [g.reshape(Z, XS, -1, g.shape[1]) for g in grads]
    extra = []
    for r in rows_in:
        extra += [pltpu.VMEM(r.shape, r.dtype), DMA((Y,)), DMA((Y,)), DMA((1,))]
    out = pl.pallas_call(
        functools.partial(sum_body, slices, shards, items, nw, nr),
        out_shape=[jax.ShapeDtypeStruct(g.shape[2:], BF) for g in grads]
        + [jax.ShapeDtypeStruct((Y, CORES) + r.shape, r.dtype) for r in rows_in],
        in_specs=[ANY] * (nw + nr),
        out_specs=[ANY] * (nw + nr),
        scratch_shapes=sum_scratch(slices, shards, items, rows) + extra,
        compiler_params=pltpu.CompilerParams(
            collective_id=cid, has_side_effects=True, vmem_limit_bytes=VMEM_ALL
        ),
    )(*grads, *rows_in)
    return out[:nw], [g.reshape((slices,) + r.shape) for g, r in zip(out[nw:], rows_in)]


def dot(a, b, ca, cb):
    return lax.dot_general(a, b, (((ca,), (cb,)), ((), ())), preferred_element_type=jnp.float32)


def swap_halves(v):
    lane = lax.broadcasted_iota(jnp.int32, v.shape, 1)
    left = pltpu.roll(v, v.shape[1] - HD // 2, 1)
    right = pltpu.roll(v, HD // 2, 1)
    return jnp.where(lax.rem(lane, HD) < HD // 2, left, right)


def forward_block(qkv, seg_col, seg_row, mixed, logsum, h, rows):
    lanes = slice(h * HD, (h + 1) * HD)
    s = dot(qkv[1, :, lanes], qkv[0, rows, lanes], 1, 1) * (LOG2E * HD**-0.5)
    s = jnp.where(seg_col[...] == seg_row[:, rows], s, NEG)
    peak = jnp.max(s, axis=0, keepdims=True)
    expo = jnp.exp2(s - peak)
    total = jnp.sum(expo, axis=0, keepdims=True)
    out = dot(expo.astype(BF), qkv[2, :, lanes], 0, 0)
    mixed[rows, lanes] = (out / total.T).astype(BF)
    logsum[h : h + 1, rows] = peak + jnp.log2(total)


def backward_block(qkv, mixed, logsum, g, seg_col, seg_row, dk, dv, dq, h, rows):
    lanes = slice(h * HD, (h + 1) * HD)
    q, gb = qkv[0, rows, lanes], g[rows, lanes]
    k, v = qkv[1, :, lanes], qkv[2, :, lanes]
    prod = gb.astype(jnp.float32) * mixed[rows, lanes].astype(jnp.float32)
    delta = jnp.sum(prod, axis=1, keepdims=True).T
    s = dot(k, q, 1, 1) * (LOG2E * HD**-0.5)
    same = seg_col[...] == seg_row[:, rows]
    probs = jnp.where(same, jnp.exp2(s - logsum[h : h + 1, rows]), 0.0)
    ds = (probs * (dot(v, gb, 1, 1) - delta)).astype(BF)
    dv[:, lanes] += dot(probs.astype(BF), gb, 1, 0)
    dk[:, lanes] += dot(ds, q, 1, 0)
    dq[rows, lanes] = dot(ds, k, 0, 0)


def forward_body(heads, block, qkv, seg_col, seg_row, mixed, logsum):
    for h in range(heads):

        def step(i, _):
            rows = pl.ds(pl.multiple_of(i * block, block), block)
            forward_block(qkv, seg_col, seg_row, mixed, logsum, h, rows)
            return 0

        lax.fori_loop(0, seg_col.shape[0] // block, step, 0)


def backward_body(
    heads, block, qkv, mixed, logsum, g, seg_col, seg_row, cos, sin, out, dk, dv, dq
):
    dk[...] = jnp.zeros_like(dk)
    dv[...] = jnp.zeros_like(dv)
    steps = seg_col.shape[0] // block
    for h in range(heads):

        def step(i, _):
            rows = pl.ds(pl.multiple_of(i * block, block), block)
            backward_block(qkv, mixed, logsum, g, seg_col, seg_row, dk, dv, dq, h, rows)
            return 0

        lax.fori_loop(0, steps, step, 0)

    def finish(i, _):
        rows = pl.ds(pl.multiple_of(i * block, block), block)
        c, s = cos[rows, :], sin[rows, :]
        for j, d in enumerate((dq, dk)):
            for t in range(heads * HD // 128):
                w = slice(t * 128, (t + 1) * 128)
                v = d[rows, w] * (HD**-0.5)
                out[j, rows, w] = (v * c - swap_halves(v) * s).astype(BF)
        out[2, rows, :] = dv[rows, :].astype(BF)
        return 0

    lax.fori_loop(0, steps, finish, 0)


def attention_forward(qkv, seg_col, seg_row, block=512):
    _, group, width = qkv.shape
    heads = width // HD
    return pl.pallas_call(
        functools.partial(forward_body, heads, block),
        out_shape=(
            jax.ShapeDtypeStruct((group, width), BF),
            jax.ShapeDtypeStruct((heads, group), jnp.float32),
        ),
        in_specs=[VM] * 3,
        out_specs=(VM, VM),
        compiler_params=pltpu.CompilerParams(vmem_limit_bytes=VMEM_ALL),
    )(qkv, seg_col, seg_row)


def attention_backward(qkv, mixed, logsum, g, seg_col, seg_row, cos, sin, block=512):
    _, group, width = qkv.shape
    total = pltpu.VMEM((group, width), jnp.float32)
    return pl.pallas_call(
        functools.partial(backward_body, width // HD, block),
        out_shape=jax.ShapeDtypeStruct((3, group, width), BF),
        in_specs=[VM] * 8,
        out_specs=VM,
        scratch_shapes=[total] * 3,
        compiler_params=pltpu.CompilerParams(vmem_limit_bytes=VMEM_ALL),
    )(qkv, mixed, logsum, g, seg_col, seg_row, cos, sin)


def project_body(h, w, cos, sin, out):
    y = jnp.dot(h[...], w[...], preferred_element_type=jnp.float32)
    turned = (pl.program_id(0) < 2).astype(jnp.float32)
    c = cos[...] * turned + (1.0 - turned)
    s = sin[...] * turned
    for t in range(y.shape[1] // 128):
        w_ = slice(t * 128, (t + 1) * 128)
        out[0, :, w_] = (y[:, w_] * c + swap_halves(y[:, w_]) * s).astype(BF)


def project(h, w, cos, sin, block=512):
    rows, width = h.shape
    const = lambda j, n: (0, 0)
    per = width // block
    return pl.pallas_call(
        project_body,
        grid=(3, per),
        out_shape=jax.ShapeDtypeStruct((3, rows, width), BF),
        in_specs=[
            pl.BlockSpec((rows, width), const),
            pl.BlockSpec((width, block), lambda j, n: (0, j * per + n)),
            pl.BlockSpec((rows, 128), const),
            pl.BlockSpec((rows, 128), const),
        ],
        out_specs=pl.BlockSpec((1, rows, block), lambda j, n: (j, 0, n)),
        compiler_params=pltpu.CompilerParams(vmem_limit_bytes=VMEM_ALL),
    )(h, w, cos, sin)


def time_embedding(steps):
    half = TEMB // 2
    freqs = jnp.exp(-math.log(BASE) * jnp.arange(half, dtype=jnp.float32) / half)
    angles = steps.astype(jnp.float32)[:, None] * freqs[None, :]
    return jnp.concatenate([jnp.sin(angles), jnp.cos(angles)], axis=-1)


def layout(lens, places):
    ends = jnp.cumsum(lens)
    starts = ends - lens
    member = (places[:, None] >= starts[None, :]) & (places[:, None] < ends[None, :])
    labels = jnp.arange(NSEQ, dtype=jnp.int32)
    segment = jnp.sum(jnp.where(member, labels[None, :], 0), axis=1)
    offset = places - jnp.sum(jnp.where(member, starts[None, :], 0), axis=1)
    return (member.astype(jnp.float32), segment, offset)


def turn_tables(offset):
    half = HD // 2
    freqs = jnp.exp(-math.log(BASE) * jnp.arange(half, dtype=jnp.float32) * 2.0 / HD)
    angles = offset.astype(jnp.float32)[:, None] * freqs[None, :]
    c, s = jnp.cos(angles), jnp.sin(angles)
    return jnp.concatenate([c] * 4, axis=1), jnp.concatenate([-s, s, -s, s], axis=1)


def norm_mod(values, scale):
    centre = jnp.mean(values, axis=-1, keepdims=True)
    centred = values - centre
    spread = jnp.mean(centred * centred, axis=-1, keepdims=True)
    return centred * lax.rsqrt(spread + EPS) * (1.0 + scale)


def pick_rows(data, wanted, labels):
    pick = (wanted[:, None] == labels[None, :]).astype(BF)
    return jnp.dot(pick, data.reshape(-1, data.shape[-1]), preferred_element_type=jnp.float32)


def on_device(tokens, lengths, time_steps, order, w_time, w_qkv, w_out, w_up, w_down, cotangent):
    rows, width = tokens.shape[1:]
    slices, shards = lax.axis_size("seq"), lax.axis_size("fsdp")
    group = rows * slices
    lens, places = lengths[0], order[0]
    gathered, (order_all, cot_all) = gather_all(
        slices, shards, width, [w_time, w_qkv, w_out, w_up, w_down], [order, cotangent[0]]
    )
    f_time, f_qkv, f_out, f_up, f_down = gathered
    order_all = order_all.reshape(group)

    member, _, offset = layout(lens, places)
    _, segment_all, offset_all = layout(lens, order_all)
    seg_col, seg_row = segment_all[:, None], segment_all[None, :]
    emb = time_embedding(time_steps[0]).astype(BF)
    scales_seq = jnp.dot(emb, f_time, preferred_element_type=jnp.float32)
    scales = jnp.dot(member, scales_seq, precision=lax.Precision.HIGHEST)
    scale_one, scale_two = scales[:, :width], scales[:, width:]
    inputs = tokens[0].astype(jnp.float32)
    normed_one, pull_one = jax.vjp(norm_mod, inputs, scale_one)
    h_one = normed_one.astype(BF)

    cos, sin = turn_tables(offset)
    packed = project(h_one, f_qkv, cos, sin)
    heads_qkv = lax.all_to_all(packed, "seq", split_axis=2, concat_axis=1, tiled=True)
    mixed_heads, logsum = attention_forward(heads_qkv, seg_col, seg_row)
    mixed = lax.all_to_all(mixed_heads, "seq", split_axis=0, concat_axis=1, tiled=True)

    x_two = inputs + jnp.dot(mixed, f_out, preferred_element_type=jnp.float32)
    normed_two, pull_two = jax.vjp(norm_mod, x_two, scale_two)
    h_two = normed_two.astype(BF)
    up = jnp.dot(h_two, f_up, preferred_element_type=jnp.float32)
    activated, pull_gelu = jax.vjp(jax.nn.gelu, up)
    hidden = activated.astype(BF)
    result = (x_two + jnp.dot(hidden, f_down, preferred_element_type=jnp.float32)).astype(BF)

    d_result = pick_rows(cot_all, places, jnp.arange(group, dtype=jnp.int32))
    d_low = d_result.astype(BF)
    grad_down = dot(hidden, d_low, 0, 0).astype(BF)
    d_up = pull_gelu(dot(d_low, f_down, 1, 1))[0].astype(BF)
    grad_up = dot(h_two, d_up, 0, 0).astype(BF)
    d_xpart, d_scale_two = pull_two(dot(d_up, f_up, 1, 1))
    d_xtwo = d_result + d_xpart
    d_attn = d_xtwo.astype(BF)
    grad_out = dot(mixed, d_attn, 0, 0).astype(BF)
    d_mixed = dot(d_attn, f_out, 1, 1).astype(BF)

    d_heads = lax.all_to_all(d_mixed, "seq", split_axis=1, concat_axis=0, tiled=True)
    cos_all, sin_all = turn_tables(offset_all)
    d_qkv_heads = attention_backward(
        heads_qkv, mixed_heads, logsum, d_heads, seg_col, seg_row, cos_all, sin_all
    )
    d_packed = lax.all_to_all(d_qkv_heads, "seq", split_axis=1, concat_axis=2, tiled=True)
    d_qkv = d_packed.transpose(1, 0, 2).reshape(rows, 3 * width)
    grad_qkv = dot(h_one, d_qkv, 0, 0).astype(BF)
    d_xone, d_scale_one = pull_one(dot(d_qkv, f_qkv, 1, 1))
    input_grad = d_xtwo + d_xone
    d_scales = lax.dot_general(
        member,
        jnp.concatenate([d_scale_one, d_scale_two], axis=1),
        (((0,), (0,)), ((), ())),
        precision=lax.Precision.HIGHEST,
        preferred_element_type=jnp.float32,
    )
    grad_time = lax.dot_general(
        emb.astype(jnp.float32),
        d_scales,
        (((0,), (0,)), ((), ())),
        precision=lax.Precision.HIGHEST,
        preferred_element_type=jnp.float32,
    ).astype(BF)

    grads, (result_all,) = sum_grads(
        slices, shards, width, "duoqt",
        [grad_down, grad_up, grad_out, grad_qkv, grad_time], [result], 1,
    )
    s_down, s_up, s_out, s_qkv, s_time = [g.astype(jnp.float32) for g in grads]
    mine = lax.axis_index("seq") * rows + jnp.arange(rows, dtype=jnp.int32)
    output = pick_rows(result_all, mine, order_all).astype(BF)
    return (output[None], input_grad[None], s_time, s_qkv, s_out, s_up, s_down)


def solution(mesh):
    row, tok, mat = P("fsdp", None), P("fsdp", "seq", None), P("fsdp", None)
    return jax.shard_map(
        on_device,
        mesh=mesh,
        in_specs=(tok, row, row, P("fsdp", "seq"), mat, mat, mat, mat, mat, tok),
        out_specs=(tok, tok, mat, mat, mat, mat, mat),
        check_vma=False,
    )
```

```python
import functools
import math

import jax
import jax.numpy as jnp
from jax import lax
from jax.experimental import pallas as pl
from jax.experimental.pallas import tpu as pltpu
from jax.sharding import PartitionSpec as P

H = 16
HD = 64
TEMB = 256
NSEQ = 3

EPS = 1e-05
NEG = -1e30
BASE = 10000.0
LOG2E = math.log2(math.e)
CORES = 2
XS = 2
BF = jnp.bfloat16

ANY = pl.BlockSpec(memory_space=pl.ANY)
VM = pl.BlockSpec(memory_space=pltpu.VMEM)
DMA = pltpu.SemaphoreType.DMA
MESH = pl.DeviceIdType.MESH
VMEM_ALL = 67043328

GATHER_CLASS = {"t": "D", "q": "CDC", "o": "C", "u": "CDCD", "d": "CDCD"}
SUM_CLASS = {"t": "DD", "q": "CDC", "o": "C", "u": "CCDC", "d": "CDCC"}


class Place:
    def __init__(self, slices, shards):
        self.Y, self.Z = slices // CORES, shards // XS
        seq, fsdp = lax.axis_index("seq"), lax.axis_index("fsdp")
        self.y, self.c = lax.div(seq, CORES), lax.rem(seq, CORES)
        self.z, self.x = lax.div(fsdp, XS), lax.rem(fsdp, XS)

    def at(self, z=None, x=None, y=None, c=None):
        z = self.z if z is None else z
        x = self.x if x is None else x
        y = self.y if y is None else y
        c = self.c if c is None else c
        return {"seq": y * CORES + c, "fsdp": z * XS + x}

    def next_y(self, d):
        return lax.rem(self.y + d, self.Y)

    def next_z(self, d):
        return lax.rem(self.z + d, self.Z)


def greet(place, seq=False):
    barrier = pltpu.get_barrier_semaphore()
    others = [place.at(c=1 - place.c), place.at(x=1 - place.x)]
    others += [place.at(y=place.next_y(d)) for d in range(1, place.Y)]
    others += [place.at(z=place.next_z(d)) for d in range(1, place.Z)]
    if seq:
        others += [place.at(y=place.next_y(d), c=1 - place.c) for d in range(1, place.Y)]
    for other in others:
        pl.semaphore_signal(barrier, inc=1, device_id=other, device_id_type=MESH)
    pl.semaphore_wait(barrier, len(others))


def push(src, dst, send_sem, recv_sem, device):
    copy = pltpu.make_async_remote_copy(
        src_ref=src,
        dst_ref=dst,
        send_sem=send_sem,
        recv_sem=recv_sem,
        device_id=device,
        device_id_type=MESH,
    )
    copy.start()
    return copy


def keep(src, dst, sem):
    copy = pltpu.make_async_copy(src, dst, sem)
    copy.start()
    return copy


def pipeline(plan, stages):
    return [
        functools.partial(stage, plan[t - k])
        for t in range(len(plan) + len(stages) - 1)
        for k, stage in enumerate(stages)
        if 0 <= t - k < len(plan)
    ]


def run(steps):
    for step in steps:
        step()


def interleave(steps, work, ahead, per):
    run(steps[:ahead])
    rest = steps[ahead:]
    for piece in work:
        piece()
        now, rest = rest[:per], rest[per:]
        run(now)
    run(rest)


class RowGather:
    def __init__(self, place, src, out, bounce, sems, rsems, lsem):
        self.place, self.src, self.out = place, src, out
        self.bounce, self.sems, self.rsems, self.lsem = bounce, sems, rsems, lsem

    def load(self):
        self.own = keep(self.src, self.bounce, self.lsem)

    def start(self):
        p = self.place
        slot = self.out.at[p.y, p.c]
        self.over_y = [
            push(self.src, slot, self.sems.at[d], self.rsems.at[d], p.at(y=p.next_y(d)))
            for d in range(1, p.Y)
        ]
        self.own.wait()
        self.own = keep(self.bounce, slot, self.lsem)

    def middle(self):
        p = self.place
        for copy in self.over_y:
            copy.wait_recv()
        self.own.wait()
        half = self.out.at[:, p.c]
        self.over_c = push(half, half, self.sems.at[0], self.rsems.at[0], p.at(c=1 - p.c))

    def end(self):
        for copy in self.over_y:
            copy.wait_send()
        self.over_c.wait()


def pieces(rows, width, which, classes):
    out = []
    for j, name in enumerate(which):
        if name == "t":
            for k, kind in enumerate(classes["t"]):
                span = 2 * width // len(classes["t"])
                out.append((j, 0, rows // 4, k * span, span, kind))
        elif name == "d":
            for k, kind in enumerate(classes["d"]):
                out.append((j, k * rows, rows, 0, width, kind))
        else:
            for k, kind in enumerate(classes[name]):
                out.append((j, 0, rows, k * width, width, kind))
    return out


class WeightGather:
    def __init__(self, place, items, shards, outs, bounce, ssem, rsem, lsem):
        self.place = place
        self.shards, self.outs, self.bounce = shards, outs, bounce
        self.ssem, self.rsem, self.lsem = ssem, rsem, lsem
        self.plan = []
        for i, (w, r0, rn, c0, cn, kind) in enumerate(items):
            half = cn // CORES
            width = half // place.Y if kind == "D" else half
            first = c0 + place.c * half
            if kind == "D":
                first = first + place.y * width
            self.plan.append(
                dict(
                    i=i,
                    w=w,
                    kind=kind,
                    rows=pl.ds(r0, rn),
                    cols=pl.ds(pl.multiple_of(first, 128), width),
                    half=pl.ds(pl.multiple_of(c0 + place.c * half, 128), half),
                    held=bounce.at[i, pl.ds(0, rn), pl.ds(0, width)],
                )
            )

    def region(self, p, z, x, cols):
        return self.outs[p["w"]].at[z, x, p["rows"], cols]

    def load(self):
        for p in self.plan:
            p["own"] = keep(
                self.shards[p["w"]].at[p["rows"], p["cols"]], p["held"], self.lsem.at[p["i"]]
            )

    def store(self):
        place = self.place
        for p in self.plan:
            p["own"].wait()
            p["own"] = keep(
                p["held"], self.region(p, place.z, place.x, p["cols"]), self.lsem.at[p["i"]]
            )

    def post(self, p, slot, src, dst, device):
        return push(src, dst, self.ssem.at[p["i"], slot], self.rsem.at[p["i"], slot], device)

    def over_z(self, p):
        place = self.place
        src = self.shards[p["w"]].at[p["rows"], p["cols"]]
        dst = self.region(p, place.z, place.x, p["cols"])
        p["z"] = [
            self.post(p, d - 1, src, dst, place.at(z=place.next_z(d))) for d in range(1, place.Z)
        ]

    def over_x(self, p):
        place = self.place
        for copy in p["z"]:
            copy.wait_recv()
        p["own"].wait()
        part = self.region(p, pl.ds(0, place.Z), place.x, p["cols"])
        p["x"] = self.post(p, place.Z - 1, part, part, place.at(x=1 - place.x))

    def over_y(self, p):
        place = self.place
        p["x"].wait_recv()
        p["y"] = []
        if p["kind"] == "D":
            part = self.region(p, pl.ds(0, place.Z), pl.ds(0, XS), p["cols"])
            p["y"] = [
                self.post(p, place.Z - 1 + d, part, part, place.at(y=place.next_y(d)))
                for d in range(1, place.Y)
            ]

    def over_c(self, p):
        place = self.place
        for copy in p["y"]:
            copy.wait_recv()
        part = self.region(p, pl.ds(0, place.Z), pl.ds(0, XS), p["half"])
        p["c"] = self.post(p, place.Z - 1 + place.Y, part, part, place.at(c=1 - place.c))

    def finish(self, p):
        p["c"].wait()
        for copy in p["z"] + p["y"] + [p["x"]]:
            copy.wait_send()

    def stages(self):
        return [self.over_z, self.over_x, self.over_y, self.over_c, self.finish]


def gather_scratch(slices, shards, items, rows):
    Y, Z = slices // CORES, shards // XS
    n = len(items)
    widest = max(cn // CORES // (Y if kind == "D" else 1) for _, _, _, _, cn, kind in items)
    return [pltpu.VMEM((n, rows, widest), BF), DMA((n, Z + Y)), DMA((n, Z + Y)), DMA((n,))]


def gathered_shapes(slices, shards, ws, rows_in):
    Y, Z = slices // CORES, shards // XS
    return [jax.ShapeDtypeStruct((Z, XS) + w.shape, w.dtype) for w in ws] + [
        jax.ShapeDtypeStruct((Y, CORES) + r.shape, r.dtype) for r in rows_in
    ]


def row_scratch(slices, rows_in):
    Y = slices // CORES
    out = []
    for r in rows_in:
        out += [pltpu.VMEM(r.shape, r.dtype), DMA((Y,)), DMA((Y,)), DMA((1,))]
    return out


def row_gathers(place, rows_in, rows_out, scratch):
    rows = []
    for k, (src, out) in enumerate(zip(rows_in, rows_out)):
        b, s, r, m = scratch[4 * k : 4 * k + 4]
        rows.append(RowGather(place, src, out, b, s, r, m.at[0]))
    return rows


def merged(fulls):
    return [g.reshape(-1, g.shape[-1]) for g in fulls]


def gather_body(slices, shards, items, nw, nr, *refs):
    ws, rows_in = refs[:nw], refs[nw : nw + nr]
    outs, rows_out = refs[nw + nr : 2 * nw + nr], refs[2 * nw + nr : 2 * (nw + nr)]
    scratch = refs[2 * (nw + nr) :]
    place = Place(slices, shards)
    gather = WeightGather(place, items, ws, outs, *scratch[:4])
    rows = row_gathers(place, rows_in, rows_out, scratch[4:])
    gather.load()
    for r in rows:
        r.load()
    greet(place)
    steps = pipeline(gather.plan, gather.stages())
    run(steps[:1])
    for r in rows:
        r.start()
    gather.store()
    run(steps[1:])
    for r in rows:
        r.middle()
    for r in rows:
        r.end()


def gather_weights(slices, shards, width, which, ws, rows_in, cid):
    rows = width // shards
    items = pieces(rows, width, which, GATHER_CLASS)
    nw, nr = len(ws), len(rows_in)
    out = pl.pallas_call(
        functools.partial(gather_body, slices, shards, items, nw, nr),
        out_shape=gathered_shapes(slices, shards, ws, rows_in),
        in_specs=[ANY] * (nw + nr),
        out_specs=[ANY] * (nw + nr),
        scratch_shapes=gather_scratch(slices, shards, items, rows) + row_scratch(slices, rows_in),
        compiler_params=pltpu.CompilerParams(
            collective_id=cid, has_side_effects=True, vmem_limit_bytes=VMEM_ALL
        ),
    )(*ws, *rows_in)
    return merged(out[:nw]), [
        g.reshape((slices,) + r.shape) for g, r in zip(out[nw:], rows_in)
    ]


def add_into(dst, src, rn):
    lead = dst.shape[:-2]

    def step(k, _):
        idx, rest = [], k
        for size in reversed(lead[1:]):
            idx.append(lax.rem(rest, size))
            rest = lax.div(rest, size)
        idx = tuple(reversed(idx + [rest]))
        a, b = dst.at[idx], src.at[idx]
        rows = pl.ds(0, rn)
        a[rows, :] = (a[rows, :].astype(jnp.float32) + b[rows, :].astype(jnp.float32)).astype(BF)
        return 0

    lax.fori_loop(0, math.prod(lead), step, 0)


class GradSum:
    def __init__(self, place, items, grads, outs, acc, rc, ry, rx, rz, fin, rf, lsem, ssem, rsem):
        self.place, self.grads, self.outs = place, grads, outs
        self.acc, self.rc, self.ry, self.rx, self.rz = acc, rc, ry, rx, rz
        self.fin, self.rf = fin, rf
        self.lsem, self.ssem, self.rsem = lsem, ssem, rsem
        self.wide = acc.shape[-1]
        self.plan = []
        for i, (w, r0, rn, c0, cn, kind) in enumerate(items):
            p = dict(i=i, w=w, kind=kind, rn=rn, c0=c0, half=cn // CORES)
            p["k"] = sum(q["kind"] == kind for q in self.plan)
            p.update(rows=pl.ds(r0, rn), vr=pl.ds(0, rn), sends=[])
            self.plan.append(p)

    def post(self, p, slot, src, dst, device):
        copy = push(src, dst, self.ssem.at[p["i"], slot], self.rsem.at[p["i"], slot], device)
        p["sends"].append(copy)
        return copy

    def cols(self, p, core, part=None):
        first = p["c0"] + core * p["half"]
        if part is None:
            return pl.ds(pl.multiple_of(first, 128), p["half"])
        return pl.ds(pl.multiple_of(first + part * self.wide, 128), self.wide)

    def parts(self, p):
        return [self.place.y] if p["kind"] == "D" else list(range(self.place.Y))

    def over_c(self, p):
        place, i, vr = self.place, p["i"], p["vr"]
        g = self.grads[p["w"]]
        first = place.Z + place.Y + place.Y
        p["own"], p["c"] = [], []
        for part in range(place.Y):
            p["own"].append(
                keep(
                    g.at[:, :, p["rows"], self.cols(p, place.c, part)],
                    self.acc.at[i, part, :, :, vr, :],
                    self.lsem.at[i, part],
                )
            )
            p["c"].append(
                self.post(
                    p,
                    first + part,
                    g.at[:, :, p["rows"], self.cols(p, 1 - place.c, part)],
                    self.rc.at[i, part, :, :, vr, :],
                    place.at(c=1 - place.c),
                )
            )

    def over_y(self, p):
        place, i, vr = self.place, p["i"], p["vr"]
        for copy in p["own"]:
            copy.wait()
        for copy in p["c"]:
            copy.wait_recv()
        for part in range(place.Y):
            add_into(self.acc.at[i, part], self.rc.at[i, part], p["rn"])
        p["y"] = []
        if p["kind"] == "D":
            for d in range(1, place.Y):
                y = place.next_y(d)
                p["y"].append(
                    self.post(
                        p,
                        d,
                        self.acc.at[i, y, :, :, vr, :],
                        self.ry.at[p["k"], d - 1, :, :, vr, :],
                        place.at(y=y),
                    )
                )

    def over_x(self, p):
        place, i, vr = self.place, p["i"], p["vr"]
        for d, copy in enumerate(p["y"]):
            copy.wait_recv()
            add_into(self.acc.at[i, place.y], self.ry.at[p["k"], d], p["rn"])
        other = 1 - place.x
        if p["kind"] == "D":
            src, dst = self.acc.at[i, place.y, :, other, vr, :], self.rx.at[i, 0, :, vr, :]
        else:
            src, dst = self.acc.at[i, :, :, other, vr, :], self.rx.at[i, :, :, vr, :]
        p["x"] = self.post(p, place.Y, src, dst, place.at(x=other))

    def over_z(self, p):
        place, i, vr = self.place, p["i"], p["vr"]
        p["x"].wait_recv()
        for k, part in enumerate(self.parts(p)):
            add_into(self.acc.at[i, part, :, place.x], self.rx.at[i, k], p["rn"])
        p["z"] = []
        for d in range(1, place.Z):
            z = place.next_z(d)
            if p["kind"] == "D":
                src = self.acc.at[i, place.y, z, place.x, vr, :]
                dst = self.rz.at[i, d - 1, 0, vr, :]
            else:
                src = self.acc.at[i, :, z, place.x, vr, :]
                dst = self.rz.at[i, d - 1, :, vr, :]
            p["z"].append(self.post(p, place.Y + d, src, dst, place.at(z=z)))

    def region(self, p, core, part=None):
        return self.outs[p["w"]].at[p["rows"], self.cols(p, core, part)]

    def back_y(self, p):
        place, i, vr = self.place, p["i"], p["vr"]
        for copy in p["z"]:
            copy.wait_recv()
        for k, part in enumerate(self.parts(p)):
            total = self.acc[i, part, place.z, place.x, vr, :].astype(jnp.float32)
            for d in range(1, place.Z):
                total = total + self.rz[i, d - 1, k, vr, :].astype(jnp.float32)
            if p["kind"] == "D":
                self.fin[i, 0, vr, :] = total.astype(BF)
            else:
                self.rf[p["k"], place.y, part, vr, :] = total.astype(BF)
        first = place.Z + place.Y - 1
        p["f"], p["st"] = [], []
        if p["kind"] == "D":
            src, dst = self.fin.at[i, 0, vr, :], self.region(p, place.c, place.y)
            p["st"].append(keep(src, dst, self.lsem.at[i, 0]))
        else:
            src = dst = self.rf.at[p["k"], place.y, :, vr, :]
        for d in range(1, place.Y):
            p["f"].append(self.post(p, first + d, src, dst, place.at(y=place.next_y(d))))

    def back_c(self, p):
        place, i, vr = self.place, p["i"], p["vr"]
        for copy in p["f"]:
            copy.wait_recv()
        if p["kind"] == "C":
            for part in range(place.Y):
                total = self.rf[p["k"], 0, part, vr, :].astype(jnp.float32)
                for y in range(1, place.Y):
                    total = total + self.rf[p["k"], y, part, vr, :].astype(jnp.float32)
                self.fin[i, part, vr, :] = total.astype(BF)
                src, dst = self.fin.at[i, part, vr, :], self.region(p, place.c, part)
                p["st"].append(keep(src, dst, self.lsem.at[i, part]))
        for copy in p["st"]:
            copy.wait()
        part = self.region(p, place.c)
        p["e"] = self.post(p, 0, part, part, place.at(c=1 - place.c))

    def finish(self, p):
        p["e"].wait_recv()
        for copy in p["sends"]:
            copy.wait_send()

    def stages(self):
        return [
            self.over_c,
            self.over_y,
            self.over_x,
            self.over_z,
            self.back_y,
            self.back_c,
            self.finish,
        ]


def sum_scratch(slices, shards, items, rows):
    Y, Z = slices // CORES, shards // XS
    n, wide = len(items), items[0][4] // CORES // Y
    nd = max(1, sum(item[5] == "D" for item in items))
    nc = max(1, n - nd)
    return [
        pltpu.VMEM((n, Y, Z, XS, rows, wide), BF),
        pltpu.VMEM((n, Y, Z, XS, rows, wide), BF),
        pltpu.VMEM((nd, Y - 1, Z, XS, rows, wide), BF),
        pltpu.VMEM((n, Y, Z, rows, wide), BF),
        pltpu.VMEM((n, Z - 1, Y, rows, wide), BF),
        pltpu.VMEM((n, Y, rows, wide), BF),
        pltpu.VMEM((nc, Y, Y, rows, wide), BF),
        DMA((n, Y)),
        DMA((n, Z + 3 * Y)),
        DMA((n, Z + 3 * Y)),
    ]


def sum_body(slices, shards, items, nw, *refs):
    place = Place(slices, shards)
    sums = GradSum(place, items, refs[:nw], refs[nw : 2 * nw], *refs[2 * nw :])
    greet(place)
    run(pipeline(sums.plan, sums.stages()))


def split_grads(shards, grads):
    return [g.reshape(shards // XS, XS, -1, g.shape[1]) for g in grads]


def sum_grads(slices, shards, width, which, grads, cid):
    rows = width // shards
    items = pieces(rows, width, which, SUM_CLASS)
    nw = len(grads)
    grads = split_grads(shards, grads)
    return pl.pallas_call(
        functools.partial(sum_body, slices, shards, items, nw),
        out_shape=[jax.ShapeDtypeStruct(g.shape[2:], BF) for g in grads],
        in_specs=[ANY] * nw,
        out_specs=[ANY] * nw,
        scratch_shapes=sum_scratch(slices, shards, items, rows),
        compiler_params=pltpu.CompilerParams(
            collective_id=cid, has_side_effects=True, vmem_limit_bytes=VMEM_ALL
        ),
    )(*grads)


def dot(a, b, ca, cb):
    return lax.dot_general(a, b, (((ca,), (cb,)), ((), ())), preferred_element_type=jnp.float32)


def swap_halves(v):
    lane = lax.broadcasted_iota(jnp.int32, v.shape, 1)
    left = pltpu.roll(v, v.shape[1] - HD // 2, 1)
    right = pltpu.roll(v, HD // 2, 1)
    return jnp.where(lax.rem(lane, HD) < HD // 2, left, right)


def forward_block(qkv, seg_col, seg_row, mixed, logsum, h, rows):
    lanes = slice(h * HD, (h + 1) * HD)
    s = dot(qkv[1, :, lanes], qkv[0, rows, lanes], 1, 1) * (LOG2E * HD**-0.5)
    s = jnp.where(seg_col[...] == seg_row[:, rows], s, NEG)
    peak = jnp.max(s, axis=0, keepdims=True)
    expo = jnp.exp2(s - peak)
    total = jnp.sum(expo, axis=0, keepdims=True)
    out = dot(expo.astype(BF), qkv[2, :, lanes], 0, 0)
    mixed[rows, lanes] = (out / total.T).astype(BF)
    logsum[h : h + 1, rows] = peak + jnp.log2(total)


def backward_block(qkv, mixed, logsum, g, seg_col, seg_row, dk, dv, dq, h, rows, slot):
    lanes = slice(h * HD, (h + 1) * HD)
    side = slice(slot * HD, (slot + 1) * HD)
    q, gb = qkv[0, rows, lanes], g[rows, lanes]
    k, v = qkv[1, :, lanes], qkv[2, :, lanes]
    prod = gb.astype(jnp.float32) * mixed[rows, lanes].astype(jnp.float32)
    delta = jnp.sum(prod, axis=1, keepdims=True).T
    s = dot(k, q, 1, 1) * (LOG2E * HD**-0.5)
    same = seg_col[...] == seg_row[:, rows]
    probs = jnp.where(same, jnp.exp2(s - logsum[h : h + 1, rows]), 0.0)
    ds = (probs * (dot(v, gb, 1, 1) - delta)).astype(BF)
    dv[:, side] += dot(probs.astype(BF), gb, 1, 0)
    dk[:, side] += dot(ds, q, 1, 0)
    dq[rows, side] = dot(ds, k, 0, 0)


class Exchange:
    def __init__(self, place, ssem, rsem, lsem):
        self.place, self.ssem, self.rsem, self.lsem = place, ssem, rsem, lsem
        self.me = place.y * CORES + place.c
        self.peers = []
        for dy in list(range(1, place.Y)) + [0]:
            for dc in (range(CORES) if dy else (1,)):
                y, c = place.next_y(dy), lax.rem(place.c + dc, CORES)
                self.peers.append((dy * CORES + dc, y * CORES + c, place.at(y=y, c=c)))
        self.copies = {}

    def give(self, k, src, dst):
        slot, _, device = self.peers[k]
        self.copies[k] = push(src, dst, self.ssem.at[slot], self.rsem.at[slot], device)

    def mine(self, src, dst):
        self.own = keep(src, dst, self.lsem)

    def take(self):
        for copy in self.copies.values():
            copy.wait_recv()
        self.own.wait()

    def close(self):
        for copy in self.copies.values():
            copy.wait_send()


def span(index, size):
    return pl.ds(pl.multiple_of(index * size, size), size)


def forward_body(slices, shards, items, nw, *refs):
    ws, packed, seg_col, seg_row = refs[:nw], *refs[nw : nw + 3]
    outs = refs[nw + 3 : 2 * nw + 3]
    qkv, mixed_heads, logsum, mixed = refs[2 * nw + 3 : 2 * nw + 7]
    scratch = refs[2 * nw + 7 :]
    place = Place(slices, shards)
    rows, part = mixed.shape[0], mixed_heads.shape[1]
    gather = WeightGather(place, items, ws, outs, *scratch[:4])
    pairs = part // 128
    come, *backs = [
        Exchange(place, *[r.at[t] for r in scratch[4:7]]) for t in range(1 + pairs)
    ]
    me = come.me
    gather.load()
    come.mine(packed.at[:, :, span(me, part)], qkv.at[:, span(me, rows), :])
    greet(place, seq=True)
    for k, (_, peer, _) in enumerate(come.peers):
        come.give(k, packed.at[:, :, span(peer, part)], qkv.at[:, span(me, rows), :])
    steps = pipeline(gather.plan, gather.stages())
    run(steps[:1])
    gather.store()

    block = 256

    def attend(h):
        def step(i, _):
            forward_block(qkv, seg_col, seg_row, mixed_heads, logsum, h, span(i, block))
            return 0

        lax.fori_loop(0, seg_col.shape[0] // block, step, 0)

    def finish(t, k, owner):
        src = mixed_heads.at[span(owner, rows), t * 128 : (t + 1) * 128]
        first = pl.multiple_of(me * part + t * 128, 128)
        dst = mixed.at[:, pl.ds(first, 128)]
        if k < len(come.peers):
            backs[t].give(k, src, dst)
        else:
            backs[t].mine(src, dst)

    work = [come.take]
    owners = [peer for _, peer, _ in come.peers] + [me]
    for t in range(pairs):
        work += [functools.partial(attend, h) for h in (2 * t, 2 * t + 1)]
        work += [functools.partial(finish, t, k, owner) for k, owner in enumerate(owners)]
    interleave(steps[1:], work, 12, 4)
    for back in backs:
        back.take()
    for ex in [come] + backs:
        ex.close()


def attention_forward(slices, shards, width, which, ws, packed, seg_col, seg_row, cid):
    rows = packed.shape[1]
    group, part = rows * slices, width // slices
    items = pieces(width // shards, width, which, GATHER_CLASS)
    nw = len(ws)
    out = pl.pallas_call(
        functools.partial(forward_body, slices, shards, items, nw),
        out_shape=gathered_shapes(slices, shards, ws, [])
        + [
            jax.ShapeDtypeStruct((3, group, part), BF),
            jax.ShapeDtypeStruct((group, part), BF),
            jax.ShapeDtypeStruct((part // HD, group), jnp.float32),
            jax.ShapeDtypeStruct((rows, width), BF),
        ],
        in_specs=[ANY] * (nw + 1) + [VM] * 2,
        out_specs=[ANY] * nw + [VM] * 4,
        scratch_shapes=gather_scratch(slices, shards, items, width // shards)
        + [DMA((1 + part // 128, slices))] * 2
        + [DMA((1 + part // 128,))],
        compiler_params=pltpu.CompilerParams(
            collective_id=cid, has_side_effects=True, vmem_limit_bytes=VMEM_ALL
        ),
    )(*ws, packed, seg_col, seg_row)
    return merged(out[:nw]), out[nw:]


def backward_body(slices, shards, items, nw, nr, *refs):
    grads, rows_in = refs[:nw], refs[nw : nw + nr]
    at = nw + nr
    d_mixed, qkv, mixed, logsum, seg_col, seg_row, cos, sin = refs[at : at + 8]
    at += 8
    sums_out, rows_out, out = refs[at : at + nw], refs[at + nw : at + nw + nr], refs[at + nw + nr]
    scratch = refs[at + nw + nr + 1 :]
    place = Place(slices, shards)
    sums = GradSum(place, items, grads, sums_out, *scratch[:10])
    gathers = row_gathers(place, rows_in, rows_out, scratch[10:])
    g, dk, dv, dq, turned, ssem, rsem, lsem = scratch[10 + 4 * nr :]
    rows, part = d_mixed.shape[0], g.shape[1]
    pairs = part // 128
    come = Exchange(place, ssem.at[0], rsem.at[0], lsem.at[0])
    backs = [
        Exchange(place, ssem.at[1 + t], rsem.at[1 + t], lsem.at[1 + t]) for t in range(pairs)
    ]
    me = come.me
    come.mine(d_mixed.at[:, span(me, part)], g.at[span(me, rows), :])
    for r in gathers:
        r.load()
    greet(place, seq=True)
    for k, (_, peer, _) in enumerate(come.peers):
        come.give(k, d_mixed.at[:, span(peer, part)], g.at[span(me, rows), :])
    for r in gathers:
        r.start()

    block = 256

    def attend(h):
        if h % 2 == 0:
            dk[...] = jnp.zeros_like(dk)
            dv[...] = jnp.zeros_like(dv)

        def step(i, _):
            backward_block(
                qkv, mixed, logsum, g, seg_col, seg_row, dk, dv, dq, h, span(i, block), h % 2
            )
            return 0

        lax.fori_loop(0, seg_col.shape[0] // block, step, 0)

    def finish(t, k, owner):
        own = span(owner, rows)
        c, s = cos[own, :], sin[own, :]
        for j, d in enumerate((dq, dk)):
            v = d[own, :] * (HD**-0.5)
            turned[t, j, own, :] = (v * c - swap_halves(v) * s).astype(BF)
        turned[t, 2, own, :] = dv[own, :].astype(BF)
        first = pl.multiple_of(me * part + t * 128, 128)
        src, dst = turned.at[t, :, own, :], out.at[:, :, pl.ds(first, 128)]
        if k < len(come.peers):
            backs[t].give(k, src, dst)
        else:
            backs[t].mine(src, dst)

    work = [come.take]
    owners = [peer for _, peer, _ in come.peers] + [me]
    for t in range(pairs):
        work += [functools.partial(attend, h) for h in (2 * t, 2 * t + 1)]
        work += [functools.partial(finish, t, k, owner) for k, owner in enumerate(owners)]
    steps = pipeline(sums.plan, sums.stages())
    interleave(steps, work, 10, 4)
    for r in gathers:
        r.middle()
    for back in backs:
        back.take()
    for r in gathers:
        r.end()
    for ex in [come] + backs:
        ex.close()


def attention_backward(
    slices, shards, width, which, grads, rows_in, d_mixed, kept, seg_col, seg_row, cos, sin, cid
):
    rows = d_mixed.shape[0]
    group, part = rows * slices, width // slices
    items = pieces(width // shards, width, which, SUM_CLASS)
    nw, nr, pairs = len(grads), len(rows_in), part // 128
    grads = split_grads(shards, grads)
    total = pltpu.VMEM((group, 128), jnp.float32)
    out = pl.pallas_call(
        functools.partial(backward_body, slices, shards, items, nw, nr),
        out_shape=[jax.ShapeDtypeStruct(w.shape[2:], BF) for w in grads]
        + gathered_shapes(slices, shards, [], rows_in)
        + [jax.ShapeDtypeStruct((3, rows, width), BF)],
        in_specs=[ANY] * (nw + nr + 1) + [VM] * 7,
        out_specs=[ANY] * (nw + nr) + [VM],
        scratch_shapes=sum_scratch(slices, shards, items, width // shards)
        + row_scratch(slices, rows_in)
        + [pltpu.VMEM((group, part), BF), total, total, total]
        + [pltpu.VMEM((pairs, 3, group, 128), BF)]
        + [DMA((1 + pairs, slices)), DMA((1 + pairs, slices)), DMA((1 + pairs,))],
        compiler_params=pltpu.CompilerParams(
            collective_id=cid, has_side_effects=True, vmem_limit_bytes=VMEM_ALL
        ),
    )(*grads, *rows_in, d_mixed, *kept, seg_col, seg_row, cos, sin)
    full = [g.reshape((slices,) + r.shape) for g, r in zip(out[nw:], rows_in)]
    return out[:nw], full, out[nw + nr]


def project_body(h, w, cos, sin, out):
    y = jnp.dot(h[...], w[...], preferred_element_type=jnp.float32)
    turned = (pl.program_id(0) < 2).astype(jnp.float32)
    c = cos[...] * turned + (1.0 - turned)
    s = sin[...] * turned
    for t in range(y.shape[1] // 128):
        w_ = slice(t * 128, (t + 1) * 128)
        out[0, :, w_] = (y[:, w_] * c + swap_halves(y[:, w_]) * s).astype(BF)


def project(h, w, cos, sin, block=512):
    rows, width = h.shape
    const = lambda j, n: (0, 0)
    per = width // block
    return pl.pallas_call(
        project_body,
        grid=(3, per),
        out_shape=jax.ShapeDtypeStruct((3, rows, width), BF),
        in_specs=[
            pl.BlockSpec((rows, width), const),
            pl.BlockSpec((width, block), lambda j, n: (0, j * per + n)),
            pl.BlockSpec((rows, 128), const),
            pl.BlockSpec((rows, 128), const),
        ],
        out_specs=pl.BlockSpec((1, rows, block), lambda j, n: (j, 0, n)),
        compiler_params=pltpu.CompilerParams(vmem_limit_bytes=VMEM_ALL),
    )(h, w, cos, sin)


def time_embedding(steps):
    half = TEMB // 2
    freqs = jnp.exp(-math.log(BASE) * jnp.arange(half, dtype=jnp.float32) / half)
    angles = steps.astype(jnp.float32)[:, None] * freqs[None, :]
    return jnp.concatenate([jnp.sin(angles), jnp.cos(angles)], axis=-1)


def layout(lens, places):
    ends = jnp.cumsum(lens)
    starts = ends - lens
    member = (places[:, None] >= starts[None, :]) & (places[:, None] < ends[None, :])
    labels = jnp.arange(NSEQ, dtype=jnp.int32)
    segment = jnp.sum(jnp.where(member, labels[None, :], 0), axis=1)
    offset = places - jnp.sum(jnp.where(member, starts[None, :], 0), axis=1)
    return (member.astype(jnp.float32), segment, offset)


def turn_tables(offset):
    half = HD // 2
    freqs = jnp.exp(-math.log(BASE) * jnp.arange(half, dtype=jnp.float32) * 2.0 / HD)
    angles = offset.astype(jnp.float32)[:, None] * freqs[None, :]
    c, s = jnp.cos(angles), jnp.sin(angles)
    return jnp.concatenate([c] * 4, axis=1), jnp.concatenate([-s, s, -s, s], axis=1)


def norm_mod(values, scale):
    centre = jnp.mean(values, axis=-1, keepdims=True)
    centred = values - centre
    spread = jnp.mean(centred * centred, axis=-1, keepdims=True)
    return centred * lax.rsqrt(spread + EPS) * (1.0 + scale)


def pick_rows(data, wanted, labels):
    pick = (wanted[:, None] == labels[None, :]).astype(BF)
    return jnp.dot(pick, data.reshape(-1, data.shape[-1]), preferred_element_type=jnp.float32)


def on_device(tokens, lengths, time_steps, order, w_time, w_qkv, w_out, w_up, w_down, cotangent):
    rows, width = tokens.shape[1:]
    slices, shards = lax.axis_size("seq"), lax.axis_size("fsdp")
    group = rows * slices
    lens, places = lengths[0], order[0]
    (f_time, f_qkv), (order_all, cot_all) = gather_weights(
        slices, shards, width, "tq", [w_time, w_qkv], [order, cotangent[0]], 0
    )
    order_all = order_all.reshape(group)

    member, _, offset = layout(lens, places)
    _, segment_all, offset_all = layout(lens, order_all)
    seg_col, seg_row = segment_all[:, None], segment_all[None, :]
    emb = time_embedding(time_steps[0]).astype(BF)
    scales_seq = jnp.dot(emb, f_time, preferred_element_type=jnp.float32)
    scales = jnp.dot(member, scales_seq, precision=lax.Precision.HIGHEST)
    scale_one, scale_two = scales[:, :width], scales[:, width:]
    inputs = tokens[0].astype(jnp.float32)
    normed_one, pull_one = jax.vjp(norm_mod, inputs, scale_one)
    h_one = normed_one.astype(BF)

    cos, sin = turn_tables(offset)
    packed = project(h_one, f_qkv, cos, sin)
    (f_out, f_up, f_down), (heads_qkv, mixed_heads, logsum, mixed) = attention_forward(
        slices, shards, width, "oud", [w_out, w_up, w_down], packed, seg_col, seg_row, 1
    )

    x_two = inputs + jnp.dot(mixed, f_out, preferred_element_type=jnp.float32)
    normed_two, pull_two = jax.vjp(norm_mod, x_two, scale_two)
    h_two = normed_two.astype(BF)
    up = jnp.dot(h_two, f_up, preferred_element_type=jnp.float32)
    activated, pull_gelu = jax.vjp(jax.nn.gelu, up)
    hidden = activated.astype(BF)
    result = (x_two + jnp.dot(hidden, f_down, preferred_element_type=jnp.float32)).astype(BF)

    d_result = pick_rows(cot_all, places, jnp.arange(group, dtype=jnp.int32))
    d_low = d_result.astype(BF)
    grad_down = dot(hidden, d_low, 0, 0).astype(BF)
    d_up = pull_gelu(dot(d_low, f_down, 1, 1))[0].astype(BF)
    grad_up = dot(h_two, d_up, 0, 0).astype(BF)
    d_xpart, d_scale_two = pull_two(dot(d_up, f_up, 1, 1))
    d_xtwo = d_result + d_xpart
    d_attn = d_xtwo.astype(BF)
    grad_out = dot(mixed, d_attn, 0, 0).astype(BF)
    d_mixed = dot(d_attn, f_out, 1, 1).astype(BF)

    cos_all, sin_all = turn_tables(offset_all)
    sums, (result_all,), d_packed = attention_backward(
        slices,
        shards,
        width,
        "duo",
        [grad_down, grad_up, grad_out],
        [result],
        d_mixed,
        (heads_qkv, mixed_heads, logsum),
        seg_col,
        seg_row,
        cos_all,
        sin_all,
        2,
    )
    d_qkv = d_packed.transpose(1, 0, 2).reshape(rows, 3 * width)
    grad_qkv = dot(h_one, d_qkv, 0, 0).astype(BF)
    d_xone, d_scale_one = pull_one(dot(d_qkv, f_qkv, 1, 1))
    input_grad = d_xtwo + d_xone
    d_scales = lax.dot_general(
        member,
        jnp.concatenate([d_scale_one, d_scale_two], axis=1),
        (((0,), (0,)), ((), ())),
        precision=lax.Precision.HIGHEST,
        preferred_element_type=jnp.float32,
    )
    grad_time = lax.dot_general(
        emb.astype(jnp.float32),
        d_scales,
        (((0,), (0,)), ((), ())),
        precision=lax.Precision.HIGHEST,
        preferred_element_type=jnp.float32,
    ).astype(BF)

    sums = sums + sum_grads(slices, shards, width, "qt", [grad_qkv, grad_time], 3)
    s_down, s_up, s_out, s_qkv, s_time = [g.astype(jnp.float32) for g in sums]
    mine = lax.axis_index("seq") * rows + jnp.arange(rows, dtype=jnp.int32)
    output = pick_rows(result_all, mine, order_all).astype(BF)
    return (output[None], input_grad[None], s_time, s_qkv, s_out, s_up, s_down)


def solution(mesh):
    row, tok, mat = P("fsdp", None), P("fsdp", "seq", None), P("fsdp", None)
    return jax.shard_map(
        on_device,
        mesh=mesh,
        in_specs=(tok, row, row, P("fsdp", "seq"), mat, mat, mat, mat, mat, tok),
        out_specs=(tok, tok, mat, mat, mat, mat, mat),
        check_vma=False,
    )
```

```python
import functools
import math

import jax
import jax.numpy as jnp
from jax import lax
from jax.experimental import pallas as pl
from jax.experimental.pallas import tpu as pltpu
from jax.sharding import PartitionSpec as P

H = 16
HD = 64
TEMB = 256
NSEQ = 3

EPS = 1e-05
NEG = -1e30
BASE = 10000.0
LOG2E = math.log2(math.e)
CORES = 2
XS = 2
BF = jnp.bfloat16

ANY = pl.BlockSpec(memory_space=pl.ANY)
VM = pl.BlockSpec(memory_space=pltpu.VMEM)
DMA = pltpu.SemaphoreType.DMA
MESH = pl.DeviceIdType.MESH
VMEM_ALL = 67043328
CUT = 2
LAG = 2

GATHER_CLASS = {"t": "D", "q": "CDC", "o": "C", "u": "CDCD", "d": "CDCD"}
SUM_CLASS = {"t": "DD", "q": "CDC", "o": "C", "u": "CCDC", "d": "CDCC"}


class Place:
    def __init__(self, slices, shards):
        self.Y, self.Z = slices // CORES, shards // XS
        seq, fsdp = lax.axis_index("seq"), lax.axis_index("fsdp")
        self.y, self.c = lax.div(seq, CORES), lax.rem(seq, CORES)
        self.z, self.x = lax.div(fsdp, XS), lax.rem(fsdp, XS)

    def at(self, z=None, x=None, y=None, c=None):
        z = self.z if z is None else z
        x = self.x if x is None else x
        y = self.y if y is None else y
        c = self.c if c is None else c
        return {"seq": y * CORES + c, "fsdp": z * XS + x}

    def next_y(self, d):
        return lax.rem(self.y + d, self.Y)

    def next_z(self, d):
        return lax.rem(self.z + d, self.Z)


def greet(place, seq=False):
    barrier = pltpu.get_barrier_semaphore()
    others = [place.at(c=1 - place.c), place.at(x=1 - place.x)]
    others += [place.at(y=place.next_y(d)) for d in range(1, place.Y)]
    others += [place.at(z=place.next_z(d)) for d in range(1, place.Z)]
    if seq:
        others += [place.at(y=place.next_y(d), c=1 - place.c) for d in range(1, place.Y)]
    for other in others:
        pl.semaphore_signal(barrier, inc=1, device_id=other, device_id_type=MESH)
    pl.semaphore_wait(barrier, len(others))


def push(src, dst, send_sem, recv_sem, device):
    copy = pltpu.make_async_remote_copy(
        src_ref=src,
        dst_ref=dst,
        send_sem=send_sem,
        recv_sem=recv_sem,
        device_id=device,
        device_id_type=MESH,
    )
    copy.start()
    return copy


def keep(src, dst, sem):
    copy = pltpu.make_async_copy(src, dst, sem)
    copy.start()
    return copy


def pipeline(plan, stages):
    lags = [LAG * k for k in range(len(stages))]
    return [
        functools.partial(stage, plan[t - lag])
        for t in range(len(plan) + lags[-1])
        for lag, stage in zip(lags, stages)
        if 0 <= t - lag < len(plan)
    ]


def run(steps):
    for step in steps:
        step()


def interleave(steps, work):
    done = 0
    for piece, count in work:
        piece()
        run(steps[done : done + count])
        done += count
    run(steps[done:])


class RowGather:
    def __init__(self, place, src, out, bounce, sems, rsems, lsem):
        self.place, self.src, self.out = place, src, out
        self.bounce, self.sems, self.rsems, self.lsem = bounce, sems, rsems, lsem

    def load(self):
        self.own = keep(self.src, self.bounce, self.lsem)

    def start(self):
        p = self.place
        slot = self.out.at[p.y, p.c]
        self.over_y = [
            push(self.src, slot, self.sems.at[d], self.rsems.at[d], p.at(y=p.next_y(d)))
            for d in range(1, p.Y)
        ]
        self.own.wait()
        self.own = keep(self.bounce, slot, self.lsem)

    def middle(self):
        p = self.place
        for copy in self.over_y:
            copy.wait_recv()
        self.own.wait()
        half = self.out.at[:, p.c]
        self.over_c = push(half, half, self.sems.at[0], self.rsems.at[0], p.at(c=1 - p.c))

    def end(self):
        for copy in self.over_y:
            copy.wait_send()
        self.over_c.wait()


def pieces(rows, width, which, classes):
    whole = []
    for j, name in enumerate(which):
        if name == "t":
            for k, kind in enumerate(classes["t"]):
                span = 2 * width // len(classes["t"])
                whole.append((j, 0, rows // 4, k * span, span, kind))
        elif name == "d":
            for k, kind in enumerate(classes["d"]):
                whole.append((j, k * rows, rows, 0, width, kind))
        else:
            for k, kind in enumerate(classes[name]):
                whole.append((j, 0, rows, k * width, width, kind))
    out = []
    for j, r0, rn, c0, cn, kind in whole:
        cuts = CUT if rn % (16 * CUT) == 0 else 1
        out += [(j, r0 + k * rn // cuts, rn // cuts, c0, cn, kind) for k in range(cuts)]
    return out


class WeightGather:
    def __init__(self, place, items, shards, outs, bounce, ssem, rsem, lsem):
        self.place = place
        self.shards, self.outs, self.bounce = shards, outs, bounce
        self.ssem, self.rsem, self.lsem = ssem, rsem, lsem
        self.plan = []
        for i, (w, r0, rn, c0, cn, kind) in enumerate(items):
            half = cn // CORES
            width = half // place.Y if kind == "D" else half
            first = c0 + place.c * half
            if kind == "D":
                first = first + place.y * width
            self.plan.append(
                dict(
                    i=i,
                    w=w,
                    kind=kind,
                    rows=pl.ds(r0, rn),
                    cols=pl.ds(pl.multiple_of(first, 128), width),
                    half=pl.ds(pl.multiple_of(c0 + place.c * half, 128), half),
                    held=bounce.at[i, pl.ds(0, rn), pl.ds(0, width)],
                )
            )

    def region(self, p, z, x, cols):
        return self.outs[p["w"]].at[z, x, p["rows"], cols]

    def load(self):
        for p in self.plan:
            p["own"] = keep(
                self.shards[p["w"]].at[p["rows"], p["cols"]], p["held"], self.lsem.at[p["i"]]
            )

    def store(self):
        place = self.place
        for p in self.plan:
            p["own"].wait()
            p["own"] = keep(
                p["held"], self.region(p, place.z, place.x, p["cols"]), self.lsem.at[p["i"]]
            )

    def post(self, p, slot, src, dst, device):
        return push(src, dst, self.ssem.at[p["i"], slot], self.rsem.at[p["i"], slot], device)

    def over_z(self, p):
        place = self.place
        src = self.shards[p["w"]].at[p["rows"], p["cols"]]
        dst = self.region(p, place.z, place.x, p["cols"])
        p["z"] = [
            self.post(p, d - 1, src, dst, place.at(z=place.next_z(d))) for d in range(1, place.Z)
        ]

    def over_x(self, p):
        place = self.place
        for copy in p["z"]:
            copy.wait_recv()
        p["own"].wait()
        part = self.region(p, pl.ds(0, place.Z), place.x, p["cols"])
        p["x"] = self.post(p, place.Z - 1, part, part, place.at(x=1 - place.x))

    def over_y(self, p):
        place = self.place
        p["x"].wait_recv()
        p["y"] = []
        if p["kind"] == "D":
            part = self.region(p, pl.ds(0, place.Z), pl.ds(0, XS), p["cols"])
            p["y"] = [
                self.post(p, place.Z - 1 + d, part, part, place.at(y=place.next_y(d)))
                for d in range(1, place.Y)
            ]

    def over_c(self, p):
        place = self.place
        for copy in p["y"]:
            copy.wait_recv()
        part = self.region(p, pl.ds(0, place.Z), pl.ds(0, XS), p["half"])
        p["c"] = self.post(p, place.Z - 1 + place.Y, part, part, place.at(c=1 - place.c))

    def finish(self, p):
        p["c"].wait()
        for copy in p["z"] + p["y"] + [p["x"]]:
            copy.wait_send()

    def stages(self):
        return [self.over_z, self.over_x, self.over_y, self.over_c, self.finish]


def gather_scratch(slices, shards, items):
    Y, Z = slices // CORES, shards // XS
    n, rows = len(items), max(item[2] for item in items)
    widest = max(cn // CORES // (Y if kind == "D" else 1) for _, _, _, _, cn, kind in items)
    return [pltpu.VMEM((n, rows, widest), BF), DMA((n, Z + Y)), DMA((n, Z + Y)), DMA((n,))]


def gathered_shapes(slices, shards, ws, rows_in):
    Y, Z = slices // CORES, shards // XS
    return [jax.ShapeDtypeStruct((Z, XS) + w.shape, w.dtype) for w in ws] + [
        jax.ShapeDtypeStruct((Y, CORES) + r.shape, r.dtype) for r in rows_in
    ]


def row_scratch(slices, rows_in):
    Y = slices // CORES
    out = []
    for r in rows_in:
        out += [pltpu.VMEM(r.shape, r.dtype), DMA((Y,)), DMA((Y,)), DMA((1,))]
    return out


def row_gathers(place, rows_in, rows_out, scratch):
    rows = []
    for k, (src, out) in enumerate(zip(rows_in, rows_out)):
        b, s, r, m = scratch[4 * k : 4 * k + 4]
        rows.append(RowGather(place, src, out, b, s, r, m.at[0]))
    return rows


def merged(fulls):
    return [g.reshape(-1, g.shape[-1]) for g in fulls]


def gather_body(slices, shards, items, nw, nr, *refs):
    ws, rows_in = refs[:nw], refs[nw : nw + nr]
    outs, rows_out = refs[nw + nr : 2 * nw + nr], refs[2 * nw + nr : 2 * (nw + nr)]
    scratch = refs[2 * (nw + nr) :]
    place = Place(slices, shards)
    gather = WeightGather(place, items, ws, outs, *scratch[:4])
    rows = row_gathers(place, rows_in, rows_out, scratch[4:])
    gather.load()
    for r in rows:
        r.load()
    greet(place)
    steps = pipeline(gather.plan, gather.stages())
    run(steps[:1])
    for r in rows:
        r.start()
    gather.store()
    run(steps[1:])
    for r in rows:
        r.middle()
    for r in rows:
        r.end()


def gather_weights(slices, shards, width, which, ws, rows_in, cid):
    rows = width // shards
    items = pieces(rows, width, which, GATHER_CLASS)
    nw, nr = len(ws), len(rows_in)
    out = pl.pallas_call(
        functools.partial(gather_body, slices, shards, items, nw, nr),
        out_shape=gathered_shapes(slices, shards, ws, rows_in),
        in_specs=[ANY] * (nw + nr),
        out_specs=[ANY] * (nw + nr),
        scratch_shapes=gather_scratch(slices, shards, items) + row_scratch(slices, rows_in),
        compiler_params=pltpu.CompilerParams(
            collective_id=cid, has_side_effects=True, vmem_limit_bytes=VMEM_ALL
        ),
    )(*ws, *rows_in)
    return merged(out[:nw]), [
        g.reshape((slices,) + r.shape) for g, r in zip(out[nw:], rows_in)
    ]


def add_into(dst, src, rn):
    lead = dst.shape[:-2]

    def step(k, _):
        idx, rest = [], k
        for size in reversed(lead[1:]):
            idx.append(lax.rem(rest, size))
            rest = lax.div(rest, size)
        idx = tuple(reversed(idx + [rest]))
        a, b = dst.at[idx], src.at[idx]
        rows = pl.ds(0, rn)
        a[rows, :] = (a[rows, :].astype(jnp.float32) + b[rows, :].astype(jnp.float32)).astype(BF)
        return 0

    lax.fori_loop(0, math.prod(lead), step, 0)


class GradSum:
    def __init__(self, place, items, grads, outs, acc, rc, ry, rx, rz, fin, rf, lsem, ssem, rsem):
        self.place, self.grads, self.outs = place, grads, outs
        self.acc, self.rc, self.ry, self.rx, self.rz = acc, rc, ry, rx, rz
        self.fin, self.rf = fin, rf
        self.lsem, self.ssem, self.rsem = lsem, ssem, rsem
        self.wide = acc.shape[-1]
        self.plan = []
        for i, (w, r0, rn, c0, cn, kind) in enumerate(items):
            p = dict(i=i, w=w, kind=kind, rn=rn, c0=c0, half=cn // CORES)
            p["k"] = sum(q["kind"] == kind for q in self.plan)
            p.update(rows=pl.ds(r0, rn), vr=pl.ds(0, rn), sends=[])
            self.plan.append(p)

    def post(self, p, slot, src, dst, device):
        copy = push(src, dst, self.ssem.at[p["i"], slot], self.rsem.at[p["i"], slot], device)
        p["sends"].append(copy)
        return copy

    def cols(self, p, core, part=None):
        first = p["c0"] + core * p["half"]
        if part is None:
            return pl.ds(pl.multiple_of(first, 128), p["half"])
        return pl.ds(pl.multiple_of(first + part * self.wide, 128), self.wide)

    def parts(self, p):
        return [self.place.y] if p["kind"] == "D" else list(range(self.place.Y))

    def over_c(self, p):
        place, i, vr = self.place, p["i"], p["vr"]
        g = self.grads[p["w"]]
        first = place.Z + place.Y + place.Y
        p["own"], p["c"] = [], []
        for part in range(place.Y):
            p["own"].append(
                keep(
                    g.at[:, :, p["rows"], self.cols(p, place.c, part)],
                    self.acc.at[i, part, :, :, vr, :],
                    self.lsem.at[i, part],
                )
            )
            p["c"].append(
                self.post(
                    p,
                    first + part,
                    g.at[:, :, p["rows"], self.cols(p, 1 - place.c, part)],
                    self.rc.at[i, part, :, :, vr, :],
                    place.at(c=1 - place.c),
                )
            )

    def over_y(self, p):
        place, i, vr = self.place, p["i"], p["vr"]
        for copy in p["own"]:
            copy.wait()
        for copy in p["c"]:
            copy.wait_recv()
        for part in range(place.Y):
            add_into(self.acc.at[i, part], self.rc.at[i, part], p["rn"])
        p["y"] = []
        if p["kind"] == "D":
            for d in range(1, place.Y):
                y = place.next_y(d)
                p["y"].append(
                    self.post(
                        p,
                        d,
                        self.acc.at[i, y, :, :, vr, :],
                        self.ry.at[p["k"], d - 1, :, :, vr, :],
                        place.at(y=y),
                    )
                )

    def over_x(self, p):
        place, i, vr = self.place, p["i"], p["vr"]
        for d, copy in enumerate(p["y"]):
            copy.wait_recv()
            add_into(self.acc.at[i, place.y], self.ry.at[p["k"], d], p["rn"])
        other = 1 - place.x
        if p["kind"] == "D":
            src, dst = self.acc.at[i, place.y, :, other, vr, :], self.rx.at[i, 0, :, vr, :]
        else:
            src, dst = self.acc.at[i, :, :, other, vr, :], self.rx.at[i, :, :, vr, :]
        p["x"] = self.post(p, place.Y, src, dst, place.at(x=other))

    def over_z(self, p):
        place, i, vr = self.place, p["i"], p["vr"]
        p["x"].wait_recv()
        for k, part in enumerate(self.parts(p)):
            add_into(self.acc.at[i, part, :, place.x], self.rx.at[i, k], p["rn"])
        p["z"] = []
        for d in range(1, place.Z):
            z = place.next_z(d)
            if p["kind"] == "D":
                src = self.acc.at[i, place.y, z, place.x, vr, :]
                dst = self.rz.at[i, d - 1, 0, vr, :]
            else:
                src = self.acc.at[i, :, z, place.x, vr, :]
                dst = self.rz.at[i, d - 1, :, vr, :]
            p["z"].append(self.post(p, place.Y + d, src, dst, place.at(z=z)))

    def region(self, p, core, part=None):
        return self.outs[p["w"]].at[p["rows"], self.cols(p, core, part)]

    def back_y(self, p):
        place, i, vr = self.place, p["i"], p["vr"]
        for copy in p["z"]:
            copy.wait_recv()
        for k, part in enumerate(self.parts(p)):
            total = self.acc[i, part, place.z, place.x, vr, :].astype(jnp.float32)
            for d in range(1, place.Z):
                total = total + self.rz[i, d - 1, k, vr, :].astype(jnp.float32)
            if p["kind"] == "D":
                self.fin[i, 0, vr, :] = total.astype(BF)
            else:
                self.rf[p["k"], place.y, part, vr, :] = total.astype(BF)
        first = place.Z + place.Y - 1
        p["f"], p["st"] = [], []
        if p["kind"] == "D":
            src, dst = self.fin.at[i, 0, vr, :], self.region(p, place.c, place.y)
            p["st"].append(keep(src, dst, self.lsem.at[i, 0]))
        else:
            src = dst = self.rf.at[p["k"], place.y, :, vr, :]
        for d in range(1, place.Y):
            p["f"].append(self.post(p, first + d, src, dst, place.at(y=place.next_y(d))))

    def back_c(self, p):
        place, i, vr = self.place, p["i"], p["vr"]
        for copy in p["f"]:
            copy.wait_recv()
        if p["kind"] == "C":
            for part in range(place.Y):
                total = self.rf[p["k"], 0, part, vr, :].astype(jnp.float32)
                for y in range(1, place.Y):
                    total = total + self.rf[p["k"], y, part, vr, :].astype(jnp.float32)
                self.fin[i, part, vr, :] = total.astype(BF)
                src, dst = self.fin.at[i, part, vr, :], self.region(p, place.c, part)
                p["st"].append(keep(src, dst, self.lsem.at[i, part]))
        for copy in p["st"]:
            copy.wait()
        part = self.region(p, place.c)
        p["e"] = self.post(p, 0, part, part, place.at(c=1 - place.c))

    def finish(self, p):
        p["e"].wait_recv()
        for copy in p["sends"]:
            copy.wait_send()

    def stages(self):
        return [
            self.over_c,
            self.over_y,
            self.over_x,
            self.over_z,
            self.back_y,
            self.back_c,
            self.finish,
        ]


def sum_scratch(slices, shards, items):
    Y, Z = slices // CORES, shards // XS
    n, wide = len(items), items[0][4] // CORES // Y
    rows = max(item[2] for item in items)
    nd = max(1, sum(item[5] == "D" for item in items))
    nc = max(1, n - nd)
    return [
        pltpu.VMEM((n, Y, Z, XS, rows, wide), BF),
        pltpu.VMEM((n, Y, Z, XS, rows, wide), BF),
        pltpu.VMEM((nd, Y - 1, Z, XS, rows, wide), BF),
        pltpu.VMEM((n, Y, Z, rows, wide), BF),
        pltpu.VMEM((n, Z - 1, Y, rows, wide), BF),
        pltpu.VMEM((n, Y, rows, wide), BF),
        pltpu.VMEM((nc, Y, Y, rows, wide), BF),
        DMA((n, Y)),
        DMA((n, Z + 3 * Y)),
        DMA((n, Z + 3 * Y)),
    ]


def sum_body(slices, shards, items, nw, *refs):
    place = Place(slices, shards)
    sums = GradSum(place, items, refs[:nw], refs[nw : 2 * nw], *refs[2 * nw :])
    greet(place)
    run(pipeline(sums.plan, sums.stages()))


def split_grads(shards, grads):
    return [g.reshape(shards // XS, XS, -1, g.shape[1]) for g in grads]


def sum_grads(slices, shards, width, which, grads, cid):
    rows = width // shards
    items = pieces(rows, width, which, SUM_CLASS)
    nw = len(grads)
    grads = split_grads(shards, grads)
    return pl.pallas_call(
        functools.partial(sum_body, slices, shards, items, nw),
        out_shape=[jax.ShapeDtypeStruct(g.shape[2:], BF) for g in grads],
        in_specs=[ANY] * nw,
        out_specs=[ANY] * nw,
        scratch_shapes=sum_scratch(slices, shards, items),
        compiler_params=pltpu.CompilerParams(
            collective_id=cid, has_side_effects=True, vmem_limit_bytes=VMEM_ALL
        ),
    )(*grads)


def dot(a, b, ca, cb):
    return lax.dot_general(a, b, (((ca,), (cb,)), ((), ())), preferred_element_type=jnp.float32)


def swap_halves(v):
    lane = lax.broadcasted_iota(jnp.int32, v.shape, 1)
    left = pltpu.roll(v, v.shape[1] - HD // 2, 1)
    right = pltpu.roll(v, HD // 2, 1)
    return jnp.where(lax.rem(lane, HD) < HD // 2, left, right)


def forward_block(qkv, seg_col, seg_row, mixed, logsum, h, rows):
    lanes = slice(h * HD, (h + 1) * HD)
    s = dot(qkv[1, :, lanes], qkv[0, rows, lanes], 1, 1) * (LOG2E * HD**-0.5)
    s = jnp.where(seg_col[...] == seg_row[:, rows], s, NEG)
    peak = jnp.max(s, axis=0, keepdims=True)
    expo = jnp.exp2(s - peak)
    total = jnp.sum(expo, axis=0, keepdims=True)
    out = dot(expo.astype(BF), qkv[2, :, lanes], 0, 0)
    mixed[rows, lanes] = (out / total.T).astype(BF)
    logsum[h : h + 1, rows] = peak + jnp.log2(total)


def backward_block(qkv, mixed, logsum, g, seg_col, seg_row, dk, dv, dq, h, rows, slot):
    lanes = slice(h * HD, (h + 1) * HD)
    side = slice(slot * HD, (slot + 1) * HD)
    q, gb = qkv[0, rows, lanes], g[rows, lanes]
    k, v = qkv[1, :, lanes], qkv[2, :, lanes]
    prod = gb.astype(jnp.float32) * mixed[rows, lanes].astype(jnp.float32)
    delta = jnp.sum(prod, axis=1, keepdims=True).T
    s = dot(k, q, 1, 1) * (LOG2E * HD**-0.5)
    same = seg_col[...] == seg_row[:, rows]
    probs = jnp.where(same, jnp.exp2(s - logsum[h : h + 1, rows]), 0.0)
    ds = (probs * (dot(v, gb, 1, 1) - delta)).astype(BF)
    dv[:, side] += dot(probs.astype(BF), gb, 1, 0)
    dk[:, side] += dot(ds, q, 1, 0)
    dq[rows, side] = dot(ds, k, 0, 0)


class Exchange:
    def __init__(self, place, ssem, rsem, lsem):
        self.place, self.ssem, self.rsem, self.lsem = place, ssem, rsem, lsem
        self.me = place.y * CORES + place.c
        self.peers = []
        for dy in list(range(1, place.Y)) + [0]:
            for dc in (range(CORES) if dy else (1,)):
                y, c = place.next_y(dy), lax.rem(place.c + dc, CORES)
                self.peers.append((dy * CORES + dc, y * CORES + c, place.at(y=y, c=c)))
        self.copies = {}

    def give(self, k, src, dst):
        slot, _, device = self.peers[k]
        self.copies[k] = push(src, dst, self.ssem.at[slot], self.rsem.at[slot], device)

    def mine(self, src, dst):
        self.own = keep(src, dst, self.lsem)

    def take(self):
        for copy in self.copies.values():
            copy.wait_recv()
        self.own.wait()

    def close(self):
        for copy in self.copies.values():
            copy.wait_send()


def span(index, size):
    return pl.ds(pl.multiple_of(index * size, size), size)


def forward_body(slices, shards, items, nw, *refs):
    ws, packed, seg_col, seg_row = refs[:nw], *refs[nw : nw + 3]
    outs = refs[nw + 3 : 2 * nw + 3]
    qkv, mixed_heads, logsum, mixed = refs[2 * nw + 3 : 2 * nw + 7]
    scratch = refs[2 * nw + 7 :]
    place = Place(slices, shards)
    rows, part = mixed.shape[0], mixed_heads.shape[1]
    gather = WeightGather(place, items, ws, outs, *scratch[:4])
    pairs = part // 128
    come, *backs = [
        Exchange(place, *[r.at[t] for r in scratch[4:7]]) for t in range(1 + pairs)
    ]
    me = come.me
    gather.load()
    come.mine(packed.at[:, :, span(me, part)], qkv.at[:, span(me, rows), :])
    greet(place, seq=True)
    for k, (_, peer, _) in enumerate(come.peers):
        come.give(k, packed.at[:, :, span(peer, part)], qkv.at[:, span(me, rows), :])
    steps = pipeline(gather.plan, gather.stages())
    run(steps[:1])
    gather.store()

    block = 256

    def attend(h):
        def step(i, _):
            forward_block(qkv, seg_col, seg_row, mixed_heads, logsum, h, span(i, block))
            return 0

        lax.fori_loop(0, seg_col.shape[0] // block, step, 0)

    def finish(t, k, owner):
        src = mixed_heads.at[span(owner, rows), t * 128 : (t + 1) * 128]
        first = pl.multiple_of(me * part + t * 128, 128)
        dst = mixed.at[:, pl.ds(first, 128)]
        if k < len(come.peers):
            backs[t].give(k, src, dst)
        else:
            backs[t].mine(src, dst)

    work = [(lambda: None, 16), (come.take, 0)]
    owners = [peer for _, peer, _ in come.peers] + [me]
    for t in range(pairs):
        work += [(functools.partial(attend, h), 8) for h in (2 * t, 2 * t + 1)]
        work += [(functools.partial(finish, t, k, owner), 0) for k, owner in enumerate(owners)]
    interleave(steps[1:], work)
    for back in backs:
        back.take()
    for ex in [come] + backs:
        ex.close()


def attention_forward(slices, shards, width, which, ws, packed, seg_col, seg_row, cid):
    rows = packed.shape[1]
    group, part = rows * slices, width // slices
    items = pieces(width // shards, width, which, GATHER_CLASS)
    nw = len(ws)
    out = pl.pallas_call(
        functools.partial(forward_body, slices, shards, items, nw),
        out_shape=gathered_shapes(slices, shards, ws, [])
        + [
            jax.ShapeDtypeStruct((3, group, part), BF),
            jax.ShapeDtypeStruct((group, part), BF),
            jax.ShapeDtypeStruct((part // HD, group), jnp.float32),
            jax.ShapeDtypeStruct((rows, width), BF),
        ],
        in_specs=[ANY] * (nw + 1) + [VM] * 2,
        out_specs=[ANY] * nw + [VM] * 4,
        scratch_shapes=gather_scratch(slices, shards, items)
        + [DMA((1 + part // 128, slices))] * 2
        + [DMA((1 + part // 128,))],
        compiler_params=pltpu.CompilerParams(
            collective_id=cid, has_side_effects=True, vmem_limit_bytes=VMEM_ALL
        ),
    )(*ws, packed, seg_col, seg_row)
    return merged(out[:nw]), out[nw:]


def backward_body(slices, shards, items, nw, nr, *refs):
    grads, rows_in = refs[:nw], refs[nw : nw + nr]
    at = nw + nr
    d_mixed, qkv, mixed, logsum, seg_col, seg_row, cos, sin = refs[at : at + 8]
    at += 8
    sums_out, rows_out, out = refs[at : at + nw], refs[at + nw : at + nw + nr], refs[at + nw + nr]
    scratch = refs[at + nw + nr + 1 :]
    place = Place(slices, shards)
    sums = GradSum(place, items, grads, sums_out, *scratch[:10])
    gathers = row_gathers(place, rows_in, rows_out, scratch[10:])
    g, dk, dv, dq, turned, ssem, rsem, lsem = scratch[10 + 4 * nr :]
    rows, part = d_mixed.shape[0], g.shape[1]
    pairs = part // 128
    come = Exchange(place, ssem.at[0], rsem.at[0], lsem.at[0])
    backs = [
        Exchange(place, ssem.at[1 + t], rsem.at[1 + t], lsem.at[1 + t]) for t in range(pairs)
    ]
    me = come.me
    come.mine(d_mixed.at[:, span(me, part)], g.at[span(me, rows), :])
    for r in gathers:
        r.load()
    greet(place, seq=True)
    for k, (_, peer, _) in enumerate(come.peers):
        come.give(k, d_mixed.at[:, span(peer, part)], g.at[span(me, rows), :])
    block = 256

    def attend(h):
        if h % 2 == 0:
            dk[...] = jnp.zeros_like(dk)
            dv[...] = jnp.zeros_like(dv)

        def step(i, _):
            backward_block(
                qkv, mixed, logsum, g, seg_col, seg_row, dk, dv, dq, h, span(i, block), h % 2
            )
            return 0

        lax.fori_loop(0, seg_col.shape[0] // block, step, 0)

    def finish(t, k, owner):
        own = span(owner, rows)
        c, s = cos[own, :], sin[own, :]
        for j, d in enumerate((dq, dk)):
            v = d[own, :] * (HD**-0.5)
            turned[t, j, own, :] = (v * c - swap_halves(v) * s).astype(BF)
        turned[t, 2, own, :] = dv[own, :].astype(BF)
        first = pl.multiple_of(me * part + t * 128, 128)
        src, dst = turned.at[t, :, own, :], out.at[:, :, pl.ds(first, 128)]
        if k < len(come.peers):
            backs[t].give(k, src, dst)
        else:
            backs[t].mine(src, dst)

    work = [(lambda: None, 10), (come.take, 0)] + [(r.start, 0) for r in gathers]
    owners = [peer for _, peer, _ in come.peers] + [me]
    for t in range(pairs):
        work += [(functools.partial(attend, h), 10) for h in (2 * t, 2 * t + 1)]
        work += [(functools.partial(finish, t, k, owner), 0) for k, owner in enumerate(owners)]
    steps = pipeline(sums.plan, sums.stages())
    interleave(steps, work)
    for r in gathers:
        r.middle()
    for back in backs:
        back.take()
    for r in gathers:
        r.end()
    for ex in [come] + backs:
        ex.close()


def attention_backward(
    slices, shards, width, which, grads, rows_in, d_mixed, kept, seg_col, seg_row, cos, sin, cid
):
    rows = d_mixed.shape[0]
    group, part = rows * slices, width // slices
    items = pieces(width // shards, width, which, SUM_CLASS)
    nw, nr, pairs = len(grads), len(rows_in), part // 128
    grads = split_grads(shards, grads)
    total = pltpu.VMEM((group, 128), jnp.float32)
    out = pl.pallas_call(
        functools.partial(backward_body, slices, shards, items, nw, nr),
        out_shape=[jax.ShapeDtypeStruct(w.shape[2:], BF) for w in grads]
        + gathered_shapes(slices, shards, [], rows_in)
        + [jax.ShapeDtypeStruct((3, rows, width), BF)],
        in_specs=[ANY] * (nw + nr + 1) + [VM] * 7,
        out_specs=[ANY] * (nw + nr) + [VM],
        scratch_shapes=sum_scratch(slices, shards, items)
        + row_scratch(slices, rows_in)
        + [pltpu.VMEM((group, part), BF), total, total, total]
        + [pltpu.VMEM((pairs, 3, group, 128), BF)]
        + [DMA((1 + pairs, slices)), DMA((1 + pairs, slices)), DMA((1 + pairs,))],
        compiler_params=pltpu.CompilerParams(
            collective_id=cid, has_side_effects=True, vmem_limit_bytes=VMEM_ALL
        ),
    )(*grads, *rows_in, d_mixed, *kept, seg_col, seg_row, cos, sin)
    full = [g.reshape((slices,) + r.shape) for g, r in zip(out[nw:], rows_in)]
    return out[:nw], full, out[nw + nr]


def project_body(h, w, cos, sin, out):
    y = jnp.dot(h[...], w[...], preferred_element_type=jnp.float32)
    turned = (pl.program_id(0) < 2).astype(jnp.float32)
    c = cos[...] * turned + (1.0 - turned)
    s = sin[...] * turned
    for t in range(y.shape[1] // 128):
        w_ = slice(t * 128, (t + 1) * 128)
        out[0, :, w_] = (y[:, w_] * c + swap_halves(y[:, w_]) * s).astype(BF)


def project(h, w, cos, sin, block=512):
    rows, width = h.shape
    const = lambda j, n: (0, 0)
    per = width // block
    return pl.pallas_call(
        project_body,
        grid=(3, per),
        out_shape=jax.ShapeDtypeStruct((3, rows, width), BF),
        in_specs=[
            pl.BlockSpec((rows, width), const),
            pl.BlockSpec((width, block), lambda j, n: (0, j * per + n)),
            pl.BlockSpec((rows, 128), const),
            pl.BlockSpec((rows, 128), const),
        ],
        out_specs=pl.BlockSpec((1, rows, block), lambda j, n: (j, 0, n)),
        compiler_params=pltpu.CompilerParams(vmem_limit_bytes=VMEM_ALL),
    )(h, w, cos, sin)


def time_embedding(steps):
    half = TEMB // 2
    freqs = jnp.exp(-math.log(BASE) * jnp.arange(half, dtype=jnp.float32) / half)
    angles = steps.astype(jnp.float32)[:, None] * freqs[None, :]
    return jnp.concatenate([jnp.sin(angles), jnp.cos(angles)], axis=-1)


def layout(lens, places):
    ends = jnp.cumsum(lens)
    starts = ends - lens
    member = (places[:, None] >= starts[None, :]) & (places[:, None] < ends[None, :])
    labels = jnp.arange(NSEQ, dtype=jnp.int32)
    segment = jnp.sum(jnp.where(member, labels[None, :], 0), axis=1)
    offset = places - jnp.sum(jnp.where(member, starts[None, :], 0), axis=1)
    return (member.astype(jnp.float32), segment, offset)


def turn_tables(offset):
    half = HD // 2
    freqs = jnp.exp(-math.log(BASE) * jnp.arange(half, dtype=jnp.float32) * 2.0 / HD)
    angles = offset.astype(jnp.float32)[:, None] * freqs[None, :]
    c, s = jnp.cos(angles), jnp.sin(angles)
    return jnp.concatenate([c] * 4, axis=1), jnp.concatenate([-s, s, -s, s], axis=1)


def norm_mod(values, scale):
    centre = jnp.mean(values, axis=-1, keepdims=True)
    centred = values - centre
    spread = jnp.mean(centred * centred, axis=-1, keepdims=True)
    return centred * lax.rsqrt(spread + EPS) * (1.0 + scale)


def pick_rows(data, wanted, labels):
    pick = (wanted[:, None] == labels[None, :]).astype(BF)
    return jnp.dot(pick, data.reshape(-1, data.shape[-1]), preferred_element_type=jnp.float32)


def on_device(tokens, lengths, time_steps, order, w_time, w_qkv, w_out, w_up, w_down, cotangent):
    rows, width = tokens.shape[1:]
    slices, shards = lax.axis_size("seq"), lax.axis_size("fsdp")
    group = rows * slices
    lens, places = lengths[0], order[0]
    (f_time, f_qkv), (order_all, cot_all) = gather_weights(
        slices, shards, width, "tq", [w_time, w_qkv], [order, cotangent[0]], 0
    )
    order_all = order_all.reshape(group)

    member, _, offset = layout(lens, places)
    _, segment_all, offset_all = layout(lens, order_all)
    seg_col, seg_row = segment_all[:, None], segment_all[None, :]
    emb = time_embedding(time_steps[0]).astype(BF)
    scales_seq = jnp.dot(emb, f_time, preferred_element_type=jnp.float32)
    scales = jnp.dot(member, scales_seq, precision=lax.Precision.HIGHEST)
    scale_one, scale_two = scales[:, :width], scales[:, width:]
    inputs = tokens[0].astype(jnp.float32)
    normed_one, pull_one = jax.vjp(norm_mod, inputs, scale_one)
    h_one = normed_one.astype(BF)

    cos, sin = turn_tables(offset)
    packed = project(h_one, f_qkv, cos, sin)
    (f_out, f_up, f_down), (heads_qkv, mixed_heads, logsum, mixed) = attention_forward(
        slices, shards, width, "oud", [w_out, w_up, w_down], packed, seg_col, seg_row, 1
    )

    x_two = inputs + jnp.dot(mixed, f_out, preferred_element_type=jnp.float32)
    normed_two, pull_two = jax.vjp(norm_mod, x_two, scale_two)
    h_two = normed_two.astype(BF)
    up = jnp.dot(h_two, f_up, preferred_element_type=jnp.float32)
    activated, pull_gelu = jax.vjp(jax.nn.gelu, up)
    hidden = activated.astype(BF)
    result = (x_two + jnp.dot(hidden, f_down, preferred_element_type=jnp.float32)).astype(BF)

    d_result = pick_rows(cot_all, places, jnp.arange(group, dtype=jnp.int32))
    d_low = d_result.astype(BF)
    grad_down = dot(hidden, d_low, 0, 0).astype(BF)
    d_up = pull_gelu(dot(d_low, f_down, 1, 1))[0].astype(BF)
    grad_up = dot(h_two, d_up, 0, 0).astype(BF)
    d_xpart, d_scale_two = pull_two(dot(d_up, f_up, 1, 1))
    d_xtwo = d_result + d_xpart
    d_attn = d_xtwo.astype(BF)
    grad_out = dot(mixed, d_attn, 0, 0).astype(BF)
    d_mixed = dot(d_attn, f_out, 1, 1).astype(BF)

    cos_all, sin_all = turn_tables(offset_all)
    sums, (result_all,), d_packed = attention_backward(
        slices,
        shards,
        width,
        "duo",
        [grad_down, grad_up, grad_out],
        [result],
        d_mixed,
        (heads_qkv, mixed_heads, logsum),
        seg_col,
        seg_row,
        cos_all,
        sin_all,
        2,
    )
    d_qkv = d_packed.transpose(1, 0, 2).reshape(rows, 3 * width)
    grad_qkv = dot(h_one, d_qkv, 0, 0).astype(BF)
    d_xone, d_scale_one = pull_one(dot(d_qkv, f_qkv, 1, 1))
    input_grad = d_xtwo + d_xone
    d_scales = lax.dot_general(
        member,
        jnp.concatenate([d_scale_one, d_scale_two], axis=1),
        (((0,), (0,)), ((), ())),
        precision=lax.Precision.HIGHEST,
        preferred_element_type=jnp.float32,
    )
    grad_time = lax.dot_general(
        emb.astype(jnp.float32),
        d_scales,
        (((0,), (0,)), ((), ())),
        precision=lax.Precision.HIGHEST,
        preferred_element_type=jnp.float32,
    ).astype(BF)

    sums = sums + sum_grads(slices, shards, width, "qt", [grad_qkv, grad_time], 3)
    s_down, s_up, s_out, s_qkv, s_time = [g.astype(jnp.float32) for g in sums]
    mine = lax.axis_index("seq") * rows + jnp.arange(rows, dtype=jnp.int32)
    output = pick_rows(result_all, mine, order_all).astype(BF)
    return (output[None], input_grad[None], s_time, s_qkv, s_out, s_up, s_down)


def solution(mesh):
    row, tok, mat = P("fsdp", None), P("fsdp", "seq", None), P("fsdp", None)
    return jax.shard_map(
        on_device,
        mesh=mesh,
        in_specs=(tok, row, row, P("fsdp", "seq"), mat, mat, mat, mat, mat, tok),
        out_specs=(tok, tok, mat, mat, mat, mat, mat),
        check_vma=False,
    )
```

```python
import functools
import math

import jax
import jax.numpy as jnp
from jax import lax
from jax.experimental import pallas as pl
from jax.experimental.pallas import tpu as pltpu
from jax.sharding import PartitionSpec as P

H = 16
HD = 64
TEMB = 256
NSEQ = 3

EPS = 1e-05
NEG = -1e30
BASE = 10000.0
LOG2E = math.log2(math.e)
CORES = 2
XS = 2
BF = jnp.bfloat16

ANY = pl.BlockSpec(memory_space=pl.ANY)
VM = pl.BlockSpec(memory_space=pltpu.VMEM)
DMA = pltpu.SemaphoreType.DMA
MESH = pl.DeviceIdType.MESH
VMEM_ALL = 67043328
CUT = 2
LAG = 2

GATHER_CLASS = {"t": "D", "q": "CDC", "o": "C", "u": "DCDC", "d": "DCDC"}
SUM_CLASS = {"t": "DD", "q": "CDC", "o": "C", "u": "CCDC", "d": "DCDC"}


class Place:
    def __init__(self, slices, shards):
        self.Y, self.Z = slices // CORES, shards // XS
        seq, fsdp = lax.axis_index("seq"), lax.axis_index("fsdp")
        self.y, self.c = lax.div(seq, CORES), lax.rem(seq, CORES)
        self.z, self.x = lax.div(fsdp, XS), lax.rem(fsdp, XS)

    def at(self, z=None, x=None, y=None, c=None):
        z = self.z if z is None else z
        x = self.x if x is None else x
        y = self.y if y is None else y
        c = self.c if c is None else c
        return {"seq": y * CORES + c, "fsdp": z * XS + x}

    def next_y(self, d):
        return lax.rem(self.y + d, self.Y)

    def next_z(self, d):
        return lax.rem(self.z + d, self.Z)


def greet(place, seq=False):
    barrier = pltpu.get_barrier_semaphore()
    others = [place.at(c=1 - place.c), place.at(x=1 - place.x)]
    others += [place.at(y=place.next_y(d)) for d in range(1, place.Y)]
    others += [place.at(z=place.next_z(d)) for d in range(1, place.Z)]
    if seq:
        others += [place.at(y=place.next_y(d), c=1 - place.c) for d in range(1, place.Y)]
    for other in others:
        pl.semaphore_signal(barrier, inc=1, device_id=other, device_id_type=MESH)
    pl.semaphore_wait(barrier, len(others))


def push(src, dst, send_sem, recv_sem, device):
    copy = pltpu.make_async_remote_copy(
        src_ref=src,
        dst_ref=dst,
        send_sem=send_sem,
        recv_sem=recv_sem,
        device_id=device,
        device_id_type=MESH,
    )
    copy.start()
    return copy


def keep(src, dst, sem):
    copy = pltpu.make_async_copy(src, dst, sem)
    copy.start()
    return copy


def pipeline(plan, stages):
    lags = [LAG * k for k in range(len(stages))]
    return [
        functools.partial(stage, plan[t - lag])
        for t in range(len(plan) + lags[-1])
        for lag, stage in zip(lags, stages)
        if 0 <= t - lag < len(plan)
    ]


def run(steps):
    for step in steps:
        step()


def interleave(steps, work):
    done = 0
    for piece, count in work:
        piece()
        run(steps[done : done + count])
        done += count
    run(steps[done:])


class RowGather:
    def __init__(self, place, src, out, bounce, sems, rsems, lsem):
        self.place, self.src, self.out = place, src, out
        self.bounce, self.sems, self.rsems, self.lsem = bounce, sems, rsems, lsem

    def load(self):
        self.own = keep(self.src, self.bounce, self.lsem)

    def start(self):
        p = self.place
        slot = self.out.at[p.y, p.c]
        self.over_y = [
            push(self.src, slot, self.sems.at[d], self.rsems.at[d], p.at(y=p.next_y(d)))
            for d in range(1, p.Y)
        ]
        self.own.wait()
        self.own = keep(self.bounce, slot, self.lsem)

    def middle(self):
        p = self.place
        for copy in self.over_y:
            copy.wait_recv()
        self.own.wait()
        half = self.out.at[:, p.c]
        self.over_c = push(half, half, self.sems.at[0], self.rsems.at[0], p.at(c=1 - p.c))

    def end(self):
        for copy in self.over_y:
            copy.wait_send()
        self.over_c.wait()


def pieces(rows, width, which, classes):
    whole = []
    for j, name in enumerate(which):
        if name == "t":
            for k, kind in enumerate(classes["t"]):
                span = 2 * width // len(classes["t"])
                whole.append((j, 0, rows // 4, k * span, span, kind))
        elif name == "d":
            for k, kind in enumerate(classes["d"]):
                whole.append((j, k * rows, rows, 0, width, kind))
        else:
            for k, kind in enumerate(classes[name]):
                whole.append((j, 0, rows, k * width, width, kind))
    out = []
    for j, r0, rn, c0, cn, kind in whole:
        cuts = CUT if rn % (16 * CUT) == 0 else 1
        out += [(j, r0 + k * rn // cuts, rn // cuts, c0, cn, kind) for k in range(cuts)]
    return out


class WeightGather:
    def __init__(self, place, items, shards, outs, bounce, ssem, rsem, lsem):
        self.place = place
        self.shards, self.outs, self.bounce = shards, outs, bounce
        self.ssem, self.rsem, self.lsem = ssem, rsem, lsem
        self.plan = []
        for i, (w, r0, rn, c0, cn, kind) in enumerate(items):
            half = cn // CORES
            width = half // place.Y if kind == "D" else half
            first = c0 + place.c * half
            if kind == "D":
                first = first + place.y * width
            self.plan.append(
                dict(
                    i=i,
                    w=w,
                    kind=kind,
                    first=c0,
                    rows=pl.ds(r0, rn),
                    cols=pl.ds(pl.multiple_of(first, 128), width),
                    half=pl.ds(pl.multiple_of(c0 + place.c * half, 128), half),
                    held=bounce.at[i, pl.ds(0, rn), pl.ds(0, width)],
                )
            )

    def region(self, p, z, x, cols):
        return self.outs[p["w"]].at[z, x, p["rows"], cols]

    def load(self):
        for p in self.plan:
            p["own"] = keep(
                self.shards[p["w"]].at[p["rows"], p["cols"]], p["held"], self.lsem.at[p["i"]]
            )

    def store(self):
        place = self.place
        for p in self.plan:
            p["own"].wait()
            p["own"] = keep(
                p["held"], self.region(p, place.z, place.x, p["cols"]), self.lsem.at[p["i"]]
            )

    def post(self, p, slot, src, dst, device):
        return push(src, dst, self.ssem.at[p["i"], slot], self.rsem.at[p["i"], slot], device)

    def over_z(self, p):
        place = self.place
        src = self.shards[p["w"]].at[p["rows"], p["cols"]]
        dst = self.region(p, place.z, place.x, p["cols"])
        p["z"] = [
            self.post(p, d - 1, src, dst, place.at(z=place.next_z(d))) for d in range(1, place.Z)
        ]

    def over_x(self, p):
        place = self.place
        for copy in p["z"]:
            copy.wait_recv()
        p["own"].wait()
        part = self.region(p, pl.ds(0, place.Z), place.x, p["cols"])
        p["x"] = self.post(p, place.Z - 1, part, part, place.at(x=1 - place.x))

    def over_y(self, p):
        place = self.place
        p["x"].wait_recv()
        p["y"] = []
        if p["kind"] == "D":
            part = self.region(p, pl.ds(0, place.Z), pl.ds(0, XS), p["cols"])
            p["y"] = [
                self.post(p, place.Z - 1 + d, part, part, place.at(y=place.next_y(d)))
                for d in range(1, place.Y)
            ]

    def over_c(self, p):
        place = self.place
        for copy in p["y"]:
            copy.wait_recv()
        part = self.region(p, pl.ds(0, place.Z), pl.ds(0, XS), p["half"])
        p["c"] = self.post(p, place.Z - 1 + place.Y, part, part, place.at(c=1 - place.c))

    def finish(self, p):
        p["c"].wait()
        for copy in p["z"] + p["y"] + [p["x"]]:
            copy.wait_send()

    def stages(self):
        return [self.over_z, self.over_x, self.over_y, self.over_c, self.finish]


def gather_scratch(slices, shards, items):
    Y, Z = slices // CORES, shards // XS
    n, rows = len(items), max(item[2] for item in items)
    widest = max(cn // CORES // (Y if kind == "D" else 1) for _, _, _, _, cn, kind in items)
    return [pltpu.VMEM((n, rows, widest), BF), DMA((n, Z + Y)), DMA((n, Z + Y)), DMA((n,))]


def gathered_shapes(slices, shards, ws, rows_in):
    Y, Z = slices // CORES, shards // XS
    return [jax.ShapeDtypeStruct((Z, XS) + w.shape, w.dtype) for w in ws] + [
        jax.ShapeDtypeStruct((Y, CORES) + r.shape, r.dtype) for r in rows_in
    ]


def row_scratch(slices, rows_in):
    Y = slices // CORES
    out = []
    for r in rows_in:
        out += [pltpu.VMEM(r.shape, r.dtype), DMA((Y,)), DMA((Y,)), DMA((1,))]
    return out


def row_gathers(place, rows_in, rows_out, scratch):
    rows = []
    for k, (src, out) in enumerate(zip(rows_in, rows_out)):
        b, s, r, m = scratch[4 * k : 4 * k + 4]
        rows.append(RowGather(place, src, out, b, s, r, m.at[0]))
    return rows


def merged(fulls):
    return [g.reshape(-1, g.shape[-1]) for g in fulls]


def add_into(dst, src, rn):
    lead = dst.shape[:-2]

    def step(k, _):
        idx, rest = [], k
        for size in reversed(lead[1:]):
            idx.append(lax.rem(rest, size))
            rest = lax.div(rest, size)
        idx = tuple(reversed(idx + [rest]))
        a, b = dst.at[idx], src.at[idx]
        rows = pl.ds(0, rn)
        a[rows, :] = (a[rows, :].astype(jnp.float32) + b[rows, :].astype(jnp.float32)).astype(BF)
        return 0

    lax.fori_loop(0, math.prod(lead), step, 0)


class GradSum:
    def __init__(self, place, items, grads, outs, acc, rc, ry, rx, rz, fin, rf, lsem, ssem, rsem):
        self.place, self.grads, self.outs = place, grads, outs
        self.acc, self.rc, self.ry, self.rx, self.rz = acc, rc, ry, rx, rz
        self.fin, self.rf = fin, rf
        self.lsem, self.ssem, self.rsem = lsem, ssem, rsem
        self.wide = acc.shape[-1]
        self.plan = []
        for i, (w, r0, rn, c0, cn, kind) in enumerate(items):
            p = dict(i=i, w=w, kind=kind, rn=rn, c0=c0, half=cn // CORES)
            p["k"] = sum(q["kind"] == kind for q in self.plan)
            p.update(rows=pl.ds(r0, rn), vr=pl.ds(0, rn), sends=[])
            self.plan.append(p)

    def post(self, p, slot, src, dst, device):
        copy = push(src, dst, self.ssem.at[p["i"], slot], self.rsem.at[p["i"], slot], device)
        p["sends"].append(copy)
        return copy

    def cols(self, p, core, part=None):
        first = p["c0"] + core * p["half"]
        if part is None:
            return pl.ds(pl.multiple_of(first, 128), p["half"])
        return pl.ds(pl.multiple_of(first + part * self.wide, 128), self.wide)

    def parts(self, p):
        return [self.place.y] if p["kind"] == "D" else list(range(self.place.Y))

    def over_c(self, p):
        place, i, vr = self.place, p["i"], p["vr"]
        g = self.grads[p["w"]]
        first = place.Z + place.Y + place.Y
        p["own"], p["c"] = [], []
        for part in range(place.Y):
            p["own"].append(
                keep(
                    g.at[:, :, p["rows"], self.cols(p, place.c, part)],
                    self.acc.at[i, part, :, :, vr, :],
                    self.lsem.at[i, part],
                )
            )
            p["c"].append(
                self.post(
                    p,
                    first + part,
                    g.at[:, :, p["rows"], self.cols(p, 1 - place.c, part)],
                    self.rc.at[i, part, :, :, vr, :],
                    place.at(c=1 - place.c),
                )
            )

    def over_y(self, p):
        place, i, vr = self.place, p["i"], p["vr"]
        for copy in p["own"]:
            copy.wait()
        for copy in p["c"]:
            copy.wait_recv()
        for part in range(place.Y):
            add_into(self.acc.at[i, part], self.rc.at[i, part], p["rn"])
        p["y"] = []
        if p["kind"] == "D":
            for d in range(1, place.Y):
                y = place.next_y(d)
                p["y"].append(
                    self.post(
                        p,
                        d,
                        self.acc.at[i, y, :, :, vr, :],
                        self.ry.at[p["k"], d - 1, :, :, vr, :],
                        place.at(y=y),
                    )
                )

    def over_x(self, p):
        place, i, vr = self.place, p["i"], p["vr"]
        for d, copy in enumerate(p["y"]):
            copy.wait_recv()
            add_into(self.acc.at[i, place.y], self.ry.at[p["k"], d], p["rn"])
        other = 1 - place.x
        if p["kind"] == "D":
            src, dst = self.acc.at[i, place.y, :, other, vr, :], self.rx.at[i, 0, :, vr, :]
        else:
            src, dst = self.acc.at[i, :, :, other, vr, :], self.rx.at[i, :, :, vr, :]
        p["x"] = self.post(p, place.Y, src, dst, place.at(x=other))

    def over_z(self, p):
        place, i, vr = self.place, p["i"], p["vr"]
        p["x"].wait_recv()
        for k, part in enumerate(self.parts(p)):
            add_into(self.acc.at[i, part, :, place.x], self.rx.at[i, k], p["rn"])
        p["z"] = []
        for d in range(1, place.Z):
            z = place.next_z(d)
            if p["kind"] == "D":
                src = self.acc.at[i, place.y, z, place.x, vr, :]
                dst = self.rz.at[i, d - 1, 0, vr, :]
            else:
                src = self.acc.at[i, :, z, place.x, vr, :]
                dst = self.rz.at[i, d - 1, :, vr, :]
            p["z"].append(self.post(p, place.Y + d, src, dst, place.at(z=z)))

    def region(self, p, core, part=None):
        return self.outs[p["w"]].at[p["rows"], self.cols(p, core, part)]

    def back_y(self, p):
        place, i, vr = self.place, p["i"], p["vr"]
        for copy in p["z"]:
            copy.wait_recv()
        for k, part in enumerate(self.parts(p)):
            total = self.acc[i, part, place.z, place.x, vr, :].astype(jnp.float32)
            for d in range(1, place.Z):
                total = total + self.rz[i, d - 1, k, vr, :].astype(jnp.float32)
            if p["kind"] == "D":
                self.fin[i, 0, vr, :] = total.astype(BF)
            else:
                self.rf[p["k"], place.y, part, vr, :] = total.astype(BF)
        first = place.Z + place.Y - 1
        p["f"], p["st"] = [], []
        if p["kind"] == "D":
            src, dst = self.fin.at[i, 0, vr, :], self.region(p, place.c, place.y)
            p["st"].append(keep(src, dst, self.lsem.at[i, 0]))
        else:
            src = dst = self.rf.at[p["k"], place.y, :, vr, :]
        for d in range(1, place.Y):
            p["f"].append(self.post(p, first + d, src, dst, place.at(y=place.next_y(d))))

    def back_c(self, p):
        place, i, vr = self.place, p["i"], p["vr"]
        for copy in p["f"]:
            copy.wait_recv()
        if p["kind"] == "C":
            for part in range(place.Y):
                total = self.rf[p["k"], 0, part, vr, :].astype(jnp.float32)
                for y in range(1, place.Y):
                    total = total + self.rf[p["k"], y, part, vr, :].astype(jnp.float32)
                self.fin[i, part, vr, :] = total.astype(BF)
                src, dst = self.fin.at[i, part, vr, :], self.region(p, place.c, part)
                p["st"].append(keep(src, dst, self.lsem.at[i, part]))
        for copy in p["st"]:
            copy.wait()
        part = self.region(p, place.c)
        p["e"] = self.post(p, 0, part, part, place.at(c=1 - place.c))

    def finish(self, p):
        p["e"].wait_recv()
        for copy in p["sends"]:
            copy.wait_send()

    def stages(self):
        return [
            self.over_c,
            self.over_y,
            self.over_x,
            self.over_z,
            self.back_y,
            self.back_c,
            self.finish,
        ]


def sum_scratch(slices, shards, items):
    Y, Z = slices // CORES, shards // XS
    n, wide = len(items), items[0][4] // CORES // Y
    rows = max(item[2] for item in items)
    nd = max(1, sum(item[5] == "D" for item in items))
    nc = max(1, n - nd)
    return [
        pltpu.VMEM((n, Y, Z, XS, rows, wide), BF),
        pltpu.VMEM((n, Y, Z, XS, rows, wide), BF),
        pltpu.VMEM((nd, Y - 1, Z, XS, rows, wide), BF),
        pltpu.VMEM((n, Y, Z, rows, wide), BF),
        pltpu.VMEM((n, Z - 1, Y, rows, wide), BF),
        pltpu.VMEM((n, Y, rows, wide), BF),
        pltpu.VMEM((nc, Y, Y, rows, wide), BF),
        DMA((n, Y)),
        DMA((n, Z + 3 * Y)),
        DMA((n, Z + 3 * Y)),
    ]


def sum_body(slices, shards, items, nw, *refs):
    place = Place(slices, shards)
    sums = GradSum(place, items, refs[:nw], refs[nw : 2 * nw], *refs[2 * nw :])
    greet(place)
    run(pipeline(sums.plan, sums.stages()))


def split_grads(shards, grads):
    return [g.reshape(shards // XS, XS, -1, g.shape[1]) for g in grads]


def sum_grads(slices, shards, width, which, grads, cid):
    rows = width // shards
    items = pieces(rows, width, which, SUM_CLASS)
    nw = len(grads)
    grads = split_grads(shards, grads)
    return pl.pallas_call(
        functools.partial(sum_body, slices, shards, items, nw),
        out_shape=[jax.ShapeDtypeStruct(g.shape[2:], BF) for g in grads],
        in_specs=[ANY] * nw,
        out_specs=[ANY] * nw,
        scratch_shapes=sum_scratch(slices, shards, items),
        compiler_params=pltpu.CompilerParams(
            collective_id=cid, has_side_effects=True, vmem_limit_bytes=VMEM_ALL
        ),
    )(*grads)


def dot(a, b, ca, cb):
    return lax.dot_general(a, b, (((ca,), (cb,)), ((), ())), preferred_element_type=jnp.float32)


def swap_halves(v):
    lane = lax.broadcasted_iota(jnp.int32, v.shape, 1)
    left = pltpu.roll(v, v.shape[1] - HD // 2, 1)
    right = pltpu.roll(v, HD // 2, 1)
    return jnp.where(lax.rem(lane, HD) < HD // 2, left, right)


def forward_block(qkv, seg_col, seg_row, mixed, logsum, h, rows):
    lanes = slice(h * HD, (h + 1) * HD)
    s = dot(qkv[1, :, lanes], qkv[0, rows, lanes], 1, 1) * (LOG2E * HD**-0.5)
    s = jnp.where(seg_col[...] == seg_row[:, rows], s, NEG)
    peak = jnp.max(s, axis=0, keepdims=True)
    expo = jnp.exp2(s - peak)
    total = jnp.sum(expo, axis=0, keepdims=True)
    out = dot(expo.astype(BF), qkv[2, :, lanes], 0, 0)
    mixed[rows, lanes] = (out / total.T).astype(BF)
    logsum[h : h + 1, rows] = peak + jnp.log2(total)


def backward_block(qkv, mixed, logsum, g, seg_col, seg_row, dk, dv, dq, h, rows, slot):
    lanes = slice(h * HD, (h + 1) * HD)
    side = slice(slot * HD, (slot + 1) * HD)
    q, gb = qkv[0, rows, lanes], g[rows, lanes]
    k, v = qkv[1, :, lanes], qkv[2, :, lanes]
    prod = gb.astype(jnp.float32) * mixed[rows, lanes].astype(jnp.float32)
    delta = jnp.sum(prod, axis=1, keepdims=True).T
    s = dot(k, q, 1, 1) * (LOG2E * HD**-0.5)
    same = seg_col[...] == seg_row[:, rows]
    probs = jnp.where(same, jnp.exp2(s - logsum[h : h + 1, rows]), 0.0)
    ds = (probs * (dot(v, gb, 1, 1) - delta)).astype(BF)
    dv[:, side] += dot(probs.astype(BF), gb, 1, 0)
    dk[:, side] += dot(ds, q, 1, 0)
    dq[rows, side] = dot(ds, k, 0, 0)


class Exchange:
    def __init__(self, place, ssem, rsem, lsem):
        self.place, self.ssem, self.rsem, self.lsem = place, ssem, rsem, lsem
        self.me = place.y * CORES + place.c
        self.peers = []
        for dy in list(range(1, place.Y)) + [0]:
            for dc in (range(CORES) if dy else (1,)):
                y, c = place.next_y(dy), lax.rem(place.c + dc, CORES)
                self.peers.append((dy * CORES + dc, y * CORES + c, place.at(y=y, c=c)))
        self.copies, self.own = {}, []

    def give(self, key, src, dst):
        slot, _, device = self.peers[key[0]]
        sems = self.ssem.at[slot, key[1]], self.rsem.at[slot, key[1]]
        self.copies[key] = push(src, dst, *sems, device)

    def mine(self, src, dst, t=0):
        self.own.append(keep(src, dst, self.lsem.at[t]))

    def take(self):
        for copy in self.copies.values():
            copy.wait_recv()
        for copy in self.own:
            copy.wait()

    def close(self):
        for copy in self.copies.values():
            copy.wait_send()


def span(index, size):
    return pl.ds(pl.multiple_of(index * size, size), size)


def after(steps, stage, hooks):
    out = []
    for step in steps:
        out.append(step)
        if step.func == stage:
            out += hooks.get(step.args[0]["i"], [])
    return out


def forward_body(slices, shards, items, nw, *refs):
    ws, (order, cot) = refs[:nw], refs[nw : nw + 2]
    tokens, member, ends, emb, cos, sin = refs[nw + 2 : nw + 8]
    refs = refs[nw + 8 :]
    outs, rows_out = refs[:nw], refs[nw : nw + 2]
    h_one, scales, seg_col, seg_row, qkv, mixed_heads, logsum, mixed = refs[nw + 2 : nw + 10]
    scratch = refs[nw + 10 :]
    place = Place(slices, shards)
    gather = WeightGather(place, items, ws, outs, *scratch[:4])
    order_rows, cot_rows = row_gathers(place, (order, cot), rows_out, scratch[4:12])
    w_time, w_part, packed, places, csem, ssem, rsem, lsem = scratch[12:]
    rows, width = tokens.shape
    part = mixed_heads.shape[1]
    pairs = part // 128
    ex = [Exchange(place, ssem.at[t], rsem.at[t], lsem.at[t]) for t in range(3 + pairs)]
    comes, backs = ex[:3], ex[3:]
    me, peers = comes[0].me, comes[0].peers

    def first_norm():
        copy = keep(outs[0], w_time, csem.at[0])
        copy.wait()
        for j in range(shards):
            add = jnp.dot(
                emb[j], w_time[j // XS, j % XS], preferred_element_type=jnp.float32
            )
            scales[...] = add if j == 0 else scales[...] + add

        def step(i, _):
            own = span(i, rows // 3)
            v = tokens[own, :].astype(jnp.float32)
            scale = sum(member[own, j : j + 1] * scales[j : j + 1, :width] for j in range(NSEQ))
            centred = v - jnp.mean(v, axis=1, keepdims=True)
            spread = jnp.mean(centred * centred, axis=1, keepdims=True)
            h_one[own, :] = (centred * lax.rsqrt(spread + EPS) * (1.0 + scale)).astype(BF)
            return 0

        lax.fori_loop(0, 3, step, 0)

    def project(j):
        copy = keep(outs[1].at[:, :, :, j * width : (j + 1) * width], w_part, csem.at[1])
        copy.wait()
        wide = 256

        def step(i, _):
            cols = span(i, wide)
            w = w_part[:, :, :, cols].reshape(width, wide)
            y = jnp.dot(h_one[...], w, preferred_element_type=jnp.float32)
            for t in range(wide // 128):
                v = y[:, t * 128 : (t + 1) * 128]
                if j < 2:
                    v = v * cos[...] + swap_halves(v) * sin[...]
                packed[j, i * (wide // 128) + t] = v.astype(BF)
            return 0

        lax.fori_loop(0, width // wide, step, 0)
        for k, (_, peer, _) in enumerate(peers):
            for t in range(pairs):
                comes[j].give(
                    (k, t),
                    packed.at[j, peer * pairs + t],
                    qkv.at[j, span(me, rows), t * 128 : (t + 1) * 128],
                )
        for t in range(pairs):
            comes[j].mine(
                packed.at[j, me * pairs + t], qkv.at[j, span(me, rows), t * 128 : (t + 1) * 128], t
            )

    def segments():
        order_rows.middle()
        order_rows.end()
        copy = keep(rows_out[0], places, csem.at[2])
        copy.wait()
        row = jnp.concatenate(
            [places[y, c] for y in range(place.Y) for c in range(CORES)], axis=1
        )
        seg = sum((row >= ends[j : j + 1, :1]).astype(jnp.float32) for j in range(NSEQ - 1))
        seg_row[...] = seg
        seg_col[...] = seg.T

    block = 256

    def attend(h):
        def step(i, _):
            forward_block(qkv, seg_col, seg_row, mixed_heads, logsum, h, span(i, block))
            return 0

        lax.fori_loop(0, seg_col.shape[0] // block, step, 0)

    def finish(t, k, owner):
        src = mixed_heads.at[span(owner, rows), t * 128 : (t + 1) * 128]
        first = pl.multiple_of(me * part + t * 128, 128)
        dst = mixed.at[:, pl.ds(first, 128)]
        if k < len(peers):
            backs[t].give((k, 0), src, dst)
        else:
            backs[t].mine(src, dst)

    def take():
        for come in comes:
            come.take()

    gather.load()
    order_rows.load()
    cot_rows.load()
    greet(place, seq=True)
    steps = pipeline(gather.plan, gather.stages())
    last = {p["w"]: p["i"] for p in gather.plan}
    ready = [[p["i"] for p in gather.plan if p["w"] == 1 and p["first"] == j * width][-1] for j in range(3)]
    hooks = {last[0]: [segments, first_norm]}
    for j in range(3):
        hooks[ready[j]] = [functools.partial(project, j)]
    steps = after(steps, gather.finish, hooks)
    run(steps[:1])
    order_rows.start()
    gather.store()
    ahead = steps.index(hooks[ready[2]][0]) + 1
    run(steps[1:ahead])
    work = [(lambda: None, 16), (take, 0), (cot_rows.start, 0)]
    owners = [peer for _, peer, _ in peers] + [me]
    for t in range(pairs):
        work += [(functools.partial(attend, h), 10) for h in (2 * t, 2 * t + 1)]
        work += [(functools.partial(finish, t, k, owner), 0) for k, owner in enumerate(owners)]
    work += [(cot_rows.middle, 0)]
    interleave(steps[ahead:], work)
    for back in backs:
        back.take()
    cot_rows.end()
    for e in ex:
        e.close()


def forward(slices, shards, which, ws, rows_in, tokens, member, ends, emb, cos, sin, cid):
    rows, width = tokens.shape
    group, part = rows * slices, width // slices
    pairs = part // 128
    items = pieces(width // shards, width, which, GATHER_CLASS)
    nw = len(ws)
    f32 = jnp.float32
    out = pl.pallas_call(
        functools.partial(forward_body, slices, shards, items, nw),
        out_shape=gathered_shapes(slices, shards, ws, rows_in)
        + [
            jax.ShapeDtypeStruct((rows, width), BF),
            jax.ShapeDtypeStruct((8, 2 * width), f32),
            jax.ShapeDtypeStruct((group, 1), f32),
            jax.ShapeDtypeStruct((1, group), f32),
            jax.ShapeDtypeStruct((3, group, part), BF),
            jax.ShapeDtypeStruct((group, part), BF),
            jax.ShapeDtypeStruct((part // HD, group), f32),
            jax.ShapeDtypeStruct((rows, width), BF),
        ],
        in_specs=[ANY] * (nw + 2) + [VM] * 6,
        out_specs=[ANY] * (nw + 2) + [VM] * 8,
        scratch_shapes=gather_scratch(slices, shards, items)
        + row_scratch(slices, rows_in)
        + [
            pltpu.VMEM((shards // XS, XS) + ws[0].shape, BF),
            pltpu.VMEM((shards // XS, XS, width // shards, width), BF),
            pltpu.VMEM((3, width // 128, rows, 128), BF),
            pltpu.VMEM((slices // CORES, CORES, 1, rows), jnp.int32),
            DMA((3,)),
            DMA((3 + pairs, slices, pairs)),
            DMA((3 + pairs, slices, pairs)),
            DMA((3 + pairs, pairs)),
        ],
        compiler_params=pltpu.CompilerParams(
            collective_id=cid, has_side_effects=True, vmem_limit_bytes=VMEM_ALL
        ),
    )(*ws, *rows_in, tokens, member, ends, emb, cos, sin)
    full = [g.reshape((slices,) + r.shape) for g, r in zip(out[nw:], rows_in)]
    return merged(out[:nw]), full, out[nw + 2 :]


def backward_body(slices, shards, items, nw, nr, *refs):
    grads, rows_in = refs[:nw], refs[nw : nw + nr]
    at = nw + nr
    d_mixed, qkv, mixed, logsum, seg_col, seg_row, cos, sin = refs[at : at + 8]
    at += 8
    sums_out, rows_out, out = refs[at : at + nw], refs[at + nw : at + nw + nr], refs[at + nw + nr]
    scratch = refs[at + nw + nr + 1 :]
    place = Place(slices, shards)
    sums = GradSum(place, items, grads, sums_out, *scratch[:10])
    gathers = row_gathers(place, rows_in, rows_out, scratch[10:])
    g, dk, dv, dq, turned, ssem, rsem, lsem = scratch[10 + 4 * nr :]
    rows, part = d_mixed.shape[0], g.shape[1]
    pairs = part // 128
    come = Exchange(place, ssem.at[0], rsem.at[0], lsem.at[0])
    backs = [
        Exchange(place, ssem.at[1 + t], rsem.at[1 + t], lsem.at[1 + t]) for t in range(pairs)
    ]
    me = come.me
    come.mine(d_mixed.at[:, span(me, part)], g.at[span(me, rows), :])
    for r in gathers:
        r.load()
    greet(place, seq=True)
    for k, (_, peer, _) in enumerate(come.peers):
        come.give((k, 0), d_mixed.at[:, span(peer, part)], g.at[span(me, rows), :])
    block = 256

    def attend(h):
        if h % 2 == 0:
            dk[...] = jnp.zeros_like(dk)
            dv[...] = jnp.zeros_like(dv)

        def step(i, _):
            backward_block(
                qkv, mixed, logsum, g, seg_col, seg_row, dk, dv, dq, h, span(i, block), h % 2
            )
            return 0

        lax.fori_loop(0, seg_col.shape[0] // block, step, 0)

    def finish(t, k, owner):
        own = span(owner, rows)
        c, s = cos[own, :], sin[own, :]
        for j, d in enumerate((dq, dk)):
            v = d[own, :] * (HD**-0.5)
            turned[t, j, own, :] = (v * c - swap_halves(v) * s).astype(BF)
        turned[t, 2, own, :] = dv[own, :].astype(BF)
        first = pl.multiple_of(me * part + t * 128, 128)
        src, dst = turned.at[t, :, own, :], out.at[:, :, pl.ds(first, 128)]
        if k < len(come.peers):
            backs[t].give((k, 0), src, dst)
        else:
            backs[t].mine(src, dst)

    work = [(lambda: None, 20), (come.take, 0)] + [(r.start, 0) for r in gathers]
    owners = [peer for _, peer, _ in come.peers] + [me]
    for t in range(pairs):
        work += [(functools.partial(attend, h), 16) for h in (2 * t, 2 * t + 1)]
        work += [(functools.partial(finish, t, k, owner), 0) for k, owner in enumerate(owners)]
    steps = pipeline(sums.plan, sums.stages())
    interleave(steps, work)
    for r in gathers:
        r.middle()
    for back in backs:
        back.take()
    for r in gathers:
        r.end()
    for ex in [come] + backs:
        ex.close()


def attention_backward(
    slices, shards, width, which, grads, rows_in, d_mixed, kept, seg_col, seg_row, cos, sin, cid
):
    rows = d_mixed.shape[0]
    group, part = rows * slices, width // slices
    items = pieces(width // shards, width, which, SUM_CLASS)
    nw, nr, pairs = len(grads), len(rows_in), part // 128
    grads = split_grads(shards, grads)
    total = pltpu.VMEM((group, 128), jnp.float32)
    out = pl.pallas_call(
        functools.partial(backward_body, slices, shards, items, nw, nr),
        out_shape=[jax.ShapeDtypeStruct(w.shape[2:], BF) for w in grads]
        + gathered_shapes(slices, shards, [], rows_in)
        + [jax.ShapeDtypeStruct((3, rows, width), BF)],
        in_specs=[ANY] * (nw + nr + 1) + [VM] * 7,
        out_specs=[ANY] * (nw + nr) + [VM],
        scratch_shapes=sum_scratch(slices, shards, items)
        + row_scratch(slices, rows_in)
        + [pltpu.VMEM((group, part), BF), total, total, total]
        + [pltpu.VMEM((pairs, 3, group, 128), BF)]
        + [DMA((1 + pairs, slices, 1)), DMA((1 + pairs, slices, 1)), DMA((1 + pairs, 1))],
        compiler_params=pltpu.CompilerParams(
            collective_id=cid, has_side_effects=True, vmem_limit_bytes=VMEM_ALL
        ),
    )(*grads, *rows_in, d_mixed, *kept, seg_col, seg_row, cos, sin)
    full = [g.reshape((slices,) + r.shape) for g, r in zip(out[nw:], rows_in)]
    return out[:nw], full, out[nw + nr]


def time_embedding(steps):
    half = TEMB // 2
    freqs = jnp.exp(-math.log(BASE) * jnp.arange(half, dtype=jnp.float32) / half)
    angles = steps.astype(jnp.float32)[:, None] * freqs[None, :]
    return jnp.concatenate([jnp.sin(angles), jnp.cos(angles)], axis=-1)


def layout(lens, places):
    ends = jnp.cumsum(lens)
    starts = ends - lens
    member = (places[:, None] >= starts[None, :]) & (places[:, None] < ends[None, :])
    labels = jnp.arange(NSEQ, dtype=jnp.int32)
    segment = jnp.sum(jnp.where(member, labels[None, :], 0), axis=1)
    offset = places - jnp.sum(jnp.where(member, starts[None, :], 0), axis=1)
    return (member.astype(jnp.float32), segment, offset)


def turn_tables(offset):
    half = HD // 2
    freqs = jnp.exp(-math.log(BASE) * jnp.arange(half, dtype=jnp.float32) * 2.0 / HD)
    angles = offset.astype(jnp.float32)[:, None] * freqs[None, :]
    c, s = jnp.cos(angles), jnp.sin(angles)
    return jnp.concatenate([c] * 4, axis=1), jnp.concatenate([-s, s, -s, s], axis=1)


def norm_mod(values, scale):
    centre = jnp.mean(values, axis=-1, keepdims=True)
    centred = values - centre
    spread = jnp.mean(centred * centred, axis=-1, keepdims=True)
    return centred * lax.rsqrt(spread + EPS) * (1.0 + scale)


def pick_rows(data, wanted, labels):
    pick = (wanted[:, None] == labels[None, :]).astype(BF)
    return jnp.dot(pick, data.reshape(-1, data.shape[-1]), preferred_element_type=jnp.float32)


def on_device(tokens, lengths, time_steps, order, w_time, w_qkv, w_out, w_up, w_down, cotangent):
    rows, width = tokens.shape[1:]
    slices, shards = lax.axis_size("seq"), lax.axis_size("fsdp")
    group = rows * slices
    lens, places = lengths[0], order[0]
    member, _, offset = layout(lens, places)
    emb = time_embedding(time_steps[0]).astype(BF)
    cos, sin = turn_tables(offset)
    fulls, (order_all, cot_all), kept = forward(
        slices,
        shards,
        "tqoud",
        [w_time, w_qkv, w_out, w_up, w_down],
        [order, cotangent[0]],
        tokens[0],
        jnp.pad(member, ((0, 0), (0, 8 - NSEQ))),
        jnp.broadcast_to(jnp.pad(jnp.cumsum(lens), (0, 8 - NSEQ))[:, None], (8, 128)),
        jnp.pad(emb, ((0, 8 - NSEQ), (0, 0))).reshape(8, shards, -1).transpose(1, 0, 2),
        cos,
        sin,
        0,
    )
    _, f_qkv, f_out, f_up, f_down = fulls
    h_one, scales_seq, seg_col, seg_row, heads_qkv, mixed_heads, logsum, mixed = kept
    order_all = order_all.reshape(group)
    _, _, offset_all = layout(lens, order_all)
    scales = jnp.dot(member, scales_seq[:NSEQ], precision=lax.Precision.HIGHEST)
    scale_one, scale_two = scales[:, :width], scales[:, width:]
    inputs = tokens[0].astype(jnp.float32)
    _, pull_one = jax.vjp(norm_mod, inputs, scale_one)

    x_two = inputs + jnp.dot(mixed, f_out, preferred_element_type=jnp.float32)
    normed_two, pull_two = jax.vjp(norm_mod, x_two, scale_two)
    h_two = normed_two.astype(BF)
    up = jnp.dot(h_two, f_up, preferred_element_type=jnp.float32)
    activated, pull_gelu = jax.vjp(jax.nn.gelu, up)
    hidden = activated.astype(BF)
    result = (x_two + jnp.dot(hidden, f_down, preferred_element_type=jnp.float32)).astype(BF)

    d_result = pick_rows(cot_all, places, jnp.arange(group, dtype=jnp.int32))
    d_low = d_result.astype(BF)
    grad_down = dot(hidden, d_low, 0, 0).astype(BF)
    d_up = pull_gelu(dot(d_low, f_down, 1, 1))[0].astype(BF)
    grad_up = dot(h_two, d_up, 0, 0).astype(BF)
    d_xpart, d_scale_two = pull_two(dot(d_up, f_up, 1, 1))
    d_xtwo = d_result + d_xpart
    d_attn = d_xtwo.astype(BF)
    grad_out = dot(mixed, d_attn, 0, 0).astype(BF)
    d_mixed = dot(d_attn, f_out, 1, 1).astype(BF)

    cos_all, sin_all = turn_tables(offset_all)
    sums, (result_all,), d_packed = attention_backward(
        slices,
        shards,
        width,
        "duo",
        [grad_down, grad_up, grad_out],
        [result],
        d_mixed,
        (heads_qkv, mixed_heads, logsum),
        seg_col,
        seg_row,
        cos_all,
        sin_all,
        2,
    )
    d_qkv = d_packed.transpose(1, 0, 2).reshape(rows, 3 * width)
    grad_qkv = dot(h_one, d_qkv, 0, 0).astype(BF)
    d_xone, d_scale_one = pull_one(dot(d_qkv, f_qkv, 1, 1))
    input_grad = d_xtwo + d_xone
    d_scales = lax.dot_general(
        member,
        jnp.concatenate([d_scale_one, d_scale_two], axis=1),
        (((0,), (0,)), ((), ())),
        precision=lax.Precision.HIGHEST,
        preferred_element_type=jnp.float32,
    )
    grad_time = lax.dot_general(
        emb.astype(jnp.float32),
        d_scales,
        (((0,), (0,)), ((), ())),
        precision=lax.Precision.HIGHEST,
        preferred_element_type=jnp.float32,
    ).astype(BF)

    sums = sums + sum_grads(slices, shards, width, "qt", [grad_qkv, grad_time], 3)
    s_down, s_up, s_out, s_qkv, s_time = [g.astype(jnp.float32) for g in sums]
    mine = lax.axis_index("seq") * rows + jnp.arange(rows, dtype=jnp.int32)
    output = pick_rows(result_all, mine, order_all).astype(BF)
    return (output[None], input_grad[None], s_time, s_qkv, s_out, s_up, s_down)


def solution(mesh):
    row, tok, mat = P("fsdp", None), P("fsdp", "seq", None), P("fsdp", None)
    return jax.shard_map(
        on_device,
        mesh=mesh,
        in_specs=(tok, row, row, P("fsdp", "seq"), mat, mat, mat, mat, mat, tok),
        out_specs=(tok, tok, mat, mat, mat, mat, mat),
        check_vma=False,
    )
```

```python
import functools
import math

import jax
import jax.numpy as jnp
from jax import lax
from jax.experimental import pallas as pl
from jax.experimental.pallas import tpu as pltpu
from jax.sharding import PartitionSpec as P

H = 16
HD = 64
TEMB = 256
NSEQ = 3

EPS = 1e-05
NEG = -1e30
BASE = 10000.0
LOG2E = math.log2(math.e)
CORES = 2
XS = 2
BF = jnp.bfloat16

ANY = pl.BlockSpec(memory_space=pl.ANY)
VM = pl.BlockSpec(memory_space=pltpu.VMEM)
DMA = pltpu.SemaphoreType.DMA
MESH = pl.DeviceIdType.MESH
VMEM_ALL = 67043328
CUT = 2
LAG = 2

GATHER_CLASS = {"t": "D", "q": "DDC", "o": "C", "u": "CCCC", "d": "CCDC"}
SUM_CLASS = {'q': 'DCD', 'o': 'C', 'u': 'CCCC', 'd': 'CDCC'}


class Place:
    def __init__(self, slices, shards):
        self.Y, self.Z = slices // CORES, shards // XS
        seq, fsdp = lax.axis_index("seq"), lax.axis_index("fsdp")
        self.y, self.c = lax.div(seq, CORES), lax.rem(seq, CORES)
        self.z, self.x = lax.div(fsdp, XS), lax.rem(fsdp, XS)

    def at(self, z=None, x=None, y=None, c=None):
        z = self.z if z is None else z
        x = self.x if x is None else x
        y = self.y if y is None else y
        c = self.c if c is None else c
        return {"seq": y * CORES + c, "fsdp": z * XS + x}

    def next_y(self, d):
        return lax.rem(self.y + d, self.Y)

    def next_z(self, d):
        return lax.rem(self.z + d, self.Z)


def greet(place, seq=False):
    barrier = pltpu.get_barrier_semaphore()
    others = [place.at(c=1 - place.c), place.at(x=1 - place.x)]
    others += [place.at(y=place.next_y(d)) for d in range(1, place.Y)]
    others += [place.at(z=place.next_z(d)) for d in range(1, place.Z)]
    if seq:
        others += [place.at(y=place.next_y(d), c=1 - place.c) for d in range(1, place.Y)]
    for other in others:
        pl.semaphore_signal(barrier, inc=1, device_id=other, device_id_type=MESH)
    pl.semaphore_wait(barrier, len(others))


def push(src, dst, send_sem, recv_sem, device):
    copy = pltpu.make_async_remote_copy(
        src_ref=src,
        dst_ref=dst,
        send_sem=send_sem,
        recv_sem=recv_sem,
        device_id=device,
        device_id_type=MESH,
    )
    copy.start()
    return copy


def keep(src, dst, sem):
    copy = pltpu.make_async_copy(src, dst, sem)
    copy.start()
    return copy


def pipeline(plan, stages):
    lags = [LAG * k for k in range(len(stages))]
    return [
        functools.partial(stage, plan[t - lag])
        for t in range(len(plan) + lags[-1])
        for lag, stage in zip(lags, stages)
        if 0 <= t - lag < len(plan)
    ]


def run(steps):
    for step in steps:
        step()


def interleave(steps, work):
    done = 0
    for piece, count in work:
        piece()
        run(steps[done : done + count])
        done += count
    run(steps[done:])


class RowGather:
    def __init__(self, place, src, out, bounce, sems, rsems, lsem):
        self.place, self.src, self.out = place, src, out
        self.bounce, self.sems, self.rsems, self.lsem = bounce, sems, rsems, lsem

    def load(self):
        self.own = keep(self.src, self.bounce, self.lsem)

    def start(self):
        p = self.place
        slot = self.out.at[p.y, p.c]
        self.over_y = [
            push(self.src, slot, self.sems.at[d], self.rsems.at[d], p.at(y=p.next_y(d)))
            for d in range(1, p.Y)
        ]
        self.own.wait()
        self.own = keep(self.bounce, slot, self.lsem)

    def middle(self):
        p = self.place
        for copy in self.over_y:
            copy.wait_recv()
        self.own.wait()
        half = self.out.at[:, p.c]
        self.over_c = push(half, half, self.sems.at[0], self.rsems.at[0], p.at(c=1 - p.c))

    def end(self):
        for copy in self.over_y:
            copy.wait_send()
        self.over_c.wait()


def pieces(rows, width, which, classes):
    whole = []
    for j, name in enumerate(which):
        if name == "t":
            for k, kind in enumerate(classes["t"]):
                span = 2 * width // len(classes["t"])
                whole.append((j, 0, rows // 4, k * span, span, kind))
        elif name == "d":
            for k, kind in enumerate(classes["d"]):
                whole.append((j, k * rows, rows, 0, width, kind))
        else:
            for k, kind in enumerate(classes[name]):
                whole.append((j, 0, rows, k * width, width, kind))
    out = []
    for j, r0, rn, c0, cn, kind in whole:
        cuts = CUT if rn % (16 * CUT) == 0 else 1
        out += [(j, r0 + k * rn // cuts, rn // cuts, c0, cn, kind) for k in range(cuts)]
    return out


class WeightGather:
    def __init__(self, place, items, shards, outs, bounce, ssem, rsem, lsem):
        self.place = place
        self.shards, self.outs, self.bounce = shards, outs, bounce
        self.ssem, self.rsem, self.lsem = ssem, rsem, lsem
        self.plan = []
        for i, (w, r0, rn, c0, cn, kind) in enumerate(items):
            half = cn // CORES
            width = half // place.Y if kind == "D" else half
            first = c0 + place.c * half
            if kind == "D":
                first = first + place.y * width
            self.plan.append(
                dict(
                    i=i,
                    w=w,
                    kind=kind,
                    first=c0,
                    rows=pl.ds(r0, rn),
                    cols=pl.ds(pl.multiple_of(first, 128), width),
                    half=pl.ds(pl.multiple_of(c0 + place.c * half, 128), half),
                    held=bounce.at[i, pl.ds(0, rn), pl.ds(0, width)],
                )
            )

    def region(self, p, z, x, cols):
        return self.outs[p["w"]].at[z, x, p["rows"], cols]

    def load(self):
        for p in self.plan:
            p["own"] = keep(
                self.shards[p["w"]].at[p["rows"], p["cols"]], p["held"], self.lsem.at[p["i"]]
            )

    def store(self):
        place = self.place
        for p in self.plan:
            p["own"].wait()
            p["own"] = keep(
                p["held"], self.region(p, place.z, place.x, p["cols"]), self.lsem.at[p["i"]]
            )

    def post(self, p, slot, src, dst, device):
        return push(src, dst, self.ssem.at[p["i"], slot], self.rsem.at[p["i"], slot], device)

    def over_z(self, p):
        place = self.place
        src = self.shards[p["w"]].at[p["rows"], p["cols"]]
        dst = self.region(p, place.z, place.x, p["cols"])
        p["z"] = [
            self.post(p, d - 1, src, dst, place.at(z=place.next_z(d))) for d in range(1, place.Z)
        ]

    def over_x(self, p):
        place = self.place
        for copy in p["z"]:
            copy.wait_recv()
        p["own"].wait()
        part = self.region(p, pl.ds(0, place.Z), place.x, p["cols"])
        p["x"] = self.post(p, place.Z - 1, part, part, place.at(x=1 - place.x))

    def over_y(self, p):
        place = self.place
        p["x"].wait_recv()
        p["y"] = []
        if p["kind"] == "D":
            part = self.region(p, pl.ds(0, place.Z), pl.ds(0, XS), p["cols"])
            p["y"] = [
                self.post(p, place.Z - 1 + d, part, part, place.at(y=place.next_y(d)))
                for d in range(1, place.Y)
            ]

    def over_c(self, p):
        place = self.place
        for copy in p["y"]:
            copy.wait_recv()
        part = self.region(p, pl.ds(0, place.Z), pl.ds(0, XS), p["half"])
        p["c"] = self.post(p, place.Z - 1 + place.Y, part, part, place.at(c=1 - place.c))

    def finish(self, p):
        p["c"].wait()
        for copy in p["z"] + p["y"] + [p["x"]]:
            copy.wait_send()

    def stages(self):
        return [self.over_z, self.over_x, self.over_y, self.over_c, self.finish]


def gather_scratch(slices, shards, items):
    Y, Z = slices // CORES, shards // XS
    n, rows = len(items), max(item[2] for item in items)
    widest = max(cn // CORES // (Y if kind == "D" else 1) for _, _, _, _, cn, kind in items)
    return [pltpu.VMEM((n, rows, widest), BF), DMA((n, Z + Y)), DMA((n, Z + Y)), DMA((n,))]


def gathered_shapes(slices, shards, ws, rows_in):
    Y, Z = slices // CORES, shards // XS
    return [jax.ShapeDtypeStruct((Z, XS) + w.shape, w.dtype) for w in ws] + [
        jax.ShapeDtypeStruct((Y, CORES) + r.shape, r.dtype) for r in rows_in
    ]


def row_scratch(slices, rows_in):
    Y = slices // CORES
    out = []
    for r in rows_in:
        out += [pltpu.VMEM(r.shape, r.dtype), DMA((Y,)), DMA((Y,)), DMA((1,))]
    return out


def row_gathers(place, rows_in, rows_out, scratch):
    rows = []
    for k, (src, out) in enumerate(zip(rows_in, rows_out)):
        b, s, r, m = scratch[4 * k : 4 * k + 4]
        rows.append(RowGather(place, src, out, b, s, r, m.at[0]))
    return rows


def merged(fulls):
    return [g.reshape(-1, g.shape[-1]) for g in fulls]


def add_into(dst, src, rn):
    lead = dst.shape[:-2]

    def step(k, _):
        idx, rest = [], k
        for size in reversed(lead[1:]):
            idx.append(lax.rem(rest, size))
            rest = lax.div(rest, size)
        idx = tuple(reversed(idx + [rest]))
        a, b = dst.at[idx], src.at[idx]
        rows = pl.ds(0, rn)
        a[rows, :] = (a[rows, :].astype(jnp.float32) + b[rows, :].astype(jnp.float32)).astype(BF)
        return 0

    lax.fori_loop(0, math.prod(lead), step, 0)


class GradSum:
    def __init__(self, place, items, grads, outs, acc, own, ry, rx, rz, fin, rf, lsem, ssem, rsem):
        self.place, self.grads, self.outs = place, grads, outs
        self.acc, self.own, self.ry, self.rx, self.rz = acc, own, ry, rx, rz
        self.fin, self.rf = fin, rf
        self.lsem, self.ssem, self.rsem = lsem, ssem, rsem
        self.wide = acc.shape[-1]
        self.plan = []
        for i, (w, r0, rn, c0, cn, kind) in enumerate(items):
            p = dict(i=i, w=w, kind=kind, rn=rn, c0=c0, half=cn // CORES)
            p["first"] = c0
            p["k"] = sum(q["kind"] == kind for q in self.plan)
            p.update(rows=pl.ds(r0, rn), vr=pl.ds(0, rn), sends=[])
            self.plan.append(p)

    def post(self, p, slot, src, dst, device):
        copy = push(src, dst, self.ssem.at[p["i"], slot], self.rsem.at[p["i"], slot], device)
        p["sends"].append(copy)
        return copy

    def cols(self, p, core, part=None):
        first = p["c0"] + core * p["half"]
        if part is None:
            return pl.ds(pl.multiple_of(first, 128), p["half"])
        return pl.ds(pl.multiple_of(first + part * self.wide, 128), self.wide)

    def parts(self, p):
        return [self.place.y] if p["kind"] == "D" else list(range(self.place.Y))

    def over_c(self, p):
        place, i, vr = self.place, p["i"], p["vr"]
        g = self.grads[p["w"]]
        first = place.Z + place.Y + place.Y
        p["own"], p["c"] = [], []
        for part in range(place.Y):
            p["own"].append(
                keep(
                    g.at[:, :, p["rows"], self.cols(p, place.c, part)],
                    self.own.at[i % (LAG + 1), part, :, :, vr, :],
                    self.lsem.at[i, part],
                )
            )
            p["c"].append(
                self.post(
                    p,
                    first + part,
                    g.at[:, :, p["rows"], self.cols(p, 1 - place.c, part)],
                    self.acc.at[i, part, :, :, vr, :],
                    place.at(c=1 - place.c),
                )
            )

    def over_y(self, p):
        place, i, vr = self.place, p["i"], p["vr"]
        for copy in p["own"]:
            copy.wait()
        for copy in p["c"]:
            copy.wait_recv()
        for part in range(place.Y):
            add_into(self.acc.at[i, part], self.own.at[i % (LAG + 1), part], p["rn"])
        p["y"] = []
        if p["kind"] == "D":
            for d in range(1, place.Y):
                y = place.next_y(d)
                p["y"].append(
                    self.post(
                        p,
                        d,
                        self.acc.at[i, y, :, :, vr, :],
                        self.ry.at[p["k"], d - 1, :, :, vr, :],
                        place.at(y=y),
                    )
                )

    def over_x(self, p):
        place, i, vr = self.place, p["i"], p["vr"]
        for d, copy in enumerate(p["y"]):
            copy.wait_recv()
            add_into(self.acc.at[i, place.y], self.ry.at[p["k"], d], p["rn"])
        other = 1 - place.x
        if p["kind"] == "D":
            src, dst = self.acc.at[i, place.y, :, other, vr, :], self.rx.at[i, 0, :, vr, :]
        else:
            src, dst = self.acc.at[i, :, :, other, vr, :], self.rx.at[i, :, :, vr, :]
        p["x"] = self.post(p, place.Y, src, dst, place.at(x=other))

    def over_z(self, p):
        place, i, vr = self.place, p["i"], p["vr"]
        p["x"].wait_recv()
        for k, part in enumerate(self.parts(p)):
            add_into(self.acc.at[i, part, :, place.x], self.rx.at[i, k], p["rn"])
        p["z"] = []
        for d in range(1, place.Z):
            z = place.next_z(d)
            if p["kind"] == "D":
                src = self.acc.at[i, place.y, z, place.x, vr, :]
                dst = self.rz.at[i, d - 1, 0, vr, :]
            else:
                src = self.acc.at[i, :, z, place.x, vr, :]
                dst = self.rz.at[i, d - 1, :, vr, :]
            p["z"].append(self.post(p, place.Y + d, src, dst, place.at(z=z)))

    def region(self, p, core, part=None):
        return self.outs[p["w"]].at[p["rows"], self.cols(p, core, part)]

    def back_y(self, p):
        place, i, vr = self.place, p["i"], p["vr"]
        for copy in p["z"]:
            copy.wait_recv()
        for k, part in enumerate(self.parts(p)):
            total = self.acc[i, part, place.z, place.x, vr, :].astype(jnp.float32)
            for d in range(1, place.Z):
                total = total + self.rz[i, d - 1, k, vr, :].astype(jnp.float32)
            if p["kind"] == "D":
                self.fin[i, 0, vr, :] = total.astype(BF)
            else:
                self.rf[p["k"], place.y, part, vr, :] = total.astype(BF)
        first = place.Z + place.Y - 1
        p["f"], p["st"] = [], []
        if p["kind"] == "D":
            src, dst = self.fin.at[i, 0, vr, :], self.region(p, place.c, place.y)
            p["st"].append(keep(src, dst, self.lsem.at[i, 0]))
        else:
            src = dst = self.rf.at[p["k"], place.y, :, vr, :]
        for d in range(1, place.Y):
            p["f"].append(self.post(p, first + d, src, dst, place.at(y=place.next_y(d))))

    def back_c(self, p):
        place, i, vr = self.place, p["i"], p["vr"]
        for copy in p["f"]:
            copy.wait_recv()
        if p["kind"] == "C":
            for part in range(place.Y):
                total = self.rf[p["k"], 0, part, vr, :].astype(jnp.float32)
                for y in range(1, place.Y):
                    total = total + self.rf[p["k"], y, part, vr, :].astype(jnp.float32)
                self.fin[i, part, vr, :] = total.astype(BF)
                src, dst = self.fin.at[i, part, vr, :], self.region(p, place.c, part)
                p["st"].append(keep(src, dst, self.lsem.at[i, part]))
        for copy in p["st"]:
            copy.wait()
        part = self.region(p, place.c)
        p["e"] = self.post(p, 0, part, part, place.at(c=1 - place.c))

    def finish(self, p):
        p["e"].wait_recv()
        for copy in p["sends"]:
            copy.wait_send()

    def stages(self):
        return [
            self.over_c,
            self.over_y,
            self.over_x,
            self.over_z,
            self.back_y,
            self.back_c,
            self.finish,
        ]


def sum_scratch(slices, shards, items):
    Y, Z = slices // CORES, shards // XS
    n, wide = len(items), items[0][4] // CORES // Y
    rows = max(item[2] for item in items)
    nd = max(1, sum(item[5] == "D" for item in items))
    nc = max(1, n - nd)
    return [
        pltpu.VMEM((n, Y, Z, XS, rows, wide), BF),
        pltpu.VMEM((LAG + 1, Y, Z, XS, rows, wide), BF),
        pltpu.VMEM((nd, Y - 1, Z, XS, rows, wide), BF),
        pltpu.VMEM((n, Y, Z, rows, wide), BF),
        pltpu.VMEM((n, Z - 1, Y, rows, wide), BF),
        pltpu.VMEM((n, Y, rows, wide), BF),
        pltpu.VMEM((nc, Y, Y, rows, wide), BF),
        DMA((n, Y)),
        DMA((n, Z + 3 * Y)),
        DMA((n, Z + 3 * Y)),
    ]


def split_grads(shards, grads):
    return [g.reshape(shards // XS, XS, -1, g.shape[1]) for g in grads]


def spread_body(slices, shards, mine, out, group, total, ssem, rsem):
    place = Place(slices, shards)
    seq = place.y * CORES + place.c
    fsdp = place.z * XS + place.x
    near, far = [], []
    for d in range(1, slices):
        near.append({"seq": lax.rem(seq + d, slices), "fsdp": fsdp})
    for d in range(1, shards):
        far.append({"seq": seq, "fsdp": lax.rem(fsdp + d, shards)})
    barrier = pltpu.get_barrier_semaphore()
    for other in near + far:
        pl.semaphore_signal(barrier, inc=1, device_id=other, device_id_type=MESH)
    pl.semaphore_wait(barrier, len(near + far))
    copies = [
        push(mine, group.at[seq], ssem.at[d], rsem.at[d], other) for d, other in enumerate(near)
    ]
    group[seq] = mine[...]
    for copy in copies:
        copy.wait_recv()
    total[...] = sum(group[k] for k in range(slices))
    first = slices - 1
    copies += [
        push(total, out.at[fsdp], ssem.at[first + d], rsem.at[first + d], other)
        for d, other in enumerate(far)
    ]
    out[fsdp] = total[...]
    for copy in copies[first:]:
        copy.wait_recv()
    for copy in copies:
        copy.wait_send()


def spread(slices, shards, mine, cid):
    n = slices + shards
    return pl.pallas_call(
        functools.partial(spread_body, slices, shards),
        out_shape=jax.ShapeDtypeStruct((shards,) + mine.shape, mine.dtype),
        in_specs=[VM],
        out_specs=VM,
        scratch_shapes=[
            pltpu.VMEM((slices,) + mine.shape, mine.dtype),
            pltpu.VMEM(mine.shape, mine.dtype),
            DMA((n,)),
            DMA((n,)),
        ],
        compiler_params=pltpu.CompilerParams(collective_id=cid, has_side_effects=True),
    )(mine)


def dot(a, b, ca, cb):
    return lax.dot_general(a, b, (((ca,), (cb,)), ((), ())), preferred_element_type=jnp.float32)


def swap_halves(v):
    lane = lax.broadcasted_iota(jnp.int32, v.shape, 1)
    left = pltpu.roll(v, v.shape[1] - HD // 2, 1)
    right = pltpu.roll(v, HD // 2, 1)
    return jnp.where(lax.rem(lane, HD) < HD // 2, left, right)


def forward_block(qkv, seg_col, seg_row, mixed, logsum, h, rows):
    lanes = slice(h * HD, (h + 1) * HD)
    s = dot(qkv[1, :, lanes], qkv[0, rows, lanes], 1, 1) * (LOG2E * HD**-0.5)
    s = jnp.where(seg_col[...] == seg_row[:, rows], s, NEG)
    peak = jnp.max(s, axis=0, keepdims=True)
    expo = jnp.exp2(s - peak)
    total = jnp.sum(expo, axis=0, keepdims=True)
    out = dot(expo.astype(BF), qkv[2, :, lanes], 0, 0)
    mixed[rows, lanes] = (out / total.T).astype(BF)
    logsum[h : h + 1, rows] = peak + jnp.log2(total)


def backward_block(qkv, mixed, logsum, g, seg_col, seg_row, dk, dv, dq, h, rows, slot):
    lanes = slice(h * HD, (h + 1) * HD)
    side = slice(slot * HD, (slot + 1) * HD)
    q, gb = qkv[0, rows, lanes], g[rows, lanes]
    k, v = qkv[1, :, lanes], qkv[2, :, lanes]
    prod = gb.astype(jnp.float32) * mixed[rows, lanes].astype(jnp.float32)
    delta = jnp.sum(prod, axis=1, keepdims=True).T
    s = dot(k, q, 1, 1) * (LOG2E * HD**-0.5)
    same = seg_col[...] == seg_row[:, rows]
    probs = jnp.where(same, jnp.exp2(s - logsum[h : h + 1, rows]), 0.0)
    ds = (probs * (dot(v, gb, 1, 1) - delta)).astype(BF)
    dv[:, side] += dot(probs.astype(BF), gb, 1, 0)
    dk[:, side] += dot(ds, q, 1, 0)
    dq[rows, side] = dot(ds, k, 0, 0)


class Exchange:
    def __init__(self, place, ssem, rsem, lsem):
        self.place, self.ssem, self.rsem, self.lsem = place, ssem, rsem, lsem
        self.me = place.y * CORES + place.c
        self.peers = []
        for dy in list(range(1, place.Y)) + [0]:
            for dc in (range(CORES) if dy else (1,)):
                y, c = place.next_y(dy), lax.rem(place.c + dc, CORES)
                self.peers.append((dy * CORES + dc, y * CORES + c, place.at(y=y, c=c)))
        self.copies, self.own = {}, []

    def give(self, key, src, dst):
        slot, _, device = self.peers[key[0]]
        sems = self.ssem.at[slot, key[1]], self.rsem.at[slot, key[1]]
        self.copies[key] = push(src, dst, *sems, device)

    def mine(self, src, dst, t=0):
        self.own.append(keep(src, dst, self.lsem.at[t]))

    def take(self):
        for copy in self.copies.values():
            copy.wait_recv()
        for copy in self.own:
            copy.wait()

    def close(self):
        for copy in self.copies.values():
            copy.wait_send()


def span(index, size):
    return pl.ds(pl.multiple_of(index * size, size), size)


def after(steps, stage, hooks):
    out = []
    for step in steps:
        out.append(step)
        if step.func == stage:
            out += hooks.get(step.args[0]["i"], [])
    return out


def forward_body(slices, shards, items, nw, *refs):
    ws, (order, cot) = refs[:nw], refs[nw : nw + 2]
    tokens, member, ends, emb, cos, sin = refs[nw + 2 : nw + 8]
    refs = refs[nw + 8 :]
    outs, rows_out = refs[:nw], refs[nw : nw + 2]
    h_one, scales, seg_col, seg_row, qkv, mixed_heads, logsum, mixed = refs[nw + 2 : nw + 10]
    scratch = refs[nw + 10 :]
    place = Place(slices, shards)
    gather = WeightGather(place, items, ws, outs, *scratch[:4])
    order_rows, cot_rows = row_gathers(place, (order, cot), rows_out, scratch[4:12])
    w_time, w_part, packed, places, csem, ssem, rsem, lsem = scratch[12:]
    rows, width = tokens.shape
    part = mixed_heads.shape[1]
    pairs = part // 128
    ex = [Exchange(place, ssem.at[t], rsem.at[t], lsem.at[t]) for t in range(3 + pairs)]
    comes, backs = ex[:3], ex[3:]
    me, peers = comes[0].me, comes[0].peers

    def first_norm():
        copy = keep(outs[0], w_time, csem.at[0])
        copy.wait()
        for j in range(shards):
            add = jnp.dot(
                emb[j], w_time[j // XS, j % XS], preferred_element_type=jnp.float32
            )
            scales[...] = add if j == 0 else scales[...] + add

        def step(i, _):
            own = span(i, rows // 3)
            v = tokens[own, :].astype(jnp.float32)
            scale = sum(member[own, j : j + 1] * scales[j : j + 1, :width] for j in range(NSEQ))
            centred = v - jnp.mean(v, axis=1, keepdims=True)
            spread = jnp.mean(centred * centred, axis=1, keepdims=True)
            h_one[own, :] = (centred * lax.rsqrt(spread + EPS) * (1.0 + scale)).astype(BF)
            return 0

        lax.fori_loop(0, 3, step, 0)

    def project(j):
        copy = keep(outs[1].at[:, :, :, j * width : (j + 1) * width], w_part, csem.at[1])
        copy.wait()
        wide = 256

        def step(i, _):
            cols = span(i, wide)
            w = w_part[:, :, :, cols].reshape(width, wide)
            y = jnp.dot(h_one[...], w, preferred_element_type=jnp.float32)
            for t in range(wide // 128):
                v = y[:, t * 128 : (t + 1) * 128]
                if j < 2:
                    v = v * cos[...] + swap_halves(v) * sin[...]
                packed[j, i * (wide // 128) + t] = v.astype(BF)
            return 0

        lax.fori_loop(0, width // wide, step, 0)
        for k, (_, peer, _) in enumerate(peers):
            for t in range(pairs):
                comes[j].give(
                    (k, t),
                    packed.at[j, peer * pairs + t],
                    qkv.at[j, span(me, rows), t * 128 : (t + 1) * 128],
                )
        for t in range(pairs):
            comes[j].mine(
                packed.at[j, me * pairs + t], qkv.at[j, span(me, rows), t * 128 : (t + 1) * 128], t
            )

    def segments():
        order_rows.middle()
        order_rows.end()
        copy = keep(rows_out[0], places, csem.at[2])
        copy.wait()
        row = jnp.concatenate(
            [places[y, c] for y in range(place.Y) for c in range(CORES)], axis=1
        )
        seg = sum((row >= ends[j : j + 1, :1]).astype(jnp.float32) for j in range(NSEQ - 1))
        seg_row[...] = seg
        seg_col[...] = seg.T

    block = 256

    def attend(h):
        def step(i, _):
            forward_block(qkv, seg_col, seg_row, mixed_heads, logsum, h, span(i, block))
            return 0

        lax.fori_loop(0, seg_col.shape[0] // block, step, 0)

    def finish(t, k, owner):
        src = mixed_heads.at[span(owner, rows), t * 128 : (t + 1) * 128]
        first = pl.multiple_of(me * part + t * 128, 128)
        dst = mixed.at[:, pl.ds(first, 128)]
        if k < len(peers):
            backs[t].give((k, 0), src, dst)
        else:
            backs[t].mine(src, dst)

    def take():
        for come in comes:
            come.take()

    gather.load()
    order_rows.load()
    cot_rows.load()
    greet(place, seq=True)
    steps = pipeline(gather.plan, gather.stages())
    last = {p["w"]: p["i"] for p in gather.plan}
    ready = [[p["i"] for p in gather.plan if p["w"] == 1 and p["first"] == j * width][-1] for j in range(3)]
    hooks = {last[0]: [segments, first_norm]}
    for j in range(3):
        hooks[ready[j]] = [functools.partial(project, j)]
    steps = after(steps, gather.finish, hooks)
    run(steps[:1])
    order_rows.start()
    gather.store()
    ahead = steps.index(hooks[ready[2]][0]) + 1
    run(steps[1:ahead])
    work = [(lambda: None, 16), (take, 0), (cot_rows.start, 0)]
    owners = [peer for _, peer, _ in peers] + [me]
    for t in range(pairs):
        work += [(functools.partial(attend, h), 10) for h in (2 * t, 2 * t + 1)]
        work += [(functools.partial(finish, t, k, owner), 0) for k, owner in enumerate(owners)]
    work += [(cot_rows.middle, 0)]
    interleave(steps[ahead:], work)
    for back in backs:
        back.take()
    cot_rows.end()
    for e in ex:
        e.close()


def forward(slices, shards, which, ws, rows_in, tokens, member, ends, emb, cos, sin, cid):
    rows, width = tokens.shape
    group, part = rows * slices, width // slices
    pairs = part // 128
    items = pieces(width // shards, width, which, GATHER_CLASS)
    nw = len(ws)
    f32 = jnp.float32
    out = pl.pallas_call(
        functools.partial(forward_body, slices, shards, items, nw),
        out_shape=gathered_shapes(slices, shards, ws, rows_in)
        + [
            jax.ShapeDtypeStruct((rows, width), BF),
            jax.ShapeDtypeStruct((8, 2 * width), f32),
            jax.ShapeDtypeStruct((group, 1), f32),
            jax.ShapeDtypeStruct((1, group), f32),
            jax.ShapeDtypeStruct((3, group, part), BF),
            jax.ShapeDtypeStruct((group, part), BF),
            jax.ShapeDtypeStruct((part // HD, group), f32),
            jax.ShapeDtypeStruct((rows, width), BF),
        ],
        in_specs=[ANY] * (nw + 2) + [VM] * 6,
        out_specs=[ANY] * (nw + 2) + [VM] * 8,
        scratch_shapes=gather_scratch(slices, shards, items)
        + row_scratch(slices, rows_in)
        + [
            pltpu.VMEM((shards // XS, XS) + ws[0].shape, BF),
            pltpu.VMEM((shards // XS, XS, width // shards, width), BF),
            pltpu.VMEM((3, width // 128, rows, 128), BF),
            pltpu.VMEM((slices // CORES, CORES, 1, rows), jnp.int32),
            DMA((3,)),
            DMA((3 + pairs, slices, pairs)),
            DMA((3 + pairs, slices, pairs)),
            DMA((3 + pairs, pairs)),
        ],
        compiler_params=pltpu.CompilerParams(
            collective_id=cid, has_side_effects=True, vmem_limit_bytes=VMEM_ALL
        ),
    )(*ws, *rows_in, tokens, member, ends, emb, cos, sin)
    full = [g.reshape((slices,) + r.shape) for g, r in zip(out[nw:], rows_in)]
    return merged(out[:nw]), full, out[nw + 2 :]


def backward_body(slices, shards, items, nw, nr, *refs):
    grads, rows_in = refs[:nw], refs[nw : nw + nr]
    at = nw + nr
    d_mixed, qkv, mixed, logsum, seg_col, seg_row, cos, sin, h_one = refs[at : at + 9]
    at += 9
    sums_out, rows_out = refs[at : at + nw + 1], refs[at + nw + 1 : at + nw + 1 + nr]
    out = refs[at + nw + 1 + nr]
    scratch = refs[at + nw + nr + 2 :]
    place = Place(slices, shards)
    g, dk, dv, dq, turned, grad_qkv, ssem, rsem, lsem = scratch[10 + 4 * nr :]
    sums = GradSum(place, items, list(grads) + [grad_qkv], sums_out, *scratch[:10])
    gathers = row_gathers(place, rows_in, rows_out, scratch[10:])
    rows, part = d_mixed.shape[0], g.shape[1]
    pairs = part // 128
    come = Exchange(place, ssem.at[0], rsem.at[0], lsem.at[0])
    backs = [
        Exchange(place, ssem.at[1 + t], rsem.at[1 + t], lsem.at[1 + t]) for t in range(pairs)
    ]
    me = come.me
    come.mine(d_mixed.at[:, span(me, part)], g.at[span(me, rows), :])
    for r in gathers:
        r.load()
    greet(place, seq=True)
    for k, (_, peer, _) in enumerate(come.peers):
        come.give((k, 0), d_mixed.at[:, span(peer, part)], g.at[span(me, rows), :])
    block = min(256, 128 * 3072 // seg_col.shape[0])

    def attend(h):
        if h % 2 == 0:
            dk[...] = jnp.zeros_like(dk)
            dv[...] = jnp.zeros_like(dv)

        def step(i, _):
            backward_block(
                qkv, mixed, logsum, g, seg_col, seg_row, dk, dv, dq, h, span(i, block), h % 2
            )
            return 0

        lax.fori_loop(0, seg_col.shape[0] // block, step, 0)

    def finish(t, k, owner):
        own = span(owner, rows)
        c, s = cos[own, :], sin[own, :]
        for j, d in enumerate((dq, dk)):
            v = d[own, :] * (HD**-0.5)
            turned[t, j, own, :] = (v * c - swap_halves(v) * s).astype(BF)
        turned[t, 2, own, :] = dv[own, :].astype(BF)
        first = pl.multiple_of(me * part + t * 128, 128)
        src, dst = turned.at[t, :, own, :], out.at[:, :, pl.ds(first, 128)]
        if k < len(come.peers):
            backs[t].give((k, 0), src, dst)
        else:
            backs[t].mine(src, dst)

    work = [(lambda: None, 14), (come.take, 0)] + [(r.start, 0) for r in gathers]
    owners = [peer for _, peer, _ in come.peers] + [me]
    for t in range(pairs):
        work += [(functools.partial(attend, h), 10) for h in (2 * t, 2 * t + 1)]
        work += [(functools.partial(finish, t, k, owner), 0) for k, owner in enumerate(owners)]
    work += [(r.middle, 0) for r in gathers]

    def weigh(j):
        if j == 0:
            for back in backs:
                back.take()
        width, wide = h_one.shape[1], 256

        def step(i, _):
            cols = span(i, wide)
            t = dot(h_one[...], out[j, :, cols], 0, 0).astype(BF)
            shape = grad_qkv.shape[:3] + (wide,)
            grad_qkv[:, :, :, pl.ds(pl.multiple_of(j * width + i * wide, wide), wide)] = t.reshape(shape)
            return 0

        lax.fori_loop(0, width // wide, step, 0)

    width = h_one.shape[1]
    steps = pipeline(sums.plan, sums.stages())
    cuts = []
    for j in range(3):
        piece = next(p for p in sums.plan if p["w"] == nw and p["first"] == j * width)
        cuts.append(
            next(k for k, st in enumerate(steps) if st.func == sums.over_c and st.args[0] is piece)
        )
    interleave(steps[: cuts[0]], work)
    for j in range(3):
        weigh(j)
        run(steps[cuts[j] : (cuts + [len(steps)])[j + 1]])
    for r in gathers:
        r.end()
    for ex in [come] + backs:
        ex.close()


def attention_backward(
    slices, shards, width, which, grads, rows_in, d_mixed, kept, seg_col, seg_row, cos, sin, h_one, cid
):
    rows = d_mixed.shape[0]
    group, part = rows * slices, width // slices
    items = pieces(width // shards, width, which, SUM_CLASS)
    nw, nr, pairs = len(grads), len(rows_in), part // 128
    grads = split_grads(shards, grads)
    total = pltpu.VMEM((group, 128), jnp.float32)
    out = pl.pallas_call(
        functools.partial(backward_body, slices, shards, items, nw, nr),
        out_shape=[jax.ShapeDtypeStruct(w.shape[2:], BF) for w in grads]
        + [jax.ShapeDtypeStruct((width // shards, 3 * width), BF)]
        + gathered_shapes(slices, shards, [], rows_in)
        + [jax.ShapeDtypeStruct((3, rows, width), BF)],
        in_specs=[ANY] * (nw + nr + 1) + [VM] * 8,
        out_specs=[ANY] * (nw + nr + 1) + [VM],
        scratch_shapes=sum_scratch(slices, shards, items)
        + row_scratch(slices, rows_in)
        + [pltpu.VMEM((group, part), BF), total, total, total]
        + [pltpu.VMEM((pairs, 3, group, 128), BF)]
        + [pltpu.VMEM((shards // XS, XS, width // shards, 3 * width), BF)]
        + [DMA((1 + pairs, slices, 1)), DMA((1 + pairs, slices, 1)), DMA((1 + pairs, 1))],
        compiler_params=pltpu.CompilerParams(
            collective_id=cid, has_side_effects=True, vmem_limit_bytes=VMEM_ALL
        ),
    )(*grads, *rows_in, d_mixed, *kept, seg_col, seg_row, cos, sin, h_one)
    full = [g.reshape((slices,) + r.shape) for g, r in zip(out[nw + 1 :], rows_in)]
    return out[: nw + 1], full, out[nw + 1 + nr]


def time_embedding(steps):
    half = TEMB // 2
    freqs = jnp.exp(-math.log(BASE) * jnp.arange(half, dtype=jnp.float32) / half)
    angles = steps.astype(jnp.float32)[:, None] * freqs[None, :]
    return jnp.concatenate([jnp.sin(angles), jnp.cos(angles)], axis=-1)


def layout(lens, places):
    ends = jnp.cumsum(lens)
    starts = ends - lens
    member = (places[:, None] >= starts[None, :]) & (places[:, None] < ends[None, :])
    labels = jnp.arange(NSEQ, dtype=jnp.int32)
    segment = jnp.sum(jnp.where(member, labels[None, :], 0), axis=1)
    offset = places - jnp.sum(jnp.where(member, starts[None, :], 0), axis=1)
    return (member.astype(jnp.float32), segment, offset)


def turn_tables(offset):
    half = HD // 2
    freqs = jnp.exp(-math.log(BASE) * jnp.arange(half, dtype=jnp.float32) * 2.0 / HD)
    angles = offset.astype(jnp.float32)[:, None] * freqs[None, :]
    c, s = jnp.cos(angles), jnp.sin(angles)
    return jnp.concatenate([c] * 4, axis=1), jnp.concatenate([-s, s, -s, s], axis=1)


def norm_mod(values, scale):
    centre = jnp.mean(values, axis=-1, keepdims=True)
    centred = values - centre
    spread = jnp.mean(centred * centred, axis=-1, keepdims=True)
    return centred * lax.rsqrt(spread + EPS) * (1.0 + scale)


def pick_rows(data, wanted, labels):
    pick = (wanted[:, None] == labels[None, :]).astype(BF)
    return jnp.dot(pick, data.reshape(-1, data.shape[-1]), preferred_element_type=jnp.float32)


def on_device(tokens, lengths, time_steps, order, w_time, w_qkv, w_out, w_up, w_down, cotangent):
    rows, width = tokens.shape[1:]
    slices, shards = lax.axis_size("seq"), lax.axis_size("fsdp")
    group = rows * slices
    lens, places = lengths[0], order[0]
    member, _, offset = layout(lens, places)
    emb = time_embedding(time_steps[0]).astype(BF)
    cos, sin = turn_tables(offset)
    fulls, (order_all, cot_all), kept = forward(
        slices,
        shards,
        "tqoud",
        [w_time, w_qkv, w_out, w_up, w_down],
        [order, cotangent[0]],
        tokens[0],
        jnp.pad(member, ((0, 0), (0, 8 - NSEQ))),
        jnp.broadcast_to(jnp.pad(jnp.cumsum(lens), (0, 8 - NSEQ))[:, None], (8, 128)),
        jnp.pad(emb, ((0, 8 - NSEQ), (0, 0))).reshape(8, shards, -1).transpose(1, 0, 2),
        cos,
        sin,
        0,
    )
    _, f_qkv, f_out, f_up, f_down = fulls
    h_one, scales_seq, seg_col, seg_row, heads_qkv, mixed_heads, logsum, mixed = kept
    order_all = order_all.reshape(group)
    _, _, offset_all = layout(lens, order_all)
    scales = jnp.dot(member, scales_seq[:NSEQ], precision=lax.Precision.HIGHEST)
    scale_one, scale_two = scales[:, :width], scales[:, width:]
    inputs = tokens[0].astype(jnp.float32)
    _, pull_one = jax.vjp(norm_mod, inputs, scale_one)

    x_two = inputs + jnp.dot(mixed, f_out, preferred_element_type=jnp.float32)
    normed_two, pull_two = jax.vjp(norm_mod, x_two, scale_two)
    h_two = normed_two.astype(BF)
    up = jnp.dot(h_two, f_up, preferred_element_type=jnp.float32)
    activated, pull_gelu = jax.vjp(jax.nn.gelu, up)
    hidden = activated.astype(BF)
    result = (x_two + jnp.dot(hidden, f_down, preferred_element_type=jnp.float32)).astype(BF)

    d_result = pick_rows(cot_all, places, jnp.arange(group, dtype=jnp.int32))
    d_low = d_result.astype(BF)
    grad_down = dot(hidden, d_low, 0, 0).astype(BF)
    d_up = pull_gelu(dot(d_low, f_down, 1, 1))[0].astype(BF)
    grad_up = dot(h_two, d_up, 0, 0).astype(BF)
    d_xpart, d_scale_two = pull_two(dot(d_up, f_up, 1, 1))
    d_xtwo = d_result + d_xpart
    d_attn = d_xtwo.astype(BF)
    grad_out = dot(mixed, d_attn, 0, 0).astype(BF)
    d_mixed = dot(d_attn, f_out, 1, 1).astype(BF)

    cos_all, sin_all = turn_tables(offset_all)
    sums, (result_all,), d_packed = attention_backward(
        slices,
        shards,
        width,
        "duoq",
        [grad_down, grad_up, grad_out],
        [result],
        d_mixed,
        (heads_qkv, mixed_heads, logsum),
        seg_col,
        seg_row,
        cos_all,
        sin_all,
        h_one,
        1,
    )
    d_qkv = d_packed.transpose(1, 0, 2).reshape(rows, 3 * width)
    d_xone, d_scale_one = pull_one(dot(d_qkv, f_qkv, 1, 1))
    input_grad = d_xtwo + d_xone
    d_scales = lax.dot_general(
        member,
        jnp.concatenate([d_scale_one, d_scale_two], axis=1),
        (((0,), (0,)), ((), ())),
        precision=lax.Precision.HIGHEST,
        preferred_element_type=jnp.float32,
    )
    emb_once = jnp.where(lax.axis_index("seq") == 0, emb.astype(jnp.float32), 0.0)
    packed = jnp.concatenate(
        [d_scales, jnp.pad(emb_once, ((0, 0), (0, 2 * width - TEMB)))], axis=0
    )
    spread_all = spread(slices, shards, jnp.pad(packed, ((0, 8 - 2 * NSEQ), (0, 0))), 2)
    shard = w_time.shape[0]
    emb_all = lax.dynamic_slice_in_dim(
        spread_all[:, NSEQ : 2 * NSEQ], lax.axis_index("fsdp") * shard, shard, 2
    )
    s_time = lax.dot_general(
        emb_all.reshape(-1, shard),
        spread_all[:, :NSEQ].reshape(-1, 2 * width),
        (((0,), (0,)), ((), ())),
        precision=lax.Precision.HIGHEST,
        preferred_element_type=jnp.float32,
    )
    s_down, s_up, s_out, s_qkv = [g.astype(jnp.float32) for g in sums]
    mine = lax.axis_index("seq") * rows + jnp.arange(rows, dtype=jnp.int32)
    output = pick_rows(result_all, mine, order_all).astype(BF)
    return (output[None], input_grad[None], s_time, s_qkv, s_out, s_up, s_down)


def solution(mesh):
    row, tok, mat = P("fsdp", None), P("fsdp", "seq", None), P("fsdp", None)
    return jax.shard_map(
        on_device,
        mesh=mesh,
        in_specs=(tok, row, row, P("fsdp", "seq"), mat, mat, mat, mat, mat, tok),
        out_specs=(tok, tok, mat, mat, mat, mat, mat),
        check_vma=False,
    )
```

```python
import functools
import math

import jax
import jax.numpy as jnp
from jax import lax
from jax.experimental import pallas as pl
from jax.experimental.pallas import tpu as pltpu
from jax.sharding import PartitionSpec as P

H = 16
HD = 64
TEMB = 256
NSEQ = 3

EPS = 1e-05
NEG = -1e30
BASE = 10000.0
LOG2E = math.log2(math.e)
CORES = 2
XS = 2
BF = jnp.bfloat16

ANY = pl.BlockSpec(memory_space=pl.ANY)
VM = pl.BlockSpec(memory_space=pltpu.VMEM)
DMA = pltpu.SemaphoreType.DMA
MESH = pl.DeviceIdType.MESH
VMEM_ALL = 67043328
CUT = 2
FIRST, PER = 14, 5
LAG = 2

GATHER_CLASS = {"t": "D", "q": "DDC", "o": "C", "u": "CCCC", "d": "CCDC"}
SUM_CLASS = {'q': 'DCD', 'o': 'C', 'u': 'CCCC', 'd': 'CDCC'}


class Place:
    def __init__(self, slices, shards):
        self.Y, self.Z = slices // CORES, shards // XS
        seq, fsdp = lax.axis_index("seq"), lax.axis_index("fsdp")
        self.y, self.c = lax.div(seq, CORES), lax.rem(seq, CORES)
        self.z, self.x = lax.div(fsdp, XS), lax.rem(fsdp, XS)

    def at(self, z=None, x=None, y=None, c=None):
        z = self.z if z is None else z
        x = self.x if x is None else x
        y = self.y if y is None else y
        c = self.c if c is None else c
        return {"seq": y * CORES + c, "fsdp": z * XS + x}

    def next_y(self, d):
        return lax.rem(self.y + d, self.Y)

    def next_z(self, d):
        return lax.rem(self.z + d, self.Z)


def greet(place, seq=False):
    barrier = pltpu.get_barrier_semaphore()
    others = [place.at(c=1 - place.c), place.at(x=1 - place.x)]
    others += [place.at(y=place.next_y(d)) for d in range(1, place.Y)]
    others += [place.at(z=place.next_z(d)) for d in range(1, place.Z)]
    if seq:
        others += [place.at(y=place.next_y(d), c=1 - place.c) for d in range(1, place.Y)]
    for other in others:
        pl.semaphore_signal(barrier, inc=1, device_id=other, device_id_type=MESH)
    pl.semaphore_wait(barrier, len(others))


def push(src, dst, send_sem, recv_sem, device):
    copy = pltpu.make_async_remote_copy(
        src_ref=src,
        dst_ref=dst,
        send_sem=send_sem,
        recv_sem=recv_sem,
        device_id=device,
        device_id_type=MESH,
    )
    copy.start()
    return copy


def keep(src, dst, sem):
    copy = pltpu.make_async_copy(src, dst, sem)
    copy.start()
    return copy


def pipeline(plan, stages):
    lags = [LAG * k for k in range(len(stages))]
    return [
        functools.partial(stage, plan[t - lag])
        for t in range(len(plan) + lags[-1])
        for lag, stage in zip(lags, stages)
        if 0 <= t - lag < len(plan)
    ]


def run(steps):
    for step in steps:
        step()


def interleave(steps, work):
    done = 0
    for piece, count in work:
        piece()
        run(steps[done : done + count])
        done += count
    run(steps[done:])


class RowGather:
    def __init__(self, place, src, out, bounce, sems, rsems, lsem):
        self.place, self.src, self.out = place, src, out
        self.bounce, self.sems, self.rsems, self.lsem = bounce, sems, rsems, lsem

    def load(self):
        self.own = keep(self.src, self.bounce, self.lsem)

    def start(self):
        p = self.place
        slot = self.out.at[p.y, p.c]
        self.over_y = [
            push(self.src, slot, self.sems.at[d], self.rsems.at[d], p.at(y=p.next_y(d)))
            for d in range(1, p.Y)
        ]
        self.own.wait()
        self.own = keep(self.bounce, slot, self.lsem)

    def middle(self):
        p = self.place
        for copy in self.over_y:
            copy.wait_recv()
        self.own.wait()
        half = self.out.at[:, p.c]
        self.over_c = push(half, half, self.sems.at[0], self.rsems.at[0], p.at(c=1 - p.c))

    def end(self):
        for copy in self.over_y:
            copy.wait_send()
        self.over_c.wait()


def pieces(rows, width, which, classes):
    whole = []
    for j, name in enumerate(which):
        if name == "t":
            for k, kind in enumerate(classes["t"]):
                span = 2 * width // len(classes["t"])
                whole.append((j, 0, rows // 4, k * span, span, kind))
        elif name == "d":
            for k, kind in enumerate(classes["d"]):
                whole.append((j, k * rows, rows, 0, width, kind))
        else:
            for k, kind in enumerate(classes[name]):
                whole.append((j, 0, rows, k * width, width, kind))
    out = []
    for j, r0, rn, c0, cn, kind in whole:
        cuts = CUT if rn % (16 * CUT) == 0 else 1
        out += [(j, r0 + k * rn // cuts, rn // cuts, c0, cn, kind) for k in range(cuts)]
    return out


class WeightGather:
    def __init__(self, place, items, shards, outs, bounce, ssem, rsem, lsem):
        self.place = place
        self.shards, self.outs, self.bounce = shards, outs, bounce
        self.ssem, self.rsem, self.lsem = ssem, rsem, lsem
        self.plan = []
        for i, (w, r0, rn, c0, cn, kind) in enumerate(items):
            half = cn // CORES
            width = half // place.Y if kind == "D" else half
            first = c0 + place.c * half
            if kind == "D":
                first = first + place.y * width
            self.plan.append(
                dict(
                    i=i,
                    w=w,
                    kind=kind,
                    first=c0,
                    rows=pl.ds(r0, rn),
                    cols=pl.ds(pl.multiple_of(first, 128), width),
                    half=pl.ds(pl.multiple_of(c0 + place.c * half, 128), half),
                    held=bounce.at[i, pl.ds(0, rn), pl.ds(0, width)],
                )
            )

    def region(self, p, z, x, cols):
        return self.outs[p["w"]].at[z, x, p["rows"], cols]

    def load(self):
        for p in self.plan:
            p["own"] = keep(
                self.shards[p["w"]].at[p["rows"], p["cols"]], p["held"], self.lsem.at[p["i"]]
            )

    def store(self):
        place = self.place
        for p in self.plan:
            p["own"].wait()
            p["own"] = keep(
                p["held"], self.region(p, place.z, place.x, p["cols"]), self.lsem.at[p["i"]]
            )

    def post(self, p, slot, src, dst, device):
        return push(src, dst, self.ssem.at[p["i"], slot], self.rsem.at[p["i"], slot], device)

    def over_z(self, p):
        place = self.place
        src = self.shards[p["w"]].at[p["rows"], p["cols"]]
        dst = self.region(p, place.z, place.x, p["cols"])
        p["z"] = [
            self.post(p, d - 1, src, dst, place.at(z=place.next_z(d))) for d in range(1, place.Z)
        ]

    def over_x(self, p):
        place = self.place
        for copy in p["z"]:
            copy.wait_recv()
        p["own"].wait()
        part = self.region(p, pl.ds(0, place.Z), place.x, p["cols"])
        p["x"] = self.post(p, place.Z - 1, part, part, place.at(x=1 - place.x))

    def over_y(self, p):
        place = self.place
        p["x"].wait_recv()
        p["y"] = []
        if p["kind"] == "D":
            part = self.region(p, pl.ds(0, place.Z), pl.ds(0, XS), p["cols"])
            p["y"] = [
                self.post(p, place.Z - 1 + d, part, part, place.at(y=place.next_y(d)))
                for d in range(1, place.Y)
            ]

    def over_c(self, p):
        place = self.place
        for copy in p["y"]:
            copy.wait_recv()
        part = self.region(p, pl.ds(0, place.Z), pl.ds(0, XS), p["half"])
        p["c"] = self.post(p, place.Z - 1 + place.Y, part, part, place.at(c=1 - place.c))

    def finish(self, p):
        p["c"].wait()
        for copy in p["z"] + p["y"] + [p["x"]]:
            copy.wait_send()

    def stages(self):
        return [self.over_z, self.over_x, self.over_y, self.over_c, self.finish]


def gather_scratch(slices, shards, items):
    Y, Z = slices // CORES, shards // XS
    n, rows = len(items), max(item[2] for item in items)
    widest = max(cn // CORES // (Y if kind == "D" else 1) for _, _, _, _, cn, kind in items)
    return [pltpu.VMEM((n, rows, widest), BF), DMA((n, Z + Y)), DMA((n, Z + Y)), DMA((n,))]


def gathered_shapes(slices, shards, ws, rows_in):
    Y, Z = slices // CORES, shards // XS
    return [jax.ShapeDtypeStruct((Z, XS) + w.shape, w.dtype) for w in ws] + [
        jax.ShapeDtypeStruct((Y, CORES) + r.shape, r.dtype) for r in rows_in
    ]


def row_scratch(slices, rows_in):
    Y = slices // CORES
    out = []
    for r in rows_in:
        out += [pltpu.VMEM(r.shape, r.dtype), DMA((Y,)), DMA((Y,)), DMA((1,))]
    return out


def row_gathers(place, rows_in, rows_out, scratch):
    rows = []
    for k, (src, out) in enumerate(zip(rows_in, rows_out)):
        b, s, r, m = scratch[4 * k : 4 * k + 4]
        rows.append(RowGather(place, src, out, b, s, r, m.at[0]))
    return rows


def merged(fulls):
    return [g.reshape(-1, g.shape[-1]) for g in fulls]


def add_into(dst, src, rn):
    lead = dst.shape[:-2]

    def step(k, _):
        idx, rest = [], k
        for size in reversed(lead[1:]):
            idx.append(lax.rem(rest, size))
            rest = lax.div(rest, size)
        idx = tuple(reversed(idx + [rest]))
        a, b = dst.at[idx], src.at[idx]
        rows = pl.ds(0, rn)
        a[rows, :] = (a[rows, :].astype(jnp.float32) + b[rows, :].astype(jnp.float32)).astype(BF)
        return 0

    lax.fori_loop(0, math.prod(lead), step, 0)


class GradSum:
    def __init__(self, place, items, grads, outs, acc, own, ry, rx, rz, fin, rf, lsem, ssem, rsem):
        self.place, self.grads, self.outs = place, grads, outs
        self.acc, self.own, self.ry, self.rx, self.rz = acc, own, ry, rx, rz
        self.fin, self.rf = fin, rf
        self.lsem, self.ssem, self.rsem = lsem, ssem, rsem
        self.wide = acc.shape[-1]
        self.plan = []
        for i, (w, r0, rn, c0, cn, kind) in enumerate(items):
            p = dict(i=i, w=w, kind=kind, rn=rn, c0=c0, half=cn // CORES)
            p["first"] = c0
            p["k"] = sum(q["kind"] == kind for q in self.plan)
            p.update(rows=pl.ds(r0, rn), vr=pl.ds(0, rn), sends=[])
            self.plan.append(p)

    def post(self, p, slot, src, dst, device):
        copy = push(src, dst, self.ssem.at[p["i"], slot], self.rsem.at[p["i"], slot], device)
        p["sends"].append(copy)
        return copy

    def cols(self, p, core, part=None):
        first = p["c0"] + core * p["half"]
        if part is None:
            return pl.ds(pl.multiple_of(first, 128), p["half"])
        return pl.ds(pl.multiple_of(first + part * self.wide, 128), self.wide)

    def parts(self, p):
        return [self.place.y] if p["kind"] == "D" else list(range(self.place.Y))

    def over_c(self, p):
        place, i, vr = self.place, p["i"], p["vr"]
        g = self.grads[p["w"]]
        first = place.Z + place.Y + place.Y
        p["own"], p["c"] = [], []
        for part in range(place.Y):
            p["own"].append(
                keep(
                    g.at[:, :, p["rows"], self.cols(p, place.c, part)],
                    self.own.at[i % (LAG + 1), part, :, :, vr, :],
                    self.lsem.at[i, part],
                )
            )
            p["c"].append(
                self.post(
                    p,
                    first + part,
                    g.at[:, :, p["rows"], self.cols(p, 1 - place.c, part)],
                    self.acc.at[i, part, :, :, vr, :],
                    place.at(c=1 - place.c),
                )
            )

    def over_y(self, p):
        place, i, vr = self.place, p["i"], p["vr"]
        for copy in p["own"]:
            copy.wait()
        for copy in p["c"]:
            copy.wait_recv()
        for part in range(place.Y):
            add_into(self.acc.at[i, part], self.own.at[i % (LAG + 1), part], p["rn"])
        p["y"] = []
        if p["kind"] == "D":
            for d in range(1, place.Y):
                y = place.next_y(d)
                p["y"].append(
                    self.post(
                        p,
                        d,
                        self.acc.at[i, y, :, :, vr, :],
                        self.ry.at[p["k"], d - 1, :, :, vr, :],
                        place.at(y=y),
                    )
                )

    def over_x(self, p):
        place, i, vr = self.place, p["i"], p["vr"]
        for d, copy in enumerate(p["y"]):
            copy.wait_recv()
            add_into(self.acc.at[i, place.y], self.ry.at[p["k"], d], p["rn"])
        other = 1 - place.x
        if p["kind"] == "D":
            src, dst = self.acc.at[i, place.y, :, other, vr, :], self.rx.at[i, 0, :, vr, :]
        else:
            src, dst = self.acc.at[i, :, :, other, vr, :], self.rx.at[i, :, :, vr, :]
        p["x"] = self.post(p, place.Y, src, dst, place.at(x=other))

    def over_z(self, p):
        place, i, vr = self.place, p["i"], p["vr"]
        p["x"].wait_recv()
        for k, part in enumerate(self.parts(p)):
            add_into(self.acc.at[i, part, :, place.x], self.rx.at[i, k], p["rn"])
        p["z"] = []
        for d in range(1, place.Z):
            z = place.next_z(d)
            if p["kind"] == "D":
                src = self.acc.at[i, place.y, z, place.x, vr, :]
                dst = self.rz.at[i, d - 1, 0, vr, :]
            else:
                src = self.acc.at[i, :, z, place.x, vr, :]
                dst = self.rz.at[i, d - 1, :, vr, :]
            p["z"].append(self.post(p, place.Y + d, src, dst, place.at(z=z)))

    def region(self, p, core, part=None):
        return self.outs[p["w"]].at[p["rows"], self.cols(p, core, part)]

    def back_y(self, p):
        place, i, vr = self.place, p["i"], p["vr"]
        for copy in p["z"]:
            copy.wait_recv()
        for k, part in enumerate(self.parts(p)):
            total = self.acc[i, part, place.z, place.x, vr, :].astype(jnp.float32)
            for d in range(1, place.Z):
                total = total + self.rz[i, d - 1, k, vr, :].astype(jnp.float32)
            if p["kind"] == "D":
                self.fin[i, 0, vr, :] = total.astype(BF)
            else:
                self.rf[p["k"], place.y, part, vr, :] = total.astype(BF)
        first = place.Z + place.Y - 1
        p["f"], p["st"] = [], []
        if p["kind"] == "D":
            src, dst = self.fin.at[i, 0, vr, :], self.region(p, place.c, place.y)
            p["st"].append(keep(src, dst, self.lsem.at[i, 0]))
        else:
            src = dst = self.rf.at[p["k"], place.y, :, vr, :]
        for d in range(1, place.Y):
            p["f"].append(self.post(p, first + d, src, dst, place.at(y=place.next_y(d))))

    def back_c(self, p):
        place, i, vr = self.place, p["i"], p["vr"]
        for copy in p["f"]:
            copy.wait_recv()
        if p["kind"] == "C":
            for part in range(place.Y):
                total = self.rf[p["k"], 0, part, vr, :].astype(jnp.float32)
                for y in range(1, place.Y):
                    total = total + self.rf[p["k"], y, part, vr, :].astype(jnp.float32)
                self.fin[i, part, vr, :] = total.astype(BF)
                src, dst = self.fin.at[i, part, vr, :], self.region(p, place.c, part)
                p["st"].append(keep(src, dst, self.lsem.at[i, part]))
        for copy in p["st"]:
            copy.wait()
        part = self.region(p, place.c)
        p["e"] = self.post(p, 0, part, part, place.at(c=1 - place.c))

    def finish(self, p):
        p["e"].wait_recv()
        for copy in p["sends"]:
            copy.wait_send()

    def stages(self):
        return [
            self.over_c,
            self.over_y,
            self.over_x,
            self.over_z,
            self.back_y,
            self.back_c,
            self.finish,
        ]


def sum_scratch(slices, shards, items):
    Y, Z = slices // CORES, shards // XS
    n, wide = len(items), items[0][4] // CORES // Y
    rows = max(item[2] for item in items)
    nd = max(1, sum(item[5] == "D" for item in items))
    nc = max(1, n - nd)
    return [
        pltpu.VMEM((n, Y, Z, XS, rows, wide), BF),
        pltpu.VMEM((LAG + 1, Y, Z, XS, rows, wide), BF),
        pltpu.VMEM((nd, Y - 1, Z, XS, rows, wide), BF),
        pltpu.VMEM((n, Y, Z, rows, wide), BF),
        pltpu.VMEM((n, Z - 1, Y, rows, wide), BF),
        pltpu.VMEM((n, Y, rows, wide), BF),
        pltpu.VMEM((nc, Y, Y, rows, wide), BF),
        DMA((n, Y)),
        DMA((n, Z + 3 * Y)),
        DMA((n, Z + 3 * Y)),
    ]


def split_grads(shards, grads):
    return [g.reshape(shards // XS, XS, -1, g.shape[1]) for g in grads]


def spread_body(slices, shards, mine, out, group, total, ssem, rsem):
    place = Place(slices, shards)
    seq = place.y * CORES + place.c
    fsdp = place.z * XS + place.x
    near, far = [], []
    for d in range(1, slices):
        near.append({"seq": lax.rem(seq + d, slices), "fsdp": fsdp})
    for d in range(1, shards):
        far.append({"seq": seq, "fsdp": lax.rem(fsdp + d, shards)})
    barrier = pltpu.get_barrier_semaphore()
    for other in near + far:
        pl.semaphore_signal(barrier, inc=1, device_id=other, device_id_type=MESH)
    pl.semaphore_wait(barrier, len(near + far))
    copies = [
        push(mine, group.at[seq], ssem.at[d], rsem.at[d], other) for d, other in enumerate(near)
    ]
    group[seq] = mine[...]
    for copy in copies:
        copy.wait_recv()
    total[...] = sum(group[k] for k in range(slices))
    first = slices - 1
    copies += [
        push(total, out.at[fsdp], ssem.at[first + d], rsem.at[first + d], other)
        for d, other in enumerate(far)
    ]
    out[fsdp] = total[...]
    for copy in copies[first:]:
        copy.wait_recv()
    for copy in copies:
        copy.wait_send()


def spread(slices, shards, mine, cid):
    n = slices + shards
    return pl.pallas_call(
        functools.partial(spread_body, slices, shards),
        out_shape=jax.ShapeDtypeStruct((shards,) + mine.shape, mine.dtype),
        in_specs=[VM],
        out_specs=VM,
        scratch_shapes=[
            pltpu.VMEM((slices,) + mine.shape, mine.dtype),
            pltpu.VMEM(mine.shape, mine.dtype),
            DMA((n,)),
            DMA((n,)),
        ],
        compiler_params=pltpu.CompilerParams(collective_id=cid, has_side_effects=True),
    )(mine)


def dot(a, b, ca, cb):
    return lax.dot_general(a, b, (((ca,), (cb,)), ((), ())), preferred_element_type=jnp.float32)


def swap_halves(v):
    lane = lax.broadcasted_iota(jnp.int32, v.shape, 1)
    left = pltpu.roll(v, v.shape[1] - HD // 2, 1)
    right = pltpu.roll(v, HD // 2, 1)
    return jnp.where(lax.rem(lane, HD) < HD // 2, left, right)


def forward_block(qkv, seg_col, seg_row, mixed, logsum, h, rows):
    lanes = slice(h * HD, (h + 1) * HD)
    s = dot(qkv[1, :, lanes], qkv[0, rows, lanes], 1, 1) * (LOG2E * HD**-0.5)
    s = jnp.where(seg_col[...] == seg_row[:, rows], s, NEG)
    peak = jnp.max(s, axis=0, keepdims=True)
    expo = jnp.exp2(s - peak)
    total = jnp.sum(expo, axis=0, keepdims=True)
    out = dot(expo.astype(BF), qkv[2, :, lanes], 0, 0)
    mixed[rows, lanes] = (out / total.T).astype(BF)
    logsum[h : h + 1, rows] = peak + jnp.log2(total)


def backward_block(qkv, mixed, logsum, g, seg_col, seg_row, dk, dv, dq, h, rows, slot):
    lanes = slice(h * HD, (h + 1) * HD)
    side = slice(slot * HD, (slot + 1) * HD)
    q, gb = qkv[0, rows, lanes], g[rows, lanes]
    k, v = qkv[1, :, lanes], qkv[2, :, lanes]
    prod = gb.astype(jnp.float32) * mixed[rows, lanes].astype(jnp.float32)
    delta = jnp.sum(prod, axis=1, keepdims=True).T
    s = dot(k, q, 1, 1) * (LOG2E * HD**-0.5)
    same = seg_col[...] == seg_row[:, rows]
    probs = jnp.where(same, jnp.exp2(s - logsum[h : h + 1, rows]), 0.0)
    ds = (probs * (dot(v, gb, 1, 1) - delta)).astype(BF)
    dv[:, side] += dot(probs.astype(BF), gb, 1, 0)
    dk[:, side] += dot(ds, q, 1, 0)
    dq[rows, side] = dot(ds, k, 0, 0)


class Exchange:
    def __init__(self, place, ssem, rsem, lsem):
        self.place, self.ssem, self.rsem, self.lsem = place, ssem, rsem, lsem
        self.me = place.y * CORES + place.c
        self.peers = []
        for dy in list(range(1, place.Y)) + [0]:
            for dc in (range(CORES) if dy else (1,)):
                y, c = place.next_y(dy), lax.rem(place.c + dc, CORES)
                self.peers.append((dy * CORES + dc, y * CORES + c, place.at(y=y, c=c)))
        self.copies, self.own = {}, []

    def give(self, key, src, dst):
        slot, _, device = self.peers[key[0]]
        sems = self.ssem.at[slot, key[1]], self.rsem.at[slot, key[1]]
        self.copies[key] = push(src, dst, *sems, device)

    def mine(self, src, dst, t=0):
        self.own.append(keep(src, dst, self.lsem.at[t]))

    def take(self):
        for copy in self.copies.values():
            copy.wait_recv()
        for copy in self.own:
            copy.wait()

    def close(self):
        for copy in self.copies.values():
            copy.wait_send()


def span(index, size):
    return pl.ds(pl.multiple_of(index * size, size), size)


def after(steps, stage, hooks):
    out = []
    for step in steps:
        out.append(step)
        if step.func == stage:
            out += hooks.get(step.args[0]["i"], [])
    return out


def forward_body(slices, shards, items, nw, *refs):
    ws, (order, cot) = refs[:nw], refs[nw : nw + 2]
    tokens, member, ends, emb, cos, sin, freqs = refs[nw + 2 : nw + 9]
    refs = refs[nw + 9 :]
    outs, rows_out = refs[:nw], refs[nw : nw + 2]
    h_one, scales, seg_col, seg_row, qkv, mixed_heads, logsum, mixed = refs[nw + 2 : nw + 10]
    cos_all, sin_all = refs[nw + 10 : nw + 12]
    scratch = refs[nw + 12 :]
    place = Place(slices, shards)
    gather = WeightGather(place, items, ws, outs, *scratch[:4])
    order_rows, cot_rows = row_gathers(place, (order, cot), rows_out, scratch[4:12])
    w_time, w_part, packed, places, csem, ssem, rsem, lsem = scratch[12:]
    rows, width = tokens.shape
    part = mixed_heads.shape[1]
    pairs = part // 128
    ex = [Exchange(place, ssem.at[t], rsem.at[t], lsem.at[t]) for t in range(3 + pairs)]
    comes, backs = ex[:3], ex[3:]
    me, peers = comes[0].me, comes[0].peers

    def first_norm():
        copy = keep(outs[0], w_time, csem.at[0])
        copy.wait()
        for j in range(shards):
            add = jnp.dot(
                emb[j], w_time[j // XS, j % XS], preferred_element_type=jnp.float32
            )
            scales[...] = add if j == 0 else scales[...] + add

        def step(i, _):
            own = span(i, rows // 3)
            v = tokens[own, :].astype(jnp.float32)
            scale = sum(member[own, j : j + 1] * scales[j : j + 1, :width] for j in range(NSEQ))
            centred = v - jnp.mean(v, axis=1, keepdims=True)
            spread = jnp.mean(centred * centred, axis=1, keepdims=True)
            h_one[own, :] = (centred * lax.rsqrt(spread + EPS) * (1.0 + scale)).astype(BF)
            return 0

        lax.fori_loop(0, 3, step, 0)

    def project(j):
        copy = keep(outs[1].at[:, :, :, j * width : (j + 1) * width], w_part, csem.at[1])
        copy.wait()
        wide = 256

        def step(i, _):
            cols = span(i, wide)
            w = w_part[:, :, :, cols].reshape(width, wide)
            y = jnp.dot(h_one[...], w, preferred_element_type=jnp.float32)
            for t in range(wide // 128):
                v = y[:, t * 128 : (t + 1) * 128]
                if j < 2:
                    v = v * cos[...] + swap_halves(v) * sin[...]
                packed[j, i * (wide // 128) + t] = v.astype(BF)
            return 0

        lax.fori_loop(0, width // wide, step, 0)
        for k, (_, peer, _) in enumerate(peers):
            for t in range(pairs):
                comes[j].give(
                    (k, t),
                    packed.at[j, peer * pairs + t],
                    qkv.at[j, span(me, rows), t * 128 : (t + 1) * 128],
                )
        for t in range(pairs):
            comes[j].mine(
                packed.at[j, me * pairs + t], qkv.at[j, span(me, rows), t * 128 : (t + 1) * 128], t
            )

    def segments():
        order_rows.middle()
        order_rows.end()
        copy = keep(rows_out[0], places, csem.at[2])
        copy.wait()
        row = jnp.concatenate(
            [places[y, c] for y in range(place.Y) for c in range(CORES)], axis=1
        )
        seg = sum((row >= ends[j : j + 1, :1]).astype(jnp.float32) for j in range(NSEQ - 1))
        seg_row[...] = seg
        seg_col[...] = seg.T

    def tables():
        row = jnp.concatenate(
            [places[y, c] for y in range(place.Y) for c in range(CORES)], axis=1
        )
        start = jnp.zeros_like(row)
        for j in range(NSEQ - 1):
            start = jnp.where(row >= ends[j : j + 1, :1], ends[j : j + 1, :1], start)
        offset = (row - start).astype(jnp.float32).T
        size = 256
        for i in range(offset.shape[0] // size):
            own = slice(i * size, (i + 1) * size)
            angles = offset[own] * freqs[0:1, :]
            cos_all[own, :] = jnp.cos(angles)
            sin_all[own, :] = jnp.sin(angles) * freqs[1:2, :]

    block = 256

    def attend(h):
        def step(i, _):
            forward_block(qkv, seg_col, seg_row, mixed_heads, logsum, h, span(i, block))
            return 0

        lax.fori_loop(0, seg_col.shape[0] // block, step, 0)

    def finish(t, k, owner):
        src = mixed_heads.at[span(owner, rows), t * 128 : (t + 1) * 128]
        first = pl.multiple_of(me * part + t * 128, 128)
        dst = mixed.at[:, pl.ds(first, 128)]
        if k < len(peers):
            backs[t].give((k, 0), src, dst)
        else:
            backs[t].mine(src, dst)

    def take():
        for come in comes:
            come.take()

    gather.load()
    order_rows.load()
    cot_rows.load()
    greet(place, seq=True)
    steps = pipeline(gather.plan, gather.stages())
    last = {p["w"]: p["i"] for p in gather.plan}
    ready = [[p["i"] for p in gather.plan if p["w"] == 1 and p["first"] == j * width][-1] for j in range(3)]
    hooks = {last[0]: [segments, first_norm]}
    for j in range(3):
        hooks[ready[j]] = [functools.partial(project, j)]
    steps = after(steps, gather.finish, hooks)
    run(steps[:1])
    order_rows.start()
    gather.store()
    ahead = steps.index(hooks[ready[2]][0]) + 1
    run(steps[1:ahead])
    work = [(lambda: None, 16), (take, 0), (cot_rows.start, 0)]
    owners = [peer for _, peer, _ in peers] + [me]
    for t in range(pairs):
        work += [(functools.partial(attend, h), 10) for h in (2 * t, 2 * t + 1)]
        work += [(functools.partial(finish, t, k, owner), 0) for k, owner in enumerate(owners)]
    work += [(tables, 4), (cot_rows.middle, 0)]
    interleave(steps[ahead:], work)
    for back in backs:
        back.take()
    cot_rows.end()
    for e in ex:
        e.close()


def forward(slices, shards, which, ws, rows_in, tokens, member, ends, emb, cos, sin, freqs, cid):
    rows, width = tokens.shape
    group, part = rows * slices, width // slices
    pairs = part // 128
    items = pieces(width // shards, width, which, GATHER_CLASS)
    nw = len(ws)
    f32 = jnp.float32
    out = pl.pallas_call(
        functools.partial(forward_body, slices, shards, items, nw),
        out_shape=gathered_shapes(slices, shards, ws, rows_in)
        + [
            jax.ShapeDtypeStruct((rows, width), BF),
            jax.ShapeDtypeStruct((8, 2 * width), f32),
            jax.ShapeDtypeStruct((group, 1), f32),
            jax.ShapeDtypeStruct((1, group), f32),
            jax.ShapeDtypeStruct((3, group, part), BF),
            jax.ShapeDtypeStruct((group, part), BF),
            jax.ShapeDtypeStruct((part // HD, group), f32),
            jax.ShapeDtypeStruct((rows, width), BF),
            jax.ShapeDtypeStruct((group, 128), f32),
            jax.ShapeDtypeStruct((group, 128), f32),
        ],
        in_specs=[ANY] * (nw + 2) + [VM] * 7,
        out_specs=[ANY] * (nw + 2) + [VM] * 10,
        scratch_shapes=gather_scratch(slices, shards, items)
        + row_scratch(slices, rows_in)
        + [
            pltpu.VMEM((shards // XS, XS) + ws[0].shape, BF),
            pltpu.VMEM((shards // XS, XS, width // shards, width), BF),
            pltpu.VMEM((3, width // 128, rows, 128), BF),
            pltpu.VMEM((slices // CORES, CORES, 1, rows), jnp.int32),
            DMA((3,)),
            DMA((3 + pairs, slices, pairs)),
            DMA((3 + pairs, slices, pairs)),
            DMA((3 + pairs, pairs)),
        ],
        compiler_params=pltpu.CompilerParams(
            collective_id=cid, has_side_effects=True, vmem_limit_bytes=VMEM_ALL
        ),
    )(*ws, *rows_in, tokens, member, ends, emb, cos, sin, freqs)
    full = [g.reshape((slices,) + r.shape) for g, r in zip(out[nw:], rows_in)]
    return merged(out[:nw]), full, out[nw + 2 :]


def backward_body(slices, shards, items, nw, nr, *refs):
    grads, rows_in = refs[:nw], refs[nw : nw + nr]
    at = nw + nr
    d_mixed, qkv, mixed, logsum, seg_col, seg_row, cos, sin, h_one = refs[at : at + 9]
    at += 9
    sums_out, rows_out = refs[at : at + nw + 1], refs[at + nw + 1 : at + nw + 1 + nr]
    out = refs[at + nw + 1 + nr]
    scratch = refs[at + nw + nr + 2 :]
    place = Place(slices, shards)
    g, dk, dv, dq, turned, grad_qkv, ssem, rsem, lsem = scratch[10 + 4 * nr :]
    sums = GradSum(place, items, list(grads) + [grad_qkv], sums_out, *scratch[:10])
    gathers = row_gathers(place, rows_in, rows_out, scratch[10:])
    rows, part = d_mixed.shape[0], g.shape[1]
    pairs = part // 128
    come = Exchange(place, ssem.at[0], rsem.at[0], lsem.at[0])
    backs = [
        Exchange(place, ssem.at[1 + t], rsem.at[1 + t], lsem.at[1 + t]) for t in range(pairs)
    ]
    me = come.me
    come.mine(d_mixed.at[:, span(me, part)], g.at[span(me, rows), :])
    for r in gathers:
        r.load()
    greet(place, seq=True)
    for k, (_, peer, _) in enumerate(come.peers):
        come.give((k, 0), d_mixed.at[:, span(peer, part)], g.at[span(me, rows), :])
    block = min(256, 128 * 3072 // seg_col.shape[0])

    def attend(h, half):
        if h % 2 == 0 and half == 0:
            dk[...] = jnp.zeros_like(dk)
            dv[...] = jnp.zeros_like(dv)

        def step(i, _):
            backward_block(
                qkv, mixed, logsum, g, seg_col, seg_row, dk, dv, dq, h, span(i, block), h % 2
            )
            return 0

        steps = seg_col.shape[0] // block // 2
        lax.fori_loop(half * steps, (half + 1) * steps, step, 0)

    def finish(t, k, owner):
        own = span(owner, rows)
        c, s = cos[own, :], sin[own, :]
        for j, d in enumerate((dq, dk)):
            v = d[own, :] * (HD**-0.5)
            turned[t, j, own, :] = (v * c - swap_halves(v) * s).astype(BF)
        turned[t, 2, own, :] = dv[own, :].astype(BF)
        first = pl.multiple_of(me * part + t * 128, 128)
        src, dst = turned.at[t, :, own, :], out.at[:, :, pl.ds(first, 128)]
        if k < len(come.peers):
            backs[t].give((k, 0), src, dst)
        else:
            backs[t].mine(src, dst)

    work = [(lambda: None, FIRST), (come.take, 0)] + [(r.start, 0) for r in gathers]
    owners = [peer for _, peer, _ in come.peers] + [me]
    for t in range(pairs):
        work += [
            (functools.partial(attend, h, half), PER)
            for h in (2 * t, 2 * t + 1)
            for half in range(2)
        ]
        work += [(functools.partial(finish, t, k, owner), 0) for k, owner in enumerate(owners)]
    work += [(r.middle, 0) for r in gathers]

    def weigh(j):
        if j == 0:
            for back in backs:
                back.take()
        width, wide = h_one.shape[1], 256

        def step(i, _):
            cols = span(i, wide)
            t = dot(h_one[...], out[j, :, cols], 0, 0).astype(BF)
            shape = grad_qkv.shape[:3] + (wide,)
            grad_qkv[:, :, :, pl.ds(pl.multiple_of(j * width + i * wide, wide), wide)] = t.reshape(shape)
            return 0

        lax.fori_loop(0, width // wide, step, 0)

    width = h_one.shape[1]
    steps = pipeline(sums.plan, sums.stages())
    cuts = []
    for j in range(3):
        piece = next(p for p in sums.plan if p["w"] == nw and p["first"] == j * width)
        cuts.append(
            next(k for k, st in enumerate(steps) if st.func == sums.over_c and st.args[0] is piece)
        )
    interleave(steps[: cuts[0]], work)
    for j in range(3):
        weigh(j)
        run(steps[cuts[j] : (cuts + [len(steps)])[j + 1]])
    for r in gathers:
        r.end()
    for ex in [come] + backs:
        ex.close()


def attention_backward(
    slices, shards, width, which, grads, rows_in, d_mixed, kept, seg_col, seg_row, cos, sin, h_one, cid
):
    rows = d_mixed.shape[0]
    group, part = rows * slices, width // slices
    items = pieces(width // shards, width, which, SUM_CLASS)
    nw, nr, pairs = len(grads), len(rows_in), part // 128
    grads = split_grads(shards, grads)
    total = pltpu.VMEM((group, 128), jnp.float32)
    out = pl.pallas_call(
        functools.partial(backward_body, slices, shards, items, nw, nr),
        out_shape=[jax.ShapeDtypeStruct(w.shape[2:], BF) for w in grads]
        + [jax.ShapeDtypeStruct((width // shards, 3 * width), BF)]
        + gathered_shapes(slices, shards, [], rows_in)
        + [jax.ShapeDtypeStruct((3, rows, width), BF)],
        in_specs=[ANY] * (nw + nr + 1) + [VM] * 8,
        out_specs=[ANY] * (nw + nr + 1) + [VM],
        scratch_shapes=sum_scratch(slices, shards, items)
        + row_scratch(slices, rows_in)
        + [pltpu.VMEM((group, part), BF), total, total, total]
        + [pltpu.VMEM((pairs, 3, group, 128), BF)]
        + [pltpu.VMEM((shards // XS, XS, width // shards, 3 * width), BF)]
        + [DMA((1 + pairs, slices, 1)), DMA((1 + pairs, slices, 1)), DMA((1 + pairs, 1))],
        compiler_params=pltpu.CompilerParams(
            collective_id=cid, has_side_effects=True, vmem_limit_bytes=VMEM_ALL
        ),
    )(*grads, *rows_in, d_mixed, *kept, seg_col, seg_row, cos, sin, h_one)
    full = [g.reshape((slices,) + r.shape) for g, r in zip(out[nw + 1 :], rows_in)]
    return out[: nw + 1], full, out[nw + 1 + nr]


def time_embedding(steps):
    half = TEMB // 2
    freqs = jnp.exp(-math.log(BASE) * jnp.arange(half, dtype=jnp.float32) / half)
    angles = steps.astype(jnp.float32)[:, None] * freqs[None, :]
    return jnp.concatenate([jnp.sin(angles), jnp.cos(angles)], axis=-1)


def layout(lens, places):
    ends = jnp.cumsum(lens)
    starts = ends - lens
    member = (places[:, None] >= starts[None, :]) & (places[:, None] < ends[None, :])
    labels = jnp.arange(NSEQ, dtype=jnp.int32)
    segment = jnp.sum(jnp.where(member, labels[None, :], 0), axis=1)
    offset = places - jnp.sum(jnp.where(member, starts[None, :], 0), axis=1)
    return (member.astype(jnp.float32), segment, offset)


def turn_rates():
    half = HD // 2
    freqs = jnp.exp(-math.log(BASE) * jnp.arange(half, dtype=jnp.float32) * 2.0 / HD)
    ones = jnp.ones(half, jnp.float32)
    sign = jnp.concatenate([-ones, ones, -ones, ones])
    return jnp.pad(jnp.stack([jnp.tile(freqs, 4), sign]), ((0, 6), (0, 0)))


def turn_tables(offset):
    half = HD // 2
    freqs = jnp.exp(-math.log(BASE) * jnp.arange(half, dtype=jnp.float32) * 2.0 / HD)
    angles = offset.astype(jnp.float32)[:, None] * freqs[None, :]
    c, s = jnp.cos(angles), jnp.sin(angles)
    return jnp.concatenate([c] * 4, axis=1), jnp.concatenate([-s, s, -s, s], axis=1)


def norm_mod(values, scale):
    centre = jnp.mean(values, axis=-1, keepdims=True)
    centred = values - centre
    spread = jnp.mean(centred * centred, axis=-1, keepdims=True)
    return centred * lax.rsqrt(spread + EPS) * (1.0 + scale)


def pick_rows(data, wanted, labels):
    pick = (wanted[:, None] == labels[None, :]).astype(BF)
    return jnp.dot(pick, data.reshape(-1, data.shape[-1]), preferred_element_type=jnp.float32)


def on_device(tokens, lengths, time_steps, order, w_time, w_qkv, w_out, w_up, w_down, cotangent):
    rows, width = tokens.shape[1:]
    slices, shards = lax.axis_size("seq"), lax.axis_size("fsdp")
    group = rows * slices
    lens, places = lengths[0], order[0]
    member, _, offset = layout(lens, places)
    emb = time_embedding(time_steps[0]).astype(BF)
    cos, sin = turn_tables(offset)
    fulls, (order_all, cot_all), kept = forward(
        slices,
        shards,
        "tqoud",
        [w_time, w_qkv, w_out, w_up, w_down],
        [order, cotangent[0]],
        tokens[0],
        jnp.pad(member, ((0, 0), (0, 8 - NSEQ))),
        jnp.broadcast_to(jnp.pad(jnp.cumsum(lens), (0, 8 - NSEQ))[:, None], (8, 128)),
        jnp.pad(emb, ((0, 8 - NSEQ), (0, 0))).reshape(8, shards, -1).transpose(1, 0, 2),
        cos,
        sin,
        turn_rates(),
        0,
    )
    _, f_qkv, f_out, f_up, f_down = fulls
    h_one, scales_seq, seg_col, seg_row, heads_qkv, mixed_heads, logsum, mixed = kept[:8]
    cos_all, sin_all = kept[8:]
    order_all = order_all.reshape(group)
    scales = jnp.dot(member, scales_seq[:NSEQ], precision=lax.Precision.HIGHEST)
    scale_one, scale_two = scales[:, :width], scales[:, width:]
    inputs = tokens[0].astype(jnp.float32)
    _, pull_one = jax.vjp(norm_mod, inputs, scale_one)

    x_two = inputs + jnp.dot(mixed, f_out, preferred_element_type=jnp.float32)
    normed_two, pull_two = jax.vjp(norm_mod, x_two, scale_two)
    h_two = normed_two.astype(BF)
    up = jnp.dot(h_two, f_up, preferred_element_type=jnp.float32)
    activated, pull_gelu = jax.vjp(jax.nn.gelu, up)
    hidden = activated.astype(BF)
    result = (x_two + jnp.dot(hidden, f_down, preferred_element_type=jnp.float32)).astype(BF)

    d_result = pick_rows(cot_all, places, jnp.arange(group, dtype=jnp.int32))
    d_low = d_result.astype(BF)
    grad_down = dot(hidden, d_low, 0, 0).astype(BF)
    d_up = pull_gelu(dot(d_low, f_down, 1, 1))[0].astype(BF)
    grad_up = dot(h_two, d_up, 0, 0).astype(BF)
    d_xpart, d_scale_two = pull_two(dot(d_up, f_up, 1, 1))
    d_xtwo = d_result + d_xpart
    d_attn = d_xtwo.astype(BF)
    grad_out = dot(mixed, d_attn, 0, 0).astype(BF)
    d_mixed = dot(d_attn, f_out, 1, 1).astype(BF)

    sums, (result_all,), d_packed = attention_backward(
        slices,
        shards,
        width,
        "duoq",
        [grad_down, grad_up, grad_out],
        [result],
        d_mixed,
        (heads_qkv, mixed_heads, logsum),
        seg_col,
        seg_row,
        cos_all,
        sin_all,
        h_one,
        1,
    )
    d_hone = sum(
        dot(d_packed[j], f_qkv[:, j * width : (j + 1) * width], 1, 1) for j in range(3)
    )
    d_xone, d_scale_one = pull_one(d_hone)
    input_grad = d_xtwo + d_xone
    d_scales = lax.dot_general(
        member,
        jnp.concatenate([d_scale_one, d_scale_two], axis=1),
        (((0,), (0,)), ((), ())),
        precision=lax.Precision.HIGHEST,
        preferred_element_type=jnp.float32,
    )
    emb_once = jnp.where(lax.axis_index("seq") == 0, emb.astype(jnp.float32), 0.0)
    packed = jnp.concatenate([d_scales.reshape(-1, 128), emb_once.reshape(-1, 128)], axis=0)
    rest = -packed.shape[0] % 8
    spread_all = spread(slices, shards, jnp.pad(packed, ((0, rest), (0, 0))), 2)
    shard, many = w_time.shape[0], d_scales.size // 128
    emb_all = spread_all[:, many : many + emb.size // 128].reshape(shards * NSEQ, TEMB)
    s_time = lax.dot_general(
        lax.dynamic_slice_in_dim(emb_all, lax.axis_index("fsdp") * shard, shard, 1),
        spread_all[:, :many].reshape(shards * NSEQ, 2 * width),
        (((0,), (0,)), ((), ())),
        precision=lax.Precision.HIGHEST,
        preferred_element_type=jnp.float32,
    )
    s_down, s_up, s_out, s_qkv = [g.astype(jnp.float32) for g in sums]
    mine = lax.axis_index("seq") * rows + jnp.arange(rows, dtype=jnp.int32)
    output = pick_rows(result_all, mine, order_all).astype(BF)
    return (output[None], input_grad[None], s_time, s_qkv, s_out, s_up, s_down)


def solution(mesh):
    row, tok, mat = P("fsdp", None), P("fsdp", "seq", None), P("fsdp", None)
    return jax.shard_map(
        on_device,
        mesh=mesh,
        in_specs=(tok, row, row, P("fsdp", "seq"), mat, mat, mat, mat, mat, tok),
        out_specs=(tok, tok, mat, mat, mat, mat, mat),
        check_vma=False,
    )
```
